32 devices in a mesh: dp: 4 (over y, z), tp: 8 (over x, core).
Axes of the slice: x: 4, y: 2, z: 2, core: 2. Of those that a mesh axis runs over, the one named last changes fastest.
The devices are a block of a 4x4x8 slice.
Arguments:
- hidden: bfloat16 [4, 768, 2560], P('dp'), parts along dimension 0
- norm_w: bfloat16 [2, 2560], replicated
- w_z: bfloat16 [2, 2560, 5120], P(None, None, 'tp')
- w_x: bfloat16 [2, 2560, 5120], P(None, None, 'tp')
- w_bc: bfloat16 [2, 2560, 256], replicated
- w_dt: bfloat16 [2, 2560, 80], P(None, None, 'tp')
- conv_x: bfloat16 [2, 4, 5120], P(None, None, 'tp')
- conv_bc: bfloat16 [2, 4, 256], replicated
- bias_x: bfloat16 [2, 5120], P(None, 'tp')
- bias_bc: bfloat16 [2, 256], replicated
- dt_bias: float32 [2, 80], P(None, 'tp')
- a_log: float32 [2, 80], P(None, 'tp')
- d_skip: float32 [2, 80], P(None, 'tp')
- gate_w: bfloat16 [2, 5120], P(None, 'tp')
- w_out: bfloat16 [2, 5120, 2560], P(None, 'tp')
Outputs:
- output: bfloat16 [4, 768, 2560], P('dp'), parts along dimension 0
There are 4 independent parts. The reference program is written for one: setup_inputs(seed, part) draws one part's arguments, and reference() takes and returns one part's arrays. A program takes and returns all parts, laid end to end along the dimension named above; an argument that names none is the same for every part.
All inputs are finite; a program needn't handle non-finite values.
Results may differ from the reference program's by a relative error of at most 0.014167.
Values sent between devices are 32-bit elements.
A program may use at most 768 MiB of HBM per device.

```python
import math
import jax
import jax.numpy as jnp
from jax import lax

BATCH_ROWS = 1
SEQ_LEN = 768
D_MODEL = 2560
HEADS = 80
HEAD_DIM = 64
STATE_DIM = 128
LAYERS = 2
CONV_WIDTH = 4
BLOCK_LEN = 256

INNER_WIDTH = HEADS * HEAD_DIM
EPSILON = 1e-5


def setup_inputs(seed: int = 0, part: int = 0) -> dict:
    key_list = jax.random.split(jax.random.key(seed), 16)
    part_key = jax.random.fold_in(jax.random.key(seed + 1), part)
    in_scale = D_MODEL ** -0.5
    hidden = jax.random.normal(part_key, (BATCH_ROWS, SEQ_LEN, D_MODEL), jnp.float32)
    head_scale = jnp.exp(jax.random.uniform(key_list[0], (LAYERS, HEADS), jnp.float32, -1.2, 1.2))
    col_scale = jnp.repeat(head_scale, HEAD_DIM, axis=1)[:, None, :]
    dt_init = jnp.exp(jax.random.uniform(key_list[1], (LAYERS, HEADS), jnp.float32, math.log(0.001), math.log(0.1)))
    return {
        'hidden': hidden.astype(jnp.bfloat16),
        'norm_w': (1.0 + 0.2 * jax.random.normal(key_list[2], (LAYERS, D_MODEL), jnp.float32)).astype(jnp.bfloat16),
        'w_z': (in_scale * jax.random.normal(key_list[3], (LAYERS, D_MODEL, INNER_WIDTH), jnp.float32)).astype(jnp.bfloat16),
        'w_x': (in_scale * col_scale * jax.random.normal(key_list[4], (LAYERS, D_MODEL, INNER_WIDTH), jnp.float32)).astype(jnp.bfloat16),
        'w_bc': (in_scale * jax.random.normal(key_list[5], (LAYERS, D_MODEL, 2 * STATE_DIM), jnp.float32)).astype(jnp.bfloat16),
        'w_dt': (0.5 * in_scale * jax.random.normal(key_list[6], (LAYERS, D_MODEL, HEADS), jnp.float32)).astype(jnp.bfloat16),
        'conv_x': (0.5 * jax.random.normal(key_list[7], (LAYERS, CONV_WIDTH, INNER_WIDTH), jnp.float32)).astype(jnp.bfloat16),
        'conv_bc': (0.5 * jax.random.normal(key_list[8], (LAYERS, CONV_WIDTH, 2 * STATE_DIM), jnp.float32)).astype(jnp.bfloat16),
        'bias_x': (0.3 * jax.random.normal(key_list[9], (LAYERS, INNER_WIDTH), jnp.float32)).astype(jnp.bfloat16),
        'bias_bc': (0.3 * jax.random.normal(key_list[10], (LAYERS, 2 * STATE_DIM), jnp.float32)).astype(jnp.bfloat16),
        'dt_bias': dt_init + jnp.log(-jnp.expm1(-dt_init)),
        'a_log': jnp.log(jax.random.uniform(key_list[11], (LAYERS, HEADS), jnp.float32, 1.0, 16.0)),
        'd_skip': jax.random.uniform(key_list[12], (LAYERS, HEADS), jnp.float32, 0.5, 2.0),
        'gate_w': (1.0 + 0.2 * jax.random.normal(key_list[13], (LAYERS, INNER_WIDTH), jnp.float32)).astype(jnp.bfloat16),
        'w_out': (INNER_WIDTH ** -0.5 * jax.random.normal(key_list[14], (LAYERS, INNER_WIDTH, D_MODEL), jnp.float32)).astype(jnp.bfloat16),
    }


def causal_conv(seq_in, kernel, conv_bias):
    n_steps = seq_in.shape[1]
    padded = jnp.pad(seq_in, ((0, 0), (CONV_WIDTH - 1, 0), (0, 0)))
    conv_sum = conv_bias.astype(jnp.float32)
    for tap_index in range(CONV_WIDTH):
        conv_sum = conv_sum + padded[:, tap_index:tap_index + n_steps, :].astype(jnp.float32) * kernel[tap_index].astype(jnp.float32)
    return conv_sum


def ssd_sequence(seq_in):
    x_heads, dt_val, a_vals, b_in, c_in = seq_in
    n_blocks = SEQ_LEN // BLOCK_LEN
    step_ids = jnp.arange(BLOCK_LEN)
    lower_tri = step_ids[:, None] >= step_ids[None, :]

    def block_step(state, block):
        x_block, dt_block, a_block, b_block, c_block = block
        a_cum = jnp.cumsum(a_block, axis=0)
        seg_sum = a_cum[:, None, :] - a_cum[None, :, :]
        decay_mat = jnp.where(lower_tri[:, :, None], jnp.exp(jnp.minimum(seg_sum, 0.0)), 0.0)
        c_dot_b = jnp.einsum('in,jn->ij', c_block, b_block)
        x_dt = x_block * dt_block[:, :, None]
        y_in = jnp.einsum('ijh,jhp->ihp', decay_mat * c_dot_b[:, :, None], x_dt)
        y_st = jnp.einsum('in,hpn->ihp', c_block, state) * jnp.exp(a_cum)[:, :, None]
        tail_decay = jnp.exp(a_cum[-1][None, :] - a_cum)
        new_state = state * jnp.exp(a_cum[-1])[:, None, None] + jnp.einsum('jn,jhp->hpn', b_block, x_dt * tail_decay[:, :, None])
        return new_state, y_in + y_st

    blocks_in = (
        x_heads.reshape(n_blocks, BLOCK_LEN, HEADS, HEAD_DIM),
        dt_val.reshape(n_blocks, BLOCK_LEN, HEADS),
        a_vals.reshape(n_blocks, BLOCK_LEN, HEADS),
        b_in.reshape(n_blocks, BLOCK_LEN, STATE_DIM),
        c_in.reshape(n_blocks, BLOCK_LEN, STATE_DIM),
    )
    init_state = jnp.zeros((HEADS, HEAD_DIM, STATE_DIM), jnp.float32)
    last_state, y_blocks = lax.scan(block_step, init_state, blocks_in)
    return y_blocks.reshape(SEQ_LEN, HEADS, HEAD_DIM)


def mixer_layer(current, layer_params):
    norm_w, w_z, w_x, w_bc, w_dt, conv_x, conv_bc, bias_x, bias_bc, dt_bias, a_log, d_skip, gate_w, w_out = layer_params
    tokens = BATCH_ROWS * SEQ_LEN
    residual = current.astype(jnp.float32)
    normed = (residual * lax.rsqrt(jnp.mean(residual * residual, axis=-1, keepdims=True) + EPSILON) * norm_w.astype(jnp.float32)).astype(jnp.bfloat16)
    flat_in = normed.reshape(tokens, D_MODEL)
    gate_z = jnp.dot(flat_in, w_z, preferred_element_type=jnp.float32).astype(jnp.bfloat16)
    x_pre = jnp.dot(flat_in, w_x, preferred_element_type=jnp.float32).astype(jnp.bfloat16)
    bc_pre = jnp.dot(flat_in, w_bc, preferred_element_type=jnp.float32).astype(jnp.bfloat16)
    dt_pre = jnp.dot(flat_in, w_dt, preferred_element_type=jnp.float32).astype(jnp.bfloat16)
    x_act = jax.nn.silu(causal_conv(x_pre.reshape(BATCH_ROWS, SEQ_LEN, INNER_WIDTH), conv_x, bias_x))
    bc_act = jax.nn.silu(causal_conv(bc_pre.reshape(BATCH_ROWS, SEQ_LEN, 2 * STATE_DIM), conv_bc, bias_bc))
    dt_val = jax.nn.softplus(dt_pre.astype(jnp.float32).reshape(BATCH_ROWS, SEQ_LEN, HEADS) + dt_bias)
    a_vals = -dt_val * jnp.exp(a_log)
    x_heads = x_act.reshape(BATCH_ROWS, SEQ_LEN, HEADS, HEAD_DIM)
    y_heads = lax.map(ssd_sequence, (x_heads, dt_val, a_vals, bc_act[..., :STATE_DIM], bc_act[..., STATE_DIM:]))
    y_heads = y_heads + d_skip[:, None] * x_heads
    gated_v = y_heads.reshape(BATCH_ROWS, SEQ_LEN, INNER_WIDTH) * jax.nn.silu(gate_z.astype(jnp.float32).reshape(BATCH_ROWS, SEQ_LEN, INNER_WIDTH))
    normed_y = (gated_v * lax.rsqrt(jnp.mean(gated_v * gated_v, axis=-1, keepdims=True) + EPSILON) * gate_w.astype(jnp.float32)).astype(jnp.bfloat16)
    mixed_out = jnp.dot(normed_y.reshape(tokens, INNER_WIDTH), w_out, preferred_element_type=jnp.float32)
    return (residual + mixed_out.reshape(BATCH_ROWS, SEQ_LEN, D_MODEL)).astype(jnp.bfloat16)


def reference(hidden, norm_w, w_z, w_x, w_bc, w_dt, conv_x, conv_bc, bias_x, bias_bc, dt_bias, a_log, d_skip, gate_w, w_out):
    params = (norm_w, w_z, w_x, w_bc, w_dt, conv_x, conv_bc, bias_x, bias_bc, dt_bias, a_log, d_skip, gate_w, w_out)

    def layer_step(current, layer_params):
        return mixer_layer(current, layer_params), None

    final_hidden, unused = lax.scan(layer_step, hidden, params)
    return final_hidden
```

```python
import functools

import jax
import jax.numpy as jnp
from jax import lax
from jax.experimental import pallas as pl
from jax.experimental.pallas import tpu as pltpu
from jax.sharding import PartitionSpec as P

EPSILON = 1e-5
F32 = jnp.float32
BF16 = jnp.bfloat16
FULL = lax.Precision.HIGHEST
MESH = pl.DeviceIdType.MESH
LANES = 128
CHUNK = 128
SLOTS = 4
HALO = 8
SIB, FAR_P, FAR_M, NEAR_P, NEAR_M, COMB_P, COMB_M, AG_P, AG_M, FW_P, FW_M, D0, D1, D2, D3 = range(15)


def full_dot(a, b, dims=(((1,), (0,)), ((), ()))):
    return lax.dot_general(a, b, dims, precision=FULL, preferred_element_type=F32)


def silu(a):
    return a * (1.0 / (1.0 + jnp.exp(-a)))


def softplus(a):
    return jnp.maximum(a, 0.0) + jnp.log1p(jnp.exp(-jnp.abs(a)))


def kernel(tp_size, conv_width, hid_hbm, norm_in, wz_hbm, wx_hbm, wbc_hbm, wdt_hbm, convx_in, convbc_in, biasx_in, biasbc_in,
           dtb_in, alog_in, dskip_in, gate_in, wout_hbm, out_hbm,
           hid, win, wdt, wout, ures, h, pre, act, v, g, dtp, state, pbuf, sib, far, near, comb, stats, nw, cw, gw, hp, ost,
           wsem, hsem, osem, ssend, srecv, msend, mrecv):
    n_layers, n_steps, d_model = ures.shape
    width = v.shape[1]
    conv_ch = act.shape[1]
    n_state = (conv_ch - width) // 2
    n_heads = dtb_in.shape[1]
    head_dim = width // n_heads
    n_chunks = n_steps // CHUNK
    n_tasks = n_layers * n_chunks
    n_chips = tp_size // 2
    half_rows = CHUNK // 2
    slice_rows = half_rows // n_chips
    piece = slice_rows // 2
    inner_width = width * tp_size

    me = lax.axis_index('tp')
    chip = me // 2
    core = lax.rem(me, 2)
    nxt = lax.rem(chip + 1, n_chips)
    prv = lax.rem(chip + n_chips - 1, n_chips)
    opp = lax.rem(chip + 2, n_chips)
    dev_nxt = {'tp': nxt * 2 + core}
    dev_prv = {'tp': prv * 2 + core}
    dev_sib = {'tp': chip * 2 + 1 - core}

    barrier = pltpu.get_barrier_semaphore()
    for off in range(1, tp_size):
        pl.semaphore_signal(barrier, inc=1, device_id={'tp': lax.rem(me + off, tp_size)}, device_id_type=MESH)

    def load_hid(i):
        rows = pl.ds(pl.multiple_of(i * CHUNK, CHUNK), CHUNK)
        return pltpu.make_async_copy(hid_hbm.at[rows], hid.at[rows], hsem.at[i])

    def load_in(layer):
        return (
            pltpu.make_async_copy(wz_hbm.at[layer], win.at[layer, :, pl.ds(0, width)], wsem.at[layer, 0]),
            pltpu.make_async_copy(wx_hbm.at[layer], win.at[layer, :, pl.ds(width, width)], wsem.at[layer, 1]),
            pltpu.make_async_copy(wbc_hbm.at[layer], win.at[layer, :, pl.ds(2 * width, 2 * n_state)], wsem.at[layer, 2]),
            pltpu.make_async_copy(wdt_hbm.at[layer], wdt.at[layer], wsem.at[layer, 3]),
        )

    def load_out(layer):
        return pltpu.make_async_copy(wout_hbm.at[layer], wout.at[layer], wsem.at[layer, 4])

    load_hid(0).start()
    for layer in range(n_layers):
        for cp in load_in(layer):
            cp.start()
        load_out(layer).start()
        if layer == 0:
            for i in range(1, n_chunks):
                load_hid(i).start()

    hp[...] = jnp.zeros_like(hp)
    dtp[...] = jnp.zeros_like(dtp)
    for layer in range(n_layers):
        nw[layer, 0:1, :] = norm_in[layer:layer + 1, :].astype(F32)
        gw[layer, 0:1, :] = gate_in[layer:layer + 1, :].astype(F32)
        cw[layer, 0:conv_width, 0:width] = convx_in[layer].astype(F32)
        cw[layer, 0:conv_width, width:conv_ch] = convbc_in[layer].astype(F32)
        cw[layer, conv_width:conv_width + 1, 0:width] = biasx_in[layer:layer + 1, :].astype(F32)
        cw[layer, conv_width:conv_width + 1, width:conv_ch] = biasbc_in[layer:layer + 1, :].astype(F32)
        hp[layer, 0:1, 0:n_heads] = dtb_in[layer:layer + 1, :]
        hp[layer, 1:2, 0:n_heads] = alog_in[layer:layer + 1, :]
        hp[layer, 2:3, 0:n_heads] = dskip_in[layer:layer + 1, :]

    pl.semaphore_wait(barrier, tp_size - 1)

    def where_of(t):
        layer = t // n_chunks
        return layer, pl.multiple_of((t - layer * n_chunks) * CHUNK, CHUNK)

    def remote(src, dst, slot, kind, dev):
        return pltpu.make_async_remote_copy(src_ref=src, dst_ref=dst, send_sem=msend.at[slot, kind], recv_sem=mrecv.at[slot, kind],
                                            device_id=dev, device_id_type=MESH)

    def slice_at(c, j):
        return pl.multiple_of(c * half_rows + j * slice_rows, slice_rows)

    def msg_rs(t, kind):
        slot = lax.rem(t, SLOTS)
        buf = pbuf.at[lax.rem(t, 2)]

        def src(j, part):
            return buf.at[pl.ds(pl.multiple_of(slice_at(core, j) + part * piece, piece), piece)]
        if kind == SIB:
            other = pl.multiple_of((1 - core) * half_rows, half_rows)
            return remote(buf.at[pl.ds(other, half_rows)], sib.at[lax.rem(t, 2)], slot, kind, dev_sib)
        if kind == FAR_P:
            return remote(src(opp, 1), far.at[slot, 0], slot, kind, dev_nxt)
        if kind == FAR_M:
            return remote(src(opp, 0), far.at[slot, 1], slot, kind, dev_prv)
        if kind == NEAR_P:
            return remote(src(nxt, 0), near.at[slot, 0], slot, kind, dev_nxt)
        if kind == NEAR_M:
            return remote(src(prv, 1), near.at[slot, 1], slot, kind, dev_prv)
        if kind == COMB_P:
            return remote(src(nxt, 1), comb.at[slot, 0], slot, kind, dev_nxt)
        return remote(src(prv, 0), comb.at[slot, 1], slot, kind, dev_prv)

    def msg_ag(t, kind, c=None):
        slot = lax.rem(t, SLOTS)
        layer, row0 = where_of(t)
        c = core if c is None else c

        def rows(j, part=None):
            base = row0 + slice_at(c, j)
            if part is None:
                return ures.at[layer, pl.ds(pl.multiple_of(base, slice_rows), slice_rows)]
            return ures.at[layer, pl.ds(pl.multiple_of(base + part * piece, piece), piece)]
        ref, dev = {
            AG_P: lambda: (rows(chip), dev_nxt),
            AG_M: lambda: (rows(chip), dev_prv),
            FW_P: lambda: (rows(prv, 0), dev_nxt),
            FW_M: lambda: (rows(nxt, 1), dev_prv),
            D0: lambda: (rows(chip), dev_sib),
            D1: lambda: (rows(prv), dev_sib),
            D2: lambda: (rows(nxt), dev_sib),
            D3: lambda: (rows(opp), dev_sib),
        }[kind]()
        return remote(ref, ref, slot, kind, dev)

    def wait_ag(t, kind):
        slot = lax.rem(t, SLOTS)
        layer, row0 = where_of(t)

        def rows(c, j, part=None):
            base = row0 + slice_at(c, j)
            if part is None:
                return ures.at[layer, pl.ds(pl.multiple_of(base, slice_rows), slice_rows)]
            return ures.at[layer, pl.ds(pl.multiple_of(base + part * piece, piece), piece)]
        ref = {
            AG_P: lambda: rows(core, prv),
            AG_M: lambda: rows(core, nxt),
            FW_P: lambda: rows(core, opp, 0),
            FW_M: lambda: rows(core, opp, 1),
            D0: lambda: rows(1 - core, chip),
            D1: lambda: rows(1 - core, prv),
            D2: lambda: rows(1 - core, nxt),
            D3: lambda: rows(1 - core, opp),
        }[kind]()
        remote(ref, ref, slot, kind, dev_sib).wait_recv()

    def msg_stat(t, off):
        slot = lax.rem(t, SLOTS)
        return pltpu.make_async_remote_copy(src_ref=stats.at[slot, me], dst_ref=stats.at[slot, me], send_sem=ssend.at[slot, off],
                                            recv_sem=srecv.at[slot, me], device_id={'tp': lax.rem(me + off, tp_size)}, device_id_type=MESH)

    def in_proj(t):
        layer, row0 = where_of(t)

        @pl.when(layer == 0)
        def _():
            load_hid(t).wait()

        @pl.when(row0 == 0)
        def _():
            for cp in load_in(layer):
                cp.wait()
            pre[0:HALO, :] = jnp.zeros((HALO, pre.shape[1]), F32)

        @pl.when(row0 > 0)
        def _():
            pre[0:HALO, :] = pre[CHUNK:CHUNK + HALO, :]

        def norm(load):
            def block(i, carry):
                r = pl.multiple_of(i * 16, 16)
                u = load(pl.multiple_of(row0 + r, 16))
                scale = lax.rsqrt(jnp.mean(u * u, axis=-1, keepdims=True) + EPSILON)
                h[pl.ds(r, 16), :] = (u * scale * nw[layer, 0:1, :]).astype(BF16)
                return carry
            lax.fori_loop(0, CHUNK // 16, block, 0)

        @pl.when(layer == 0)
        def _():
            norm(lambda r: hid[pl.ds(r, 16), :].astype(F32))

        @pl.when(layer > 0)
        def _():
            norm(lambda r: ures[jnp.maximum(layer - 1, 0), pl.ds(r, 16), :])

        def tile(i, carry):
            o = pl.multiple_of(i * 256, 256)
            prod = jnp.dot(h[...], win[layer, :, pl.ds(o, 256)], preferred_element_type=F32)
            pre[HALO:HALO + CHUNK, pl.ds(o, 256)] = prod.astype(BF16).astype(F32)
            return carry
        lax.fori_loop(0, pre.shape[1] // 256, tile, 0)
        prod = jnp.dot(h[...], wdt[layer], preferred_element_type=F32)
        dtp[:, 0:n_heads] = prod.astype(BF16).astype(F32)

    def mix(t):
        slot = lax.rem(t, SLOTS)
        layer, row0 = where_of(t)

        @pl.when(row0 == 0)
        def _():
            state[...] = jnp.zeros_like(state)

        def conv(i, carry):
            o = pl.multiple_of(i * LANES, LANES)
            acc = jnp.broadcast_to(cw[layer, conv_width:conv_width + 1, pl.ds(o, LANES)], (CHUNK, LANES))
            for j in range(conv_width):
                first = HALO - (conv_width - 1) + j
                acc = acc + pre[first:first + CHUNK, pl.ds(pl.multiple_of(width + o, LANES), LANES)] * cw[layer, j:j + 1, pl.ds(o, LANES)]
            act[:, pl.ds(o, LANES)] = silu(acc)
            return carry
        lax.fori_loop(0, conv_ch // LANES, conv, 0)

        row_id = lax.broadcasted_iota(jnp.int32, (CHUNK, CHUNK), 0)
        col_id = lax.broadcasted_iota(jnp.int32, (CHUNK, CHUNK), 1)
        lower = row_id >= col_id
        left = col_id < head_dim
        left_row = left[0:1, :]
        dt = softplus(dtp[...] + hp[layer, 0:1, :])
        a = -dt * jnp.exp(hp[layer, 1:2, :])
        a_cum = full_dot(jnp.where(lower, 1.0, 0.0).astype(F32), a)
        a_cum_t = a_cum.T
        a_last = a_cum[CHUNK - 1:CHUNK, :]
        from_start = jnp.exp(a_cum)
        to_end = jnp.exp(a_last - a_cum)
        whole = jnp.exp(a_last)
        skip = hp[layer, 2:3, :]
        b = act[:, width:width + n_state]
        c = act[:, width + n_state:conv_ch]
        c_dot_b = full_dot(c, b, (((1,), (1,)), ((), ())))
        b_t = b.T
        sq = jnp.zeros((CHUNK, LANES), F32)
        for p in range(width // LANES):
            cols = slice(p * LANES, (p + 1) * LANES)
            h0, h1 = 2 * p, 2 * p + 1

            def spread(m):
                return jnp.where(left, m[:, h0:h0 + 1], m[:, h1:h1 + 1])

            def spread_row(m):
                return jnp.where(left_row, m[:, h0:h0 + 1], m[:, h1:h1 + 1])

            def mixer(n):
                seg = a_cum[:, n:n + 1] - a_cum_t[n:n + 1, :]
                return jnp.where(lower, jnp.exp(jnp.minimum(seg, 0.0)), 0.0) * c_dot_b
            x = act[:, cols]
            x_dt = x * spread(dt)
            both = jnp.concatenate([jnp.where(left, x_dt, 0.0), jnp.where(left, 0.0, x_dt)], axis=0)
            y = full_dot(jnp.concatenate([mixer(h0), mixer(h1)], axis=1), both)
            s_in = state[:, cols]
            y = y + full_dot(c, s_in) * spread(from_start)
            state[:, cols] = s_in * spread_row(whole) + full_dot(b_t, x_dt * spread(to_end))
            y = y + spread_row(skip) * x
            gated = y * silu(pre[HALO:HALO + CHUNK, cols])
            v[:, cols] = gated
            sq = sq + gated * gated
        total = jnp.sum(sq.T, axis=0, keepdims=True)
        stats[slot, me] = jnp.broadcast_to(total, (8, CHUNK))
        for off in range(1, tp_size):
            msg_stat(t, off).start()

    def out_proj(t):
        slot = lax.rem(t, SLOTS)
        layer, row0 = where_of(t)

        @pl.when(row0 == 0)
        def _():
            load_out(layer).wait()
        for off in range(1, tp_size):
            peer = lax.rem(me + off, tp_size)
            pltpu.make_async_remote_copy(src_ref=stats.at[slot, peer], dst_ref=stats.at[slot, peer], send_sem=ssend.at[slot, off],
                                         recv_sem=srecv.at[slot, peer], device_id=dev_sib, device_id_type=MESH).wait_recv()
        for off in range(1, tp_size):
            msg_stat(t, off).wait_send()
        total = stats[slot, 0]
        for r in range(1, tp_size):
            total = total + stats[slot, r]
        scale = lax.rsqrt(total / inner_width + EPSILON)
        scale = jnp.broadcast_to(scale[0:1, :], (LANES, CHUNK)).T
        for p in range(width // LANES):
            cols = slice(p * LANES, (p + 1) * LANES)
            g[:, cols] = (v[:, cols] * scale * gw[layer, 0:1, cols]).astype(BF16)
        buf = pbuf.at[lax.rem(t, 2)]

        def tile(i, carry):
            o = pl.multiple_of(i * 256, 256)
            buf[:, pl.ds(o, 256)] = jnp.dot(g[...], wout[layer, :, pl.ds(o, 256)], preferred_element_type=F32)
            return carry
        lax.fori_loop(0, d_model // 256, tile, 0)
        msg_rs(t, SIB).start()

    def pair_sum(t):
        msg_rs(t, SIB).wait_recv()
        buf, other = pbuf.at[lax.rem(t, 2)], sib.at[lax.rem(t, 2)]

        def block(i, carry):
            r = pl.multiple_of(i * 8, 8)
            mine = pl.ds(pl.multiple_of(core * half_rows + r, 8), 8)
            buf[mine, :] = buf[mine, :] + other[pl.ds(r, 8), :]
            return carry
        lax.fori_loop(0, half_rows // 8, block, 0)
        for kind in (FAR_P, FAR_M, NEAR_P, NEAR_M):
            msg_rs(t, kind).start()

    def relay_sum(t):
        slot = lax.rem(t, SLOTS)
        buf = pbuf.at[lax.rem(t, 2)]
        for way, (wait, send, j, part) in enumerate(((FAR_P, COMB_P, nxt, 1), (FAR_M, COMB_M, prv, 0))):
            msg_rs(t, wait).wait_recv()
            rows = pl.ds(pl.multiple_of(slice_at(core, j) + part * piece, piece), piece)
            buf[rows, :] = buf[rows, :] + far[slot, way]
            msg_rs(t, send).start()

    def finish(t):
        slot = lax.rem(t, SLOTS)
        layer, row0 = where_of(t)
        buf = pbuf.at[lax.rem(t, 2)]
        for kind in (NEAR_P, NEAR_M, COMB_P, COMB_M):
            msg_rs(t, kind).wait_recv()
        base = slice_at(core, chip)
        dst = pl.ds(pl.multiple_of(row0 + base, slice_rows), slice_rows)

        def store(res):
            lo = buf[pl.ds(base, piece), :] + near[slot, 0] + comb[slot, 1]
            hi = buf[pl.ds(pl.multiple_of(base + piece, piece), piece), :] + near[slot, 1] + comb[slot, 0]
            ures[layer, dst, :] = (res + jnp.concatenate([lo, hi], axis=0)).astype(BF16).astype(F32)

        @pl.when(layer == 0)
        def _():
            store(hid[dst, :].astype(F32))

        @pl.when(layer > 0)
        def _():
            store(ures[jnp.maximum(layer - 1, 0), dst, :])
        for kind in (AG_P, AG_M, D0):
            msg_ag(t, kind).start()
        for kind in (SIB, FAR_P, FAR_M, NEAR_P, NEAR_M, COMB_P, COMB_M):
            msg_rs(t, kind).wait_send()

    def forward(t):
        wait_ag(t, AG_P)
        msg_ag(t, FW_P).start()
        wait_ag(t, AG_M)
        msg_ag(t, FW_M).start()
        msg_ag(t, D1).start()
        msg_ag(t, D2).start()

    def collect(t):
        layer, row0 = where_of(t)
        wait_ag(t, FW_P)
        wait_ag(t, FW_M)
        msg_ag(t, D3).start()
        for kind in (D0, D1, D2, D3):
            wait_ag(t, kind)
        for kind in (AG_P, AG_M, FW_P, FW_M, D0, D1, D2, D3):
            msg_ag(t, kind).wait_send()

        @pl.when(layer == n_layers - 1)
        def _():
            rows = pl.ds(row0, CHUNK)

            def block(i, carry):
                r = pl.multiple_of(i * 16, 16)
                ost[pl.ds(r, 16), :] = ures[layer, pl.ds(pl.multiple_of(row0 + r, 16), 16), :].astype(BF16)
                return carry

            @pl.when(row0 > 0)
            def _():
                pltpu.make_async_copy(ost, out_hbm.at[rows], osem).wait()
            lax.fori_loop(0, CHUNK // 16, block, 0)
            pltpu.make_async_copy(ost, out_hbm.at[rows], osem).start()

    def guarded(step, t):
        @pl.when((t >= 0) & (t < n_tasks))
        def _():
            step(t)

    def iteration(t, carry):
        guarded(mix, t)
        guarded(forward, t - 3)
        guarded(pair_sum, t - 1)
        guarded(finish, t - 2)
        guarded(in_proj, t + 1)
        guarded(relay_sum, t - 1)
        guarded(out_proj, t)
        guarded(collect, t - 4)
        return carry
    lax.fori_loop(-1, n_tasks + 4, iteration, 0)
    pltpu.make_async_copy(ost, out_hbm.at[pl.ds(0, CHUNK)], osem).wait()


def layers(tp_size, hidden, norm_w, w_z, w_x, w_bc, w_dt, conv_x, conv_bc, bias_x, bias_bc, dt_bias, a_log, d_skip, gate_w, w_out):
    n_batch, n_steps, d_model = hidden.shape
    n_layers, conv_width, width = conv_x.shape
    n_heads = dt_bias.shape[-1]
    state2 = w_bc.shape[-1]
    piece = CHUNK // tp_size // 2
    any_spec = pl.BlockSpec(memory_space=pl.ANY)
    vmem_spec = pl.BlockSpec(memory_space=pltpu.VMEM)
    dma = pltpu.SemaphoreType.DMA
    run = pl.pallas_call(
        functools.partial(kernel, tp_size, conv_width),
        out_shape=jax.ShapeDtypeStruct((n_steps, d_model), BF16),
        in_specs=[any_spec, vmem_spec, any_spec, any_spec, any_spec, any_spec] + [vmem_spec] * 8 + [any_spec],
        out_specs=any_spec,
        scratch_shapes=[
            pltpu.VMEM((n_steps, d_model), BF16),
            pltpu.VMEM((n_layers, d_model, 2 * width + state2), BF16),
            pltpu.VMEM((n_layers, d_model, n_heads), BF16),
            pltpu.VMEM((n_layers, width, d_model), BF16),
            pltpu.VMEM((n_layers, n_steps, d_model), F32),
            pltpu.VMEM((CHUNK, d_model), BF16),
            pltpu.VMEM((HALO + CHUNK, 2 * width + state2), F32),
            pltpu.VMEM((CHUNK, width + state2), F32),
            pltpu.VMEM((CHUNK, width), F32),
            pltpu.VMEM((CHUNK, width), BF16),
            pltpu.VMEM((CHUNK, LANES), F32),
            pltpu.VMEM((state2 // 2, width), F32),
            pltpu.VMEM((2, CHUNK, d_model), F32),
            pltpu.VMEM((2, CHUNK // 2, d_model), F32),
            pltpu.VMEM((SLOTS, 2, piece, d_model), F32),
            pltpu.VMEM((SLOTS, 2, piece, d_model), F32),
            pltpu.VMEM((SLOTS, 2, piece, d_model), F32),
            pltpu.VMEM((SLOTS, tp_size, 8, CHUNK), F32),
            pltpu.VMEM((n_layers, 8, d_model), F32),
            pltpu.VMEM((n_layers, 8, width + state2), F32),
            pltpu.VMEM((n_layers, 8, width), F32),
            pltpu.VMEM((n_layers, 8, LANES), F32),
            pltpu.VMEM((CHUNK, d_model), BF16),
            dma((n_layers, 5)), dma((n_steps // CHUNK,)), dma,
            dma((SLOTS, tp_size)), dma((SLOTS, tp_size)), dma((SLOTS, 15)), dma((SLOTS, 15)),
        ],
        compiler_params=pltpu.CompilerParams(collective_id=0, has_side_effects=True, vmem_limit_bytes=67_043_328),
    )
    outs = [run(hidden[i], norm_w, w_z, w_x, w_bc, w_dt, conv_x, conv_bc, bias_x, bias_bc, dt_bias, a_log, d_skip, gate_w, w_out)
            for i in range(n_batch)]
    return jnp.stack(outs)


def solution(mesh):
    col_spec = P(None, None, 'tp')
    vec_spec = P(None, 'tp')
    in_specs = (P('dp'), P(), col_spec, col_spec, P(), col_spec, col_spec, P(), vec_spec, P(), vec_spec, vec_spec, vec_spec, vec_spec, P(None, 'tp', None))
    return jax.shard_map(functools.partial(layers, mesh.shape['tp']), mesh=mesh, in_specs=in_specs, out_specs=P('dp'), check_vma=False)
```

```python
import functools

import jax
import jax.numpy as jnp
from jax import lax
from jax.experimental import pallas as pl
from jax.experimental.pallas import tpu as pltpu
from jax.sharding import PartitionSpec as P

EPSILON = 1e-5
F32 = jnp.float32
BF16 = jnp.bfloat16
FULL = lax.Precision.HIGHEST
MESH = pl.DeviceIdType.MESH
LANES = 128
CHUNK = 128
SLOTS = 4
HALO = 8
TILE = 256
SIB, FAR_P, FAR_M, NEAR_P, NEAR_M, COMB_P, COMB_M, AG_P, AG_M, FW_P, FW_M, D0, D1, D2, D3 = range(15)


def full_dot(a, b, dims=(((1,), (0,)), ((), ()))):
    return lax.dot_general(a, b, dims, precision=FULL, preferred_element_type=F32)


def silu(a):
    return a * (1.0 / (1.0 + jnp.exp(-a)))


def softplus(a):
    return jnp.maximum(a, 0.0) + jnp.log1p(jnp.exp(-jnp.abs(a)))


def kernel(tp_size, conv_width, hid_hbm, norm_hbm, wz_hbm, wx_hbm, wbc_hbm, wdt_hbm, convx_hbm, convbc_hbm, biasx_hbm, biasbc_hbm,
           dtb_hbm, alog_hbm, dskip_hbm, gate_hbm, wout_hbm, out,
           norm_in, wdt_in, convx_in, convbc_in, biasx_in, biasbc_in, dtb_in, alog_in, dskip_in, gate_in,
           hid, win, wdt, wdt_f, wout, ures, h, pre, act, v, g, dtp, state, pbuf, sib, far, near, comb, stats, nw, cw, gw, hp,
           wsem, hsem, psem, ssend, srecv, msend, mrecv):
    n_layers, n_steps, d_model = ures.shape
    width = v.shape[1]
    conv_ch = act.shape[1]
    n_state = (conv_ch - width) // 2
    n_heads = dtb_in.shape[1]
    head_dim = width // n_heads
    n_chunks = n_steps // CHUNK
    n_tasks = n_layers * n_chunks
    n_chips = tp_size // 2
    n_tiles = pre.shape[1] // TILE
    half_rows = CHUNK // 2
    slice_rows = half_rows // n_chips
    piece = slice_rows // 2
    inner_width = width * tp_size

    me = lax.axis_index('tp')
    chip = me // 2
    core = lax.rem(me, 2)
    nxt = lax.rem(chip + 1, n_chips)
    prv = lax.rem(chip + n_chips - 1, n_chips)
    opp = lax.rem(chip + 2, n_chips)
    dev_nxt = {'tp': nxt * 2 + core}
    dev_prv = {'tp': prv * 2 + core}
    dev_sib = {'tp': chip * 2 + 1 - core}

    barrier = pltpu.get_barrier_semaphore()
    for off in range(1, tp_size):
        pl.semaphore_signal(barrier, inc=1, device_id={'tp': lax.rem(me + off, tp_size)}, device_id_type=MESH)

    def load_hid(i):
        rows = pl.ds(pl.multiple_of(i * CHUNK, CHUNK), CHUNK)
        return pltpu.make_async_copy(hid_hbm.at[rows], hid.at[rows], hsem.at[i])

    def load_in(layer):
        copies = []
        for w_hbm, first, n_cols in ((wz_hbm, 0, width), (wx_hbm, width, width), (wbc_hbm, 2 * width, 2 * n_state)):
            done = 0
            while done < n_cols:
                n = min(TILE - (first + done) % TILE, n_cols - done)
                at = first + done
                copies.append(pltpu.make_async_copy(w_hbm.at[layer, :, pl.ds(done, n)], win.at[layer, :, pl.ds(at, n)],
                                                    wsem.at[layer, at // TILE]))
                done += n
        return copies

    def wait_in(layer, tile):
        ref = win.at[layer, :, pl.ds(pl.multiple_of(tile * TILE, TILE), TILE)]
        pltpu.make_async_copy(ref, ref, wsem.at[layer, tile]).wait()

    def load_out(layer):
        return pltpu.make_async_copy(wout_hbm.at[layer], wout.at[layer], wsem.at[layer, n_tiles])

    params = ((norm_hbm, norm_in), (wdt_hbm, wdt_in), (convx_hbm, convx_in), (convbc_hbm, convbc_in), (biasx_hbm, biasx_in),
              (biasbc_hbm, biasbc_in), (dtb_hbm, dtb_in), (alog_hbm, alog_in), (dskip_hbm, dskip_in), (gate_hbm, gate_in))
    small = [pltpu.make_async_copy(src, dst, psem.at[i]) for i, (src, dst) in enumerate(params)]
    load_hid(0).start()
    for cp in small:
        cp.start()
    for cp in load_in(0):
        cp.start()
    for cp in small:
        cp.wait()

    hp[...] = jnp.zeros_like(hp)
    wdt_f[...] = jnp.zeros_like(wdt_f)
    for n in range(n_heads):
        cols = wdt_in[n].astype(F32)
        for layer in range(n_layers):
            wdt_f[layer, n:n + 1, :] = cols[layer:layer + 1, :]
    wdt[...] = wdt_f[...].astype(BF16)
    dtp[...] = jnp.zeros_like(dtp)
    for layer in range(n_layers):
        nw[layer, 0:1, :] = norm_in[layer:layer + 1, :].astype(F32)
        gw[layer, 0:1, :] = gate_in[layer:layer + 1, :].astype(F32)
        cw[layer, 0:conv_width, 0:width] = convx_in[layer].astype(F32)
        cw[layer, 0:conv_width, width:conv_ch] = convbc_in[layer].astype(F32)
        cw[layer, conv_width:conv_width + 1, 0:width] = biasx_in[layer:layer + 1, :].astype(F32)
        cw[layer, conv_width:conv_width + 1, width:conv_ch] = biasbc_in[layer:layer + 1, :].astype(F32)
        hp[layer, 0:1, 0:n_heads] = dtb_in[layer:layer + 1, :]
        hp[layer, 1:2, 0:n_heads] = alog_in[layer:layer + 1, :]
        hp[layer, 2:3, 0:n_heads] = dskip_in[layer:layer + 1, :]

    pl.semaphore_wait(barrier, tp_size - 1)

    def where_of(t):
        layer = t // n_chunks
        return layer, pl.multiple_of((t - layer * n_chunks) * CHUNK, CHUNK)

    def remote(src, dst, slot, kind, dev):
        return pltpu.make_async_remote_copy(src_ref=src, dst_ref=dst, send_sem=msend.at[slot, kind], recv_sem=mrecv.at[slot, kind],
                                            device_id=dev, device_id_type=MESH)

    def slice_at(c, j):
        return pl.multiple_of(c * half_rows + j * slice_rows, slice_rows)

    def msg_rs(t, kind):
        slot = lax.rem(t, SLOTS)
        buf = pbuf.at[lax.rem(t, 2)]

        def src(j, part):
            return buf.at[pl.ds(pl.multiple_of(slice_at(core, j) + part * piece, piece), piece)]
        if kind == SIB:
            other = pl.multiple_of((1 - core) * half_rows, half_rows)
            return remote(buf.at[pl.ds(other, half_rows)], sib.at[lax.rem(t, 2)], slot, kind, dev_sib)
        if kind == FAR_P:
            return remote(src(opp, 1), far.at[slot, 0], slot, kind, dev_nxt)
        if kind == FAR_M:
            return remote(src(opp, 0), far.at[slot, 1], slot, kind, dev_prv)
        if kind == NEAR_P:
            return remote(src(nxt, 0), near.at[slot, 0], slot, kind, dev_nxt)
        if kind == NEAR_M:
            return remote(src(prv, 1), near.at[slot, 1], slot, kind, dev_prv)
        if kind == COMB_P:
            return remote(src(nxt, 1), comb.at[slot, 0], slot, kind, dev_nxt)
        return remote(src(prv, 0), comb.at[slot, 1], slot, kind, dev_prv)

    def msg_ag(t, kind, c=None):
        slot = lax.rem(t, SLOTS)
        layer, row0 = where_of(t)
        c = core if c is None else c

        def rows(j, part=None):
            base = row0 + slice_at(c, j)
            if part is None:
                return ures.at[layer, pl.ds(pl.multiple_of(base, slice_rows), slice_rows)]
            return ures.at[layer, pl.ds(pl.multiple_of(base + part * piece, piece), piece)]
        ref, dev = {
            AG_P: lambda: (rows(chip), dev_nxt),
            AG_M: lambda: (rows(chip), dev_prv),
            FW_P: lambda: (rows(prv, 0), dev_nxt),
            FW_M: lambda: (rows(nxt, 1), dev_prv),
            D0: lambda: (rows(chip), dev_sib),
            D1: lambda: (rows(prv), dev_sib),
            D2: lambda: (rows(nxt), dev_sib),
            D3: lambda: (rows(opp), dev_sib),
        }[kind]()
        return remote(ref, ref, slot, kind, dev)

    def wait_ag(t, kind):
        slot = lax.rem(t, SLOTS)
        layer, row0 = where_of(t)

        def rows(c, j, part=None):
            base = row0 + slice_at(c, j)
            if part is None:
                return ures.at[layer, pl.ds(pl.multiple_of(base, slice_rows), slice_rows)]
            return ures.at[layer, pl.ds(pl.multiple_of(base + part * piece, piece), piece)]
        ref = {
            AG_P: lambda: rows(core, prv),
            AG_M: lambda: rows(core, nxt),
            FW_P: lambda: rows(core, opp, 0),
            FW_M: lambda: rows(core, opp, 1),
            D0: lambda: rows(1 - core, chip),
            D1: lambda: rows(1 - core, prv),
            D2: lambda: rows(1 - core, nxt),
            D3: lambda: rows(1 - core, opp),
        }[kind]()
        remote(ref, ref, slot, kind, dev_sib).wait_recv()

    def msg_stat(t, off):
        slot = lax.rem(t, SLOTS)
        return pltpu.make_async_remote_copy(src_ref=stats.at[slot, me], dst_ref=stats.at[slot, me], send_sem=ssend.at[slot, off],
                                            recv_sem=srecv.at[slot, me], device_id={'tp': lax.rem(me + off, tp_size)}, device_id_type=MESH)

    def in_proj(t):
        layer, row0 = where_of(t)

        @pl.when(layer == 0)
        def _():
            load_hid(t).wait()

        @pl.when(row0 == 0)
        def _():
            pre[0:HALO, :] = jnp.zeros((HALO, pre.shape[1]), F32)

        @pl.when(row0 > 0)
        def _():
            pre[0:HALO, :] = pre[CHUNK:CHUNK + HALO, :]

        def norm(load):
            def block(i, carry):
                r = pl.multiple_of(i * 16, 16)
                u = load(pl.multiple_of(row0 + r, 16))
                scale = lax.rsqrt(jnp.mean(u * u, axis=-1, keepdims=True) + EPSILON)
                h[pl.ds(r, 16), :] = (u * scale * nw[layer, 0:1, :]).astype(BF16)
                return carry
            lax.fori_loop(0, CHUNK // 16, block, 0)

        @pl.when(layer == 0)
        def _():
            norm(lambda r: hid[pl.ds(r, 16), :].astype(F32))

        @pl.when(layer > 0)
        def _():
            norm(lambda r: ures[jnp.maximum(layer - 1, 0), pl.ds(r, 16), :])

        def tile(i, carry):
            @pl.when(row0 == 0)
            def _():
                wait_in(layer, i)
            o = pl.multiple_of(i * TILE, TILE)
            prod = jnp.dot(h[...], win[layer, :, pl.ds(o, TILE)], preferred_element_type=F32)
            pre[HALO:HALO + CHUNK, pl.ds(o, TILE)] = prod.astype(BF16).astype(F32)
            return carry
        lax.fori_loop(0, pre.shape[1] // TILE, tile, 0)
        prod = lax.dot_general(h[...], wdt[layer], (((1,), (1,)), ((), ())), preferred_element_type=F32)
        dtp[:, 0:wdt.shape[1]] = prod.astype(BF16).astype(F32)

        @pl.when(t == 0)
        def _():
            load_out(0).start()
            for i in range(1, n_chunks):
                load_hid(i).start()

        @pl.when((row0 == CHUNK) & (layer < n_layers - 1))
        def _():
            for k in range(1, n_layers):
                @pl.when(layer == k - 1)
                def _():
                    for cp in load_in(k):
                        cp.start()
                    load_out(k).start()

    def mix(t):
        slot = lax.rem(t, SLOTS)
        layer, row0 = where_of(t)

        @pl.when(row0 == 0)
        def _():
            state[...] = jnp.zeros_like(state)

        def conv(i, carry):
            o = pl.multiple_of(i * LANES, LANES)
            acc = jnp.broadcast_to(cw[layer, conv_width:conv_width + 1, pl.ds(o, LANES)], (CHUNK, LANES))
            for j in range(conv_width):
                first = HALO - (conv_width - 1) + j
                acc = acc + pre[first:first + CHUNK, pl.ds(pl.multiple_of(width + o, LANES), LANES)] * cw[layer, j:j + 1, pl.ds(o, LANES)]
            act[:, pl.ds(o, LANES)] = silu(acc)
            return carry
        lax.fori_loop(0, conv_ch // LANES, conv, 0)

        row_id = lax.broadcasted_iota(jnp.int32, (CHUNK, CHUNK), 0)
        col_id = lax.broadcasted_iota(jnp.int32, (CHUNK, CHUNK), 1)
        lower = row_id >= col_id
        left = col_id < head_dim
        left_row = left[0:1, :]
        dt = softplus(dtp[...] + hp[layer, 0:1, :])
        a = -dt * jnp.exp(hp[layer, 1:2, :])
        a_cum = full_dot(jnp.where(lower, 1.0, 0.0).astype(F32), a)
        a_cum_t = a_cum.T
        a_last = a_cum[CHUNK - 1:CHUNK, :]
        from_start = jnp.exp(a_cum)
        to_end = jnp.exp(a_last - a_cum)
        whole = jnp.exp(a_last)
        skip = hp[layer, 2:3, :]
        b = act[:, width:width + n_state]
        c = act[:, width + n_state:conv_ch]
        c_dot_b = full_dot(c, b, (((1,), (1,)), ((), ())))
        b_t = b.T
        sq = jnp.zeros((CHUNK, LANES), F32)
        for p in range(width // LANES):
            cols = slice(p * LANES, (p + 1) * LANES)
            h0, h1 = 2 * p, 2 * p + 1

            def spread(m):
                return jnp.where(left, m[:, h0:h0 + 1], m[:, h1:h1 + 1])

            def spread_row(m):
                return jnp.where(left_row, m[:, h0:h0 + 1], m[:, h1:h1 + 1])

            def mixer(n):
                seg = a_cum[:, n:n + 1] - a_cum_t[n:n + 1, :]
                return jnp.where(lower, jnp.exp(jnp.minimum(seg, 0.0)), 0.0) * c_dot_b
            x = act[:, cols]
            x_dt = x * spread(dt)
            both = jnp.concatenate([jnp.where(left, x_dt, 0.0), jnp.where(left, 0.0, x_dt)], axis=0)
            y = full_dot(jnp.concatenate([mixer(h0), mixer(h1)], axis=1), both)
            s_in = state[:, cols]
            y = y + full_dot(c, s_in) * spread(from_start)
            state[:, cols] = s_in * spread_row(whole) + full_dot(b_t, x_dt * spread(to_end))
            y = y + spread_row(skip) * x
            gated = y * silu(pre[HALO:HALO + CHUNK, cols])
            v[:, cols] = gated
            sq = sq + gated * gated
        total = jnp.sum(sq.T, axis=0, keepdims=True)
        stats[slot, me] = jnp.broadcast_to(total, (8, CHUNK))
        for off in range(1, tp_size):
            msg_stat(t, off).start()

    def out_proj(t):
        slot = lax.rem(t, SLOTS)
        layer, row0 = where_of(t)

        @pl.when(row0 == 0)
        def _():
            load_out(layer).wait()
        for off in range(1, tp_size):
            peer = lax.rem(me + off, tp_size)
            pltpu.make_async_remote_copy(src_ref=stats.at[slot, peer], dst_ref=stats.at[slot, peer], send_sem=ssend.at[slot, off],
                                         recv_sem=srecv.at[slot, peer], device_id=dev_sib, device_id_type=MESH).wait_recv()
        for off in range(1, tp_size):
            msg_stat(t, off).wait_send()
        total = stats[slot, 0]
        for r in range(1, tp_size):
            total = total + stats[slot, r]
        scale = lax.rsqrt(total / inner_width + EPSILON)
        scale = jnp.broadcast_to(scale[0:1, :], (LANES, CHUNK)).T
        for p in range(width // LANES):
            cols = slice(p * LANES, (p + 1) * LANES)
            g[:, cols] = (v[:, cols] * scale * gw[layer, 0:1, cols]).astype(BF16)
        buf = pbuf.at[lax.rem(t, 2)]

        def tile(i, carry):
            o = pl.multiple_of(i * TILE, TILE)
            buf[:, pl.ds(o, TILE)] = jnp.dot(g[...], wout[layer, :, pl.ds(o, TILE)], preferred_element_type=F32)
            return carry
        lax.fori_loop(0, d_model // TILE, tile, 0)
        msg_rs(t, SIB).start()

    def pair_sum(t):
        msg_rs(t, SIB).wait_recv()
        buf, other = pbuf.at[lax.rem(t, 2)], sib.at[lax.rem(t, 2)]

        def block(i, carry):
            r = pl.multiple_of(i * 8, 8)
            mine = pl.ds(pl.multiple_of(core * half_rows + r, 8), 8)
            buf[mine, :] = buf[mine, :] + other[pl.ds(r, 8), :]
            return carry
        lax.fori_loop(0, half_rows // 8, block, 0)
        for kind in (FAR_P, FAR_M, NEAR_P, NEAR_M):
            msg_rs(t, kind).start()

    def relay_sum(t):
        slot = lax.rem(t, SLOTS)
        buf = pbuf.at[lax.rem(t, 2)]
        for way, (wait, send, j, part) in enumerate(((FAR_P, COMB_P, nxt, 1), (FAR_M, COMB_M, prv, 0))):
            msg_rs(t, wait).wait_recv()
            rows = pl.ds(pl.multiple_of(slice_at(core, j) + part * piece, piece), piece)
            buf[rows, :] = buf[rows, :] + far[slot, way]
            msg_rs(t, send).start()

    def finish(t):
        slot = lax.rem(t, SLOTS)
        layer, row0 = where_of(t)
        buf = pbuf.at[lax.rem(t, 2)]
        for kind in (NEAR_P, NEAR_M, COMB_P, COMB_M):
            msg_rs(t, kind).wait_recv()
        base = slice_at(core, chip)
        dst = pl.ds(pl.multiple_of(row0 + base, slice_rows), slice_rows)

        def store(res):
            lo = buf[pl.ds(base, piece), :] + near[slot, 0] + comb[slot, 1]
            hi = buf[pl.ds(pl.multiple_of(base + piece, piece), piece), :] + near[slot, 1] + comb[slot, 0]
            ures[layer, dst, :] = (res + jnp.concatenate([lo, hi], axis=0)).astype(BF16).astype(F32)

        @pl.when(layer == 0)
        def _():
            store(hid[dst, :].astype(F32))

        @pl.when(layer > 0)
        def _():
            store(ures[jnp.maximum(layer - 1, 0), dst, :])
        for kind in (AG_P, AG_M, D0):
            msg_ag(t, kind).start()
        for kind in (SIB, FAR_P, FAR_M, NEAR_P, NEAR_M, COMB_P, COMB_M):
            msg_rs(t, kind).wait_send()

    def forward(t):
        wait_ag(t, AG_P)
        msg_ag(t, FW_P).start()
        wait_ag(t, AG_M)
        msg_ag(t, FW_M).start()
        msg_ag(t, D1).start()
        msg_ag(t, D2).start()

    def collect(t):
        layer, row0 = where_of(t)
        wait_ag(t, FW_P)
        wait_ag(t, FW_M)
        msg_ag(t, D3).start()
        for kind in (D0, D1, D2, D3):
            wait_ag(t, kind)
        for kind in (AG_P, AG_M, FW_P, FW_M, D0, D1, D2, D3):
            msg_ag(t, kind).wait_send()

        @pl.when(layer == n_layers - 1)
        def _():
            def block(i, carry):
                rows = pl.ds(pl.multiple_of(row0 + i * 16, 16), 16)
                out[rows, :] = ures[layer, rows, :].astype(BF16)
                return carry
            lax.fori_loop(0, CHUNK // 16, block, 0)

    def guarded(step, t):
        @pl.when((t >= 0) & (t < n_tasks))
        def _():
            step(t)

    def iteration(t, carry):
        guarded(mix, t)
        guarded(pair_sum, t - 1)
        guarded(finish, t - 2)
        guarded(in_proj, t + 1)
        guarded(out_proj, t)
        guarded(relay_sum, t - 1)
        guarded(forward, t - 3)
        guarded(collect, t - 4)
        return carry
    lax.fori_loop(-1, n_tasks + 4, iteration, 0)


def layers(tp_size, hidden, norm_w, w_z, w_x, w_bc, w_dt, conv_x, conv_bc, bias_x, bias_bc, dt_bias, a_log, d_skip, gate_w, w_out):
    n_batch, n_steps, d_model = hidden.shape
    n_layers, conv_width, width = conv_x.shape
    head_rows = pl.cdiv(dt_bias.shape[-1], 16) * 16
    w_dt = jnp.transpose(w_dt, (2, 0, 1))
    state2 = w_bc.shape[-1]
    piece = CHUNK // tp_size // 2
    any_spec = pl.BlockSpec(memory_space=pl.ANY)
    dma = pltpu.SemaphoreType.DMA
    run = pl.pallas_call(
        functools.partial(kernel, tp_size, conv_width),
        out_shape=pltpu.VMEM((n_steps, d_model), BF16),
        in_specs=[any_spec] * 15,
        out_specs=pl.BlockSpec(memory_space=pltpu.VMEM),
        scratch_shapes=[pltpu.VMEM(p.shape, p.dtype) for p in (norm_w, w_dt, conv_x, conv_bc, bias_x, bias_bc, dt_bias, a_log, d_skip, gate_w)] + [
            pltpu.VMEM((n_steps, d_model), BF16),
            pltpu.VMEM((n_layers, d_model, 2 * width + state2), BF16),
            pltpu.VMEM((n_layers, head_rows, d_model), BF16),
            pltpu.VMEM((n_layers, head_rows, d_model), F32),
            pltpu.VMEM((n_layers, width, d_model), BF16),
            pltpu.VMEM((n_layers, n_steps, d_model), F32),
            pltpu.VMEM((CHUNK, d_model), BF16),
            pltpu.VMEM((HALO + CHUNK, 2 * width + state2), F32),
            pltpu.VMEM((CHUNK, width + state2), F32),
            pltpu.VMEM((CHUNK, width), F32),
            pltpu.VMEM((CHUNK, width), BF16),
            pltpu.VMEM((CHUNK, LANES), F32),
            pltpu.VMEM((state2 // 2, width), F32),
            pltpu.VMEM((2, CHUNK, d_model), F32),
            pltpu.VMEM((2, CHUNK // 2, d_model), F32),
            pltpu.VMEM((SLOTS, 2, piece, d_model), F32),
            pltpu.VMEM((SLOTS, 2, piece, d_model), F32),
            pltpu.VMEM((SLOTS, 2, piece, d_model), F32),
            pltpu.VMEM((SLOTS, tp_size, 8, CHUNK), F32),
            pltpu.VMEM((n_layers, 8, d_model), F32),
            pltpu.VMEM((n_layers, 8, width + state2), F32),
            pltpu.VMEM((n_layers, 8, width), F32),
            pltpu.VMEM((n_layers, 8, LANES), F32),
            dma((n_layers, (2 * width + state2) // TILE + 1)), dma((n_steps // CHUNK,)), dma((10,)),
            dma((SLOTS, tp_size)), dma((SLOTS, tp_size)), dma((SLOTS, 15)), dma((SLOTS, 15)),
        ],
        compiler_params=pltpu.CompilerParams(collective_id=0, has_side_effects=True, vmem_limit_bytes=62_000_000),
    )
    outs = [run(hidden[i], norm_w, w_z, w_x, w_bc, w_dt, conv_x, conv_bc, bias_x, bias_bc, dt_bias, a_log, d_skip, gate_w, w_out)
            for i in range(n_batch)]
    return jnp.stack(outs)


def solution(mesh):
    col_spec = P(None, None, 'tp')
    vec_spec = P(None, 'tp')
    in_specs = (P('dp'), P(), col_spec, col_spec, P(), col_spec, col_spec, P(), vec_spec, P(), vec_spec, vec_spec, vec_spec, vec_spec, P(None, 'tp', None))
    return jax.shard_map(functools.partial(layers, mesh.shape['tp']), mesh=mesh, in_specs=in_specs, out_specs=P('dp'), check_vma=False)
```

```python
import functools

import jax
import jax.numpy as jnp
from jax import lax
from jax.experimental import pallas as pl
from jax.experimental.pallas import tpu as pltpu
from jax.sharding import PartitionSpec as P

EPSILON = 1e-5
F32 = jnp.float32
BF16 = jnp.bfloat16
FULL = lax.Precision.HIGHEST
MESH = pl.DeviceIdType.MESH
LANES = 128
CHUNK = 128
SLOTS = 4
SEM_SLOTS = 6
HALO = 8
TILE = 256
(SIB, FAR_P, FAR_M, NEAR_P, NEAR_M, COMB_P, COMB_M, OWN_P1, OWN_P2, OWN_M1, OWN_M2, FW_P, FW_M, D0, D1, D2, D3) = range(17)


def full_dot(a, b, dims=(((1,), (0,)), ((), ()))):
    return lax.dot_general(a, b, dims, precision=FULL, preferred_element_type=F32)


def silu(a):
    return a * (1.0 / (1.0 + jnp.exp(-a)))


def softplus(a):
    return jnp.maximum(a, 0.0) + jnp.log1p(jnp.exp(-jnp.abs(a)))


def kernel(tp_size, conv_width, hid_hbm, norm_hbm, wz_hbm, wx_hbm, wbc_hbm, wdt_hbm, convx_hbm, convbc_hbm, biasx_hbm, biasbc_hbm,
           dtb_hbm, alog_hbm, dskip_hbm, gate_hbm, wout_hbm, out,
           norm_in, wdt_in, convx_in, convbc_in, biasx_in, biasbc_in, dtb_in, alog_in, dskip_in, gate_in,
           hid, win, wdt, wdt_f, wout, ures, h, pre, act, v, g, dtp, state, pbuf, sib, far, near, comb, stats, nw, cw, gw, hp,
           wsem, hsem, psem, ssend, srecv, msend, mrecv):
    n_layers, n_steps, d_model = ures.shape
    width = v.shape[1]
    conv_ch = act.shape[1]
    n_state = (conv_ch - width) // 2
    n_heads = dtb_in.shape[1]
    head_dim = width // n_heads
    n_chunks = n_steps // CHUNK
    n_tasks = n_layers * n_chunks
    n_chips = tp_size // 2
    n_tiles = pre.shape[1] // TILE
    half_rows = CHUNK // 2
    slice_rows = half_rows // n_chips
    piece = slice_rows // 2
    inner_width = width * tp_size

    me = lax.axis_index('tp')
    chip = me // 2
    core = lax.rem(me, 2)
    nxt = lax.rem(chip + 1, n_chips)
    prv = lax.rem(chip + n_chips - 1, n_chips)
    opp = lax.rem(chip + 2, n_chips)
    dev_nxt = {'tp': nxt * 2 + core}
    dev_prv = {'tp': prv * 2 + core}
    dev_sib = {'tp': chip * 2 + 1 - core}

    barrier = pltpu.get_barrier_semaphore()
    for off in range(1, tp_size):
        pl.semaphore_signal(barrier, inc=1, device_id={'tp': lax.rem(me + off, tp_size)}, device_id_type=MESH)

    def load_hid(i):
        rows = pl.ds(pl.multiple_of(i * CHUNK, CHUNK), CHUNK)
        return pltpu.make_async_copy(hid_hbm.at[rows], hid.at[rows], hsem.at[i])

    def load_in(layer):
        copies = []
        for w_hbm, first, n_cols in ((wz_hbm, 0, width), (wx_hbm, width, width), (wbc_hbm, 2 * width, 2 * n_state)):
            done = 0
            while done < n_cols:
                n = min(TILE - (first + done) % TILE, n_cols - done)
                at = first + done
                copies.append(pltpu.make_async_copy(w_hbm.at[layer, :, pl.ds(done, n)], win.at[layer, :, pl.ds(at, n)],
                                                    wsem.at[layer, at // TILE]))
                done += n
        return copies

    def wait_in(layer, tile):
        ref = win.at[layer, :, pl.ds(pl.multiple_of(tile * TILE, TILE), TILE)]
        pltpu.make_async_copy(ref, ref, wsem.at[layer, tile]).wait()

    def load_out(layer):
        return pltpu.make_async_copy(wout_hbm.at[layer], wout.at[layer], wsem.at[layer, n_tiles])

    params = ((norm_hbm, norm_in), (wdt_hbm, wdt_in), (convx_hbm, convx_in), (convbc_hbm, convbc_in), (biasx_hbm, biasx_in),
              (biasbc_hbm, biasbc_in), (dtb_hbm, dtb_in), (alog_hbm, alog_in), (dskip_hbm, dskip_in), (gate_hbm, gate_in))
    small = [pltpu.make_async_copy(src, dst, psem.at[i]) for i, (src, dst) in enumerate(params)]
    load_hid(0).start()
    for cp in small:
        cp.start()
    for cp in load_in(0):
        cp.start()
    for cp in small:
        cp.wait()

    hp[...] = jnp.zeros_like(hp)
    wdt_f[...] = jnp.zeros_like(wdt_f)
    for n in range(n_heads):
        cols = wdt_in[n].astype(F32)
        for layer in range(n_layers):
            wdt_f[layer, n:n + 1, :] = cols[layer:layer + 1, :]
    wdt[...] = wdt_f[...].astype(BF16)
    dtp[...] = jnp.zeros_like(dtp)
    for layer in range(n_layers):
        nw[layer, 0:1, :] = norm_in[layer:layer + 1, :].astype(F32)
        gw[layer, 0:1, :] = gate_in[layer:layer + 1, :].astype(F32)
        cw[layer, 0:conv_width, 0:width] = convx_in[layer].astype(F32)
        cw[layer, 0:conv_width, width:conv_ch] = convbc_in[layer].astype(F32)
        cw[layer, conv_width:conv_width + 1, 0:width] = biasx_in[layer:layer + 1, :].astype(F32)
        cw[layer, conv_width:conv_width + 1, width:conv_ch] = biasbc_in[layer:layer + 1, :].astype(F32)
        hp[layer, 0:1, 0:n_heads] = dtb_in[layer:layer + 1, :]
        hp[layer, 1:2, 0:n_heads] = alog_in[layer:layer + 1, :]
        hp[layer, 2:3, 0:n_heads] = dskip_in[layer:layer + 1, :]

    pl.semaphore_wait(barrier, tp_size - 1)

    def where_of(t):
        layer = t // n_chunks
        return layer, pl.multiple_of((t - layer * n_chunks) * CHUNK, CHUNK)

    def remote(src, dst, t, kind, dev):
        slot = lax.rem(t, SEM_SLOTS)
        return pltpu.make_async_remote_copy(src_ref=src, dst_ref=dst, send_sem=msend.at[slot, kind], recv_sem=mrecv.at[slot, kind],
                                            device_id=dev, device_id_type=MESH)

    def slice_at(c, j):
        return pl.multiple_of(c * half_rows + j * slice_rows, slice_rows)

    def msg_rs(t, kind):
        slot = lax.rem(t, SLOTS)
        buf = pbuf.at[lax.rem(t, 2)]

        def src(j, part):
            return buf.at[pl.ds(pl.multiple_of(slice_at(core, j) + part * piece, piece), piece)]
        if kind == SIB:
            other = pl.multiple_of((1 - core) * half_rows, half_rows)
            return remote(buf.at[pl.ds(other, half_rows)], sib.at[lax.rem(t, 2)], t, kind, dev_sib)
        if kind == FAR_P:
            return remote(src(opp, 1), far.at[slot, 0], t, kind, dev_nxt)
        if kind == FAR_M:
            return remote(src(opp, 0), far.at[slot, 1], t, kind, dev_prv)
        if kind == NEAR_P:
            return remote(src(nxt, 0), near.at[slot, 0], t, kind, dev_nxt)
        if kind == NEAR_M:
            return remote(src(prv, 1), near.at[slot, 1], t, kind, dev_prv)
        if kind == COMB_P:
            return remote(src(nxt, 1), comb.at[slot, 0], t, kind, dev_nxt)
        return remote(src(prv, 0), comb.at[slot, 1], t, kind, dev_prv)

    def ag_rows(t, c, j, part=None):
        layer, row0 = where_of(t)
        base = row0 + slice_at(c, j)
        if part is None:
            return ures.at[layer, pl.ds(pl.multiple_of(base, slice_rows), slice_rows)]
        return ures.at[layer, pl.ds(pl.multiple_of(base + part * piece, piece), piece)]

    ag_sent = {OWN_P1: (chip, 0, dev_nxt), OWN_P2: (chip, 1, dev_nxt), OWN_M1: (chip, 1, dev_prv), OWN_M2: (chip, 0, dev_prv),
               FW_P: (prv, 0, dev_nxt), FW_M: (nxt, 1, dev_prv),
               D0: (chip, None, dev_sib), D1: (prv, None, dev_sib), D2: (nxt, None, dev_sib), D3: (opp, None, dev_sib)}
    ag_got = {OWN_P1: (core, prv, 0), OWN_P2: (core, prv, 1), OWN_M1: (core, nxt, 1), OWN_M2: (core, nxt, 0),
              FW_P: (core, opp, 0), FW_M: (core, opp, 1),
              D0: (1 - core, chip, None), D1: (1 - core, prv, None), D2: (1 - core, nxt, None), D3: (1 - core, opp, None)}

    def msg_ag(t, kind):
        j, part, dev = ag_sent[kind]
        ref = ag_rows(t, core, j, part)
        return remote(ref, ref, t, kind, dev)

    def wait_ag(t, kind):
        ref = ag_rows(t, *ag_got[kind])
        remote(ref, ref, t, kind, dev_sib).wait_recv()

    def msg_stat(t, off):
        slot = lax.rem(t, SLOTS)
        return pltpu.make_async_remote_copy(src_ref=stats.at[slot, me], dst_ref=stats.at[slot, me], send_sem=ssend.at[slot, off],
                                            recv_sem=srecv.at[slot, me], device_id={'tp': lax.rem(me + off, tp_size)}, device_id_type=MESH)

    def in_proj(t):
        layer, row0 = where_of(t)

        @pl.when(layer == 0)
        def _():
            load_hid(t).wait()

        @pl.when(row0 == 0)
        def _():
            pre[0:HALO, :] = jnp.zeros((HALO, pre.shape[1]), F32)

        @pl.when(row0 > 0)
        def _():
            pre[0:HALO, :] = pre[CHUNK:CHUNK + HALO, :]

        def norm(load):
            def block(i, carry):
                r = pl.multiple_of(i * 16, 16)
                u = load(pl.multiple_of(row0 + r, 16))
                scale = lax.rsqrt(jnp.mean(u * u, axis=-1, keepdims=True) + EPSILON)
                h[pl.ds(r, 16), :] = (u * scale * nw[layer, 0:1, :]).astype(BF16)
                return carry
            lax.fori_loop(0, CHUNK // 16, block, 0)

        @pl.when(layer == 0)
        def _():
            norm(lambda r: hid[pl.ds(r, 16), :].astype(F32))

        @pl.when(layer > 0)
        def _():
            norm(lambda r: ures[jnp.maximum(layer - 1, 0), pl.ds(r, 16), :])

        def tile(i, carry):
            @pl.when(row0 == 0)
            def _():
                wait_in(layer, i)
            o = pl.multiple_of(i * TILE, TILE)
            prod = jnp.dot(h[...], win[layer, :, pl.ds(o, TILE)], preferred_element_type=F32)
            pre[HALO:HALO + CHUNK, pl.ds(o, TILE)] = prod.astype(BF16).astype(F32)
            return carry
        lax.fori_loop(0, pre.shape[1] // TILE, tile, 0)
        prod = lax.dot_general(h[...], wdt[layer], (((1,), (1,)), ((), ())), preferred_element_type=F32)
        dtp[:, 0:wdt.shape[1]] = prod.astype(BF16).astype(F32)

        @pl.when(t == 0)
        def _():
            load_out(0).start()
            for i in range(1, n_chunks):
                load_hid(i).start()

        @pl.when((row0 == CHUNK) & (layer < n_layers - 1))
        def _():
            for k in range(1, n_layers):
                @pl.when(layer == k - 1)
                def _():
                    for cp in load_in(k):
                        cp.start()
                    load_out(k).start()

    def mix(t):
        slot = lax.rem(t, SLOTS)
        layer, row0 = where_of(t)

        @pl.when(row0 == 0)
        def _():
            state[...] = jnp.zeros_like(state)

        def conv(i, carry):
            o = pl.multiple_of(i * LANES, LANES)
            acc = jnp.broadcast_to(cw[layer, conv_width:conv_width + 1, pl.ds(o, LANES)], (CHUNK, LANES))
            for j in range(conv_width):
                first = HALO - (conv_width - 1) + j
                acc = acc + pre[first:first + CHUNK, pl.ds(pl.multiple_of(width + o, LANES), LANES)] * cw[layer, j:j + 1, pl.ds(o, LANES)]
            act[:, pl.ds(o, LANES)] = silu(acc)
            return carry
        lax.fori_loop(0, conv_ch // LANES, conv, 0)

        row_id = lax.broadcasted_iota(jnp.int32, (CHUNK, CHUNK), 0)
        col_id = lax.broadcasted_iota(jnp.int32, (CHUNK, CHUNK), 1)
        lower = row_id >= col_id
        left = col_id < head_dim
        left_row = left[0:1, :]
        dt = softplus(dtp[...] + hp[layer, 0:1, :])
        a = -dt * jnp.exp(hp[layer, 1:2, :])
        a_cum = full_dot(jnp.where(lower, 1.0, 0.0).astype(F32), a)
        a_cum_t = a_cum.T
        a_last = a_cum[CHUNK - 1:CHUNK, :]
        from_start = jnp.exp(a_cum)
        to_end = jnp.exp(a_last - a_cum)
        whole = jnp.exp(a_last)
        skip = hp[layer, 2:3, :]
        b = act[:, width:width + n_state]
        c = act[:, width + n_state:conv_ch]
        c_dot_b = full_dot(c, b, (((1,), (1,)), ((), ())))
        b_t = b.T
        sq = jnp.zeros((CHUNK, LANES), F32)
        for p in range(width // LANES):
            cols = slice(p * LANES, (p + 1) * LANES)
            h0, h1 = 2 * p, 2 * p + 1

            def spread(m):
                return jnp.where(left, m[:, h0:h0 + 1], m[:, h1:h1 + 1])

            def spread_row(m):
                return jnp.where(left_row, m[:, h0:h0 + 1], m[:, h1:h1 + 1])

            def mixer(n):
                seg = a_cum[:, n:n + 1] - a_cum_t[n:n + 1, :]
                return jnp.where(lower, jnp.exp(jnp.minimum(seg, 0.0)), 0.0) * c_dot_b
            x = act[:, cols]
            x_dt = x * spread(dt)
            both = jnp.concatenate([jnp.where(left, x_dt, 0.0), jnp.where(left, 0.0, x_dt)], axis=0)
            y = full_dot(jnp.concatenate([mixer(h0), mixer(h1)], axis=1), both)
            s_in = state[:, cols]
            y = y + full_dot(c, s_in) * spread(from_start)
            state[:, cols] = s_in * spread_row(whole) + full_dot(b_t, x_dt * spread(to_end))
            y = y + spread_row(skip) * x
            gated = y * silu(pre[HALO:HALO + CHUNK, cols])
            v[:, cols] = gated
            sq = sq + gated * gated
        total = jnp.sum(sq.T, axis=0, keepdims=True)
        stats[slot, me] = jnp.broadcast_to(total, (8, CHUNK))
        for off in range(1, tp_size):
            msg_stat(t, off).start()

    def out_proj(t):
        slot = lax.rem(t, SLOTS)
        layer, row0 = where_of(t)

        @pl.when(row0 == 0)
        def _():
            load_out(layer).wait()
        for off in range(1, tp_size):
            peer = lax.rem(me + off, tp_size)
            pltpu.make_async_remote_copy(src_ref=stats.at[slot, peer], dst_ref=stats.at[slot, peer], send_sem=ssend.at[slot, off],
                                         recv_sem=srecv.at[slot, peer], device_id=dev_sib, device_id_type=MESH).wait_recv()
        for off in range(1, tp_size):
            msg_stat(t, off).wait_send()
        total = stats[slot, 0]
        for r in range(1, tp_size):
            total = total + stats[slot, r]
        scale = lax.rsqrt(total / inner_width + EPSILON)
        scale = jnp.broadcast_to(scale[0:1, :], (LANES, CHUNK)).T
        for p in range(width // LANES):
            cols = slice(p * LANES, (p + 1) * LANES)
            g[:, cols] = (v[:, cols] * scale * gw[layer, 0:1, cols]).astype(BF16)
        buf = pbuf.at[lax.rem(t, 2)]

        def tile(i, carry):
            o = pl.multiple_of(i * TILE, TILE)
            buf[:, pl.ds(o, TILE)] = jnp.dot(g[...], wout[layer, :, pl.ds(o, TILE)], preferred_element_type=F32)
            return carry
        lax.fori_loop(0, d_model // TILE, tile, 0)
        msg_rs(t, SIB).start()

    def pair_sum(t):
        msg_rs(t, SIB).wait_recv()
        buf, other = pbuf.at[lax.rem(t, 2)], sib.at[lax.rem(t, 2)]

        def block(i, carry):
            r = pl.multiple_of(i * 8, 8)
            mine = pl.ds(pl.multiple_of(core * half_rows + r, 8), 8)
            buf[mine, :] = buf[mine, :] + other[pl.ds(r, 8), :]
            return carry
        lax.fori_loop(0, half_rows // 8, block, 0)
        for kind in (FAR_P, FAR_M, NEAR_P, NEAR_M):
            msg_rs(t, kind).start()

    def relay_sum(t):
        slot = lax.rem(t, SLOTS)
        buf = pbuf.at[lax.rem(t, 2)]
        for way, (wait, send, j, part) in enumerate(((FAR_P, COMB_P, nxt, 1), (FAR_M, COMB_M, prv, 0))):
            msg_rs(t, wait).wait_recv()
            rows = pl.ds(pl.multiple_of(slice_at(core, j) + part * piece, piece), piece)
            buf[rows, :] = buf[rows, :] + far[slot, way]
            msg_rs(t, send).start()

    def finish(t):
        slot = lax.rem(t, SLOTS)
        layer, row0 = where_of(t)
        buf = pbuf.at[lax.rem(t, 2)]
        for kind in (NEAR_P, NEAR_M, COMB_P, COMB_M):
            msg_rs(t, kind).wait_recv()
        base = slice_at(core, chip)
        dst = pl.ds(pl.multiple_of(row0 + base, slice_rows), slice_rows)

        def store(res):
            lo = buf[pl.ds(base, piece), :] + near[slot, 0] + comb[slot, 1]
            hi = buf[pl.ds(pl.multiple_of(base + piece, piece), piece), :] + near[slot, 1] + comb[slot, 0]
            ures[layer, dst, :] = (res + jnp.concatenate([lo, hi], axis=0)).astype(BF16).astype(F32)

        @pl.when(layer == 0)
        def _():
            store(hid[dst, :].astype(F32))

        @pl.when(layer > 0)
        def _():
            store(ures[jnp.maximum(layer - 1, 0), dst, :])
        for kind in (OWN_P1, OWN_M1, OWN_P2, OWN_M2, D0):
            msg_ag(t, kind).start()
        for kind in (SIB, FAR_P, FAR_M, NEAR_P, NEAR_M, COMB_P, COMB_M):
            msg_rs(t, kind).wait_send()

    def forward(t):
        for wait, send in ((OWN_P1, FW_P), (OWN_M1, FW_M)):
            wait_ag(t, wait)
            msg_ag(t, send).start()

    def share(t):
        for waits, send in (((OWN_P2,), D1), ((OWN_M2,), D2), ((FW_P, FW_M), D3)):
            for kind in waits:
                wait_ag(t, kind)
            msg_ag(t, send).start()

    def collect(t):
        layer, row0 = where_of(t)
        for kind in (D0, D1, D2, D3):
            wait_ag(t, kind)
        for kind in ag_sent:
            msg_ag(t, kind).wait_send()

        @pl.when(layer == n_layers - 1)
        def _():
            def block(i, carry):
                rows = pl.ds(pl.multiple_of(row0 + i * 16, 16), 16)
                out[rows, :] = ures[layer, rows, :].astype(BF16)
                return carry
            lax.fori_loop(0, CHUNK // 16, block, 0)

    def guarded(step, t):
        @pl.when((t >= 0) & (t < n_tasks))
        def _():
            step(t)

    def iteration(t, carry):
        guarded(mix, t)
        guarded(collect, t - 5)
        guarded(pair_sum, t - 1)
        guarded(in_proj, t + 1)
        guarded(finish, t - 2)
        guarded(out_proj, t)
        guarded(relay_sum, t - 1)
        guarded(forward, t - 3)
        guarded(share, t - 4)
        return carry
    lax.fori_loop(-1, n_tasks + 5, iteration, 0)


def layers(tp_size, hidden, norm_w, w_z, w_x, w_bc, w_dt, conv_x, conv_bc, bias_x, bias_bc, dt_bias, a_log, d_skip, gate_w, w_out):
    n_batch, n_steps, d_model = hidden.shape
    n_layers, conv_width, width = conv_x.shape
    head_rows = pl.cdiv(dt_bias.shape[-1], 16) * 16
    w_dt = jnp.transpose(w_dt, (2, 0, 1))
    state2 = w_bc.shape[-1]
    piece = CHUNK // tp_size // 2
    any_spec = pl.BlockSpec(memory_space=pl.ANY)
    dma = pltpu.SemaphoreType.DMA
    run = pl.pallas_call(
        functools.partial(kernel, tp_size, conv_width),
        out_shape=pltpu.VMEM((n_steps, d_model), BF16),
        in_specs=[any_spec] * 15,
        out_specs=pl.BlockSpec(memory_space=pltpu.VMEM),
        scratch_shapes=[pltpu.VMEM(p.shape, p.dtype) for p in (norm_w, w_dt, conv_x, conv_bc, bias_x, bias_bc, dt_bias, a_log, d_skip, gate_w)] + [
            pltpu.VMEM((n_steps, d_model), BF16),
            pltpu.VMEM((n_layers, d_model, 2 * width + state2), BF16),
            pltpu.VMEM((n_layers, head_rows, d_model), BF16),
            pltpu.VMEM((n_layers, head_rows, d_model), F32),
            pltpu.VMEM((n_layers, width, d_model), BF16),
            pltpu.VMEM((n_layers, n_steps, d_model), F32),
            pltpu.VMEM((CHUNK, d_model), BF16),
            pltpu.VMEM((HALO + CHUNK, 2 * width + state2), F32),
            pltpu.VMEM((CHUNK, width + state2), F32),
            pltpu.VMEM((CHUNK, width), F32),
            pltpu.VMEM((CHUNK, width), BF16),
            pltpu.VMEM((CHUNK, LANES), F32),
            pltpu.VMEM((state2 // 2, width), F32),
            pltpu.VMEM((2, CHUNK, d_model), F32),
            pltpu.VMEM((2, CHUNK // 2, d_model), F32),
            pltpu.VMEM((SLOTS, 2, piece, d_model), F32),
            pltpu.VMEM((SLOTS, 2, piece, d_model), F32),
            pltpu.VMEM((SLOTS, 2, piece, d_model), F32),
            pltpu.VMEM((SLOTS, tp_size, 8, CHUNK), F32),
            pltpu.VMEM((n_layers, 8, d_model), F32),
            pltpu.VMEM((n_layers, 8, width + state2), F32),
            pltpu.VMEM((n_layers, 8, width), F32),
            pltpu.VMEM((n_layers, 8, LANES), F32),
            dma((n_layers, (2 * width + state2) // TILE + 1)), dma((n_steps // CHUNK,)), dma((10,)),
            dma((SLOTS, tp_size)), dma((SLOTS, tp_size)), dma((SEM_SLOTS, 17)), dma((SEM_SLOTS, 17)),
        ],
        compiler_params=pltpu.CompilerParams(collective_id=0, has_side_effects=True, vmem_limit_bytes=62_000_000),
    )
    outs = [run(hidden[i], norm_w, w_z, w_x, w_bc, w_dt, conv_x, conv_bc, bias_x, bias_bc, dt_bias, a_log, d_skip, gate_w, w_out)
            for i in range(n_batch)]
    return jnp.stack(outs)


def solution(mesh):
    col_spec = P(None, None, 'tp')
    vec_spec = P(None, 'tp')
    in_specs = (P('dp'), P(), col_spec, col_spec, P(), col_spec, col_spec, P(), vec_spec, P(), vec_spec, vec_spec, vec_spec, vec_spec, P(None, 'tp', None))
    return jax.shard_map(functools.partial(layers, mesh.shape['tp']), mesh=mesh, in_specs=in_specs, out_specs=P('dp'), check_vma=False)
```

```python
import functools

import jax
import jax.numpy as jnp
from jax import lax
from jax.experimental import pallas as pl
from jax.experimental.pallas import tpu as pltpu
from jax.sharding import PartitionSpec as P

EPSILON = 1e-5
F32 = jnp.float32
BF16 = jnp.bfloat16
MESH = pl.DeviceIdType.MESH
LANES = 128
CHUNK = 128
SLOTS = 4
SEM_SLOTS = 6
HALO = 8
TILE = 256
(SIB, FAR_P, FAR_M, NEAR_P, NEAR_M, COMB_P, COMB_M, OWN_P1, OWN_P2, OWN_M1, OWN_M2, FW_P, FW_M, D0, D1, D2, D3) = range(17)


def fast_dot(a, b, dims=(((1,), (0,)), ((), ()))):
    return lax.dot_general(a, b, dims, preferred_element_type=F32)


def split(m):
    hi = m.astype(BF16)
    rest = m - hi.astype(F32)
    mid = rest.astype(BF16)
    return hi, mid, (rest - mid.astype(F32)).astype(BF16)


def left_parts(m):
    hi, mid, lo = split(m)
    return jnp.concatenate([hi, hi], axis=1), jnp.concatenate([mid, mid], axis=1), jnp.concatenate([lo, hi], axis=1)


def three_dots(p1, p2, p3, parts, cols):
    n = parts.shape[0] // 3
    upper = parts[0:2 * n, cols]
    return (fast_dot(p3, parts[n:3 * n, cols]) + fast_dot(p2, upper)) + fast_dot(p1, upper)


def silu(a):
    return a * (1.0 / (1.0 + jnp.exp(-a)))


def softplus(a):
    return jnp.maximum(a, 0.0) + jnp.log1p(jnp.exp(-jnp.abs(a)))


def kernel(tp_size, conv_width, hid_hbm, norm_hbm, wz_hbm, wx_hbm, wbc_hbm, wdt_hbm, convx_hbm, convbc_hbm, biasx_hbm, biasbc_hbm,
           dtb_hbm, alog_hbm, dskip_hbm, gate_hbm, wout_hbm, out,
           norm_in, wdt_in, convx_in, convbc_in, biasx_in, biasbc_in, dtb_in, alog_in, dskip_in, gate_in,
           hid, win, wdt, wdt_f, wout, ures, h, pre, act, v, g, dtp, state, state3, weighted3, pbuf, sib, far, near, comb, stats, nw, cw, gw, hp,
           wsem, hsem, psem, ssend, srecv, msend, mrecv):
    n_layers, n_steps, d_model = ures.shape
    width = v.shape[1]
    conv_ch = act.shape[1]
    n_state = (conv_ch - width) // 2
    n_heads = dtb_in.shape[1]
    head_dim = width // n_heads
    n_chunks = n_steps // CHUNK
    n_tasks = n_layers * n_chunks
    n_chips = tp_size // 2
    n_tiles = pre.shape[1] // TILE
    half_rows = CHUNK // 2
    slice_rows = half_rows // n_chips
    piece = slice_rows // 2
    inner_width = width * tp_size

    me = lax.axis_index('tp')
    chip = me // 2
    core = lax.rem(me, 2)
    nxt = lax.rem(chip + 1, n_chips)
    prv = lax.rem(chip + n_chips - 1, n_chips)
    opp = lax.rem(chip + 2, n_chips)
    dev_nxt = {'tp': nxt * 2 + core}
    dev_prv = {'tp': prv * 2 + core}
    dev_sib = {'tp': chip * 2 + 1 - core}

    barrier = pltpu.get_barrier_semaphore()
    for off in range(1, tp_size):
        pl.semaphore_signal(barrier, inc=1, device_id={'tp': lax.rem(me + off, tp_size)}, device_id_type=MESH)

    def load_hid(i):
        rows = pl.ds(pl.multiple_of(i * CHUNK, CHUNK), CHUNK)
        return pltpu.make_async_copy(hid_hbm.at[rows], hid.at[rows], hsem.at[i])

    def load_in(layer):
        copies = []
        for w_hbm, first, n_cols in ((wz_hbm, 0, width), (wx_hbm, width, width), (wbc_hbm, 2 * width, 2 * n_state)):
            done = 0
            while done < n_cols:
                n = min(TILE - (first + done) % TILE, n_cols - done)
                at = first + done
                copies.append(pltpu.make_async_copy(w_hbm.at[layer, :, pl.ds(done, n)], win.at[layer, :, pl.ds(at, n)],
                                                    wsem.at[layer, at // TILE]))
                done += n
        return copies

    def wait_in(layer, tile):
        ref = win.at[layer, :, pl.ds(pl.multiple_of(tile * TILE, TILE), TILE)]
        pltpu.make_async_copy(ref, ref, wsem.at[layer, tile]).wait()

    def load_out(layer):
        return pltpu.make_async_copy(wout_hbm.at[layer], wout.at[layer], wsem.at[layer, n_tiles])

    params = ((norm_hbm, norm_in), (wdt_hbm, wdt_in), (convx_hbm, convx_in), (convbc_hbm, convbc_in), (biasx_hbm, biasx_in),
              (biasbc_hbm, biasbc_in), (dtb_hbm, dtb_in), (alog_hbm, alog_in), (dskip_hbm, dskip_in), (gate_hbm, gate_in))
    small = [pltpu.make_async_copy(src, dst, psem.at[i]) for i, (src, dst) in enumerate(params)]
    load_hid(0).start()
    for cp in small:
        cp.start()
    for cp in load_in(0):
        cp.start()
    for cp in small:
        cp.wait()

    hp[...] = jnp.zeros_like(hp)
    wdt_f[...] = jnp.zeros_like(wdt_f)
    for n in range(n_heads):
        cols = wdt_in[n].astype(F32)
        for layer in range(n_layers):
            wdt_f[layer, n:n + 1, :] = cols[layer:layer + 1, :]
    wdt[...] = wdt_f[...].astype(BF16)
    dtp[...] = jnp.zeros_like(dtp)
    for layer in range(n_layers):
        nw[layer, 0:1, :] = norm_in[layer:layer + 1, :].astype(F32)
        gw[layer, 0:1, :] = gate_in[layer:layer + 1, :].astype(F32)
        cw[layer, 0:conv_width, 0:width] = convx_in[layer].astype(F32)
        cw[layer, 0:conv_width, width:conv_ch] = convbc_in[layer].astype(F32)
        cw[layer, conv_width:conv_width + 1, 0:width] = biasx_in[layer:layer + 1, :].astype(F32)
        cw[layer, conv_width:conv_width + 1, width:conv_ch] = biasbc_in[layer:layer + 1, :].astype(F32)
        hp[layer, 0:1, 0:n_heads] = dtb_in[layer:layer + 1, :]
        hp[layer, 1:2, 0:n_heads] = alog_in[layer:layer + 1, :]
        hp[layer, 2:3, 0:n_heads] = dskip_in[layer:layer + 1, :]

    pl.semaphore_wait(barrier, tp_size - 1)

    def where_of(t):
        layer = t // n_chunks
        return layer, pl.multiple_of((t - layer * n_chunks) * CHUNK, CHUNK)

    def remote(src, dst, t, kind, dev):
        slot = lax.rem(t, SEM_SLOTS)
        return pltpu.make_async_remote_copy(src_ref=src, dst_ref=dst, send_sem=msend.at[slot, kind], recv_sem=mrecv.at[slot, kind],
                                            device_id=dev, device_id_type=MESH)

    def slice_at(c, j):
        return pl.multiple_of(c * half_rows + j * slice_rows, slice_rows)

    def msg_rs(t, kind):
        slot = lax.rem(t, SLOTS)
        buf = pbuf.at[lax.rem(t, 2)]

        def src(j, part):
            return buf.at[pl.ds(pl.multiple_of(slice_at(core, j) + part * piece, piece), piece)]
        if kind == SIB:
            other = pl.multiple_of((1 - core) * half_rows, half_rows)
            return remote(buf.at[pl.ds(other, half_rows)], sib.at[lax.rem(t, 2)], t, kind, dev_sib)
        if kind == FAR_P:
            return remote(src(opp, 1), far.at[slot, 0], t, kind, dev_nxt)
        if kind == FAR_M:
            return remote(src(opp, 0), far.at[slot, 1], t, kind, dev_prv)
        if kind == NEAR_P:
            return remote(src(nxt, 0), near.at[slot, 0], t, kind, dev_nxt)
        if kind == NEAR_M:
            return remote(src(prv, 1), near.at[slot, 1], t, kind, dev_prv)
        if kind == COMB_P:
            return remote(src(nxt, 1), comb.at[slot, 0], t, kind, dev_nxt)
        return remote(src(prv, 0), comb.at[slot, 1], t, kind, dev_prv)

    def ag_rows(t, c, j, part=None):
        layer, row0 = where_of(t)
        base = row0 + slice_at(c, j)
        if part is None:
            return ures.at[layer, pl.ds(pl.multiple_of(base, slice_rows), slice_rows)]
        return ures.at[layer, pl.ds(pl.multiple_of(base + part * piece, piece), piece)]

    ag_sent = {OWN_P1: (chip, 0, dev_nxt), OWN_P2: (chip, 1, dev_nxt), OWN_M1: (chip, 1, dev_prv), OWN_M2: (chip, 0, dev_prv),
               FW_P: (prv, 0, dev_nxt), FW_M: (nxt, 1, dev_prv),
               D0: (chip, None, dev_sib), D1: (prv, None, dev_sib), D2: (nxt, None, dev_sib), D3: (opp, None, dev_sib)}
    ag_got = {OWN_P1: (core, prv, 0), OWN_P2: (core, prv, 1), OWN_M1: (core, nxt, 1), OWN_M2: (core, nxt, 0),
              FW_P: (core, opp, 0), FW_M: (core, opp, 1),
              D0: (1 - core, chip, None), D1: (1 - core, prv, None), D2: (1 - core, nxt, None), D3: (1 - core, opp, None)}

    def msg_ag(t, kind):
        j, part, dev = ag_sent[kind]
        ref = ag_rows(t, core, j, part)
        return remote(ref, ref, t, kind, dev)

    def wait_ag(t, kind):
        ref = ag_rows(t, *ag_got[kind])
        remote(ref, ref, t, kind, dev_sib).wait_recv()

    def msg_stat(t, off):
        slot = lax.rem(t, SLOTS)
        return pltpu.make_async_remote_copy(src_ref=stats.at[slot, me], dst_ref=stats.at[slot, me], send_sem=ssend.at[slot, off],
                                            recv_sem=srecv.at[slot, me], device_id={'tp': lax.rem(me + off, tp_size)}, device_id_type=MESH)

    def in_proj(t):
        layer, row0 = where_of(t)

        @pl.when(layer == 0)
        def _():
            load_hid(t).wait()

        @pl.when(row0 == 0)
        def _():
            pre[0:HALO, :] = jnp.zeros((HALO, pre.shape[1]), F32)

        @pl.when(row0 > 0)
        def _():
            pre[0:HALO, :] = pre[CHUNK:CHUNK + HALO, :]

        def norm(load):
            def block(i, carry):
                r = pl.multiple_of(i * 16, 16)
                u = load(pl.multiple_of(row0 + r, 16))
                scale = lax.rsqrt(jnp.mean(u * u, axis=-1, keepdims=True) + EPSILON)
                h[pl.ds(r, 16), :] = (u * scale * nw[layer, 0:1, :]).astype(BF16)
                return carry
            lax.fori_loop(0, CHUNK // 16, block, 0)

        @pl.when(layer == 0)
        def _():
            norm(lambda r: hid[pl.ds(r, 16), :].astype(F32))

        @pl.when(layer > 0)
        def _():
            norm(lambda r: ures[jnp.maximum(layer - 1, 0), pl.ds(r, 16), :])

        def tile(i, carry):
            @pl.when(row0 == 0)
            def _():
                wait_in(layer, i)
            o = pl.multiple_of(i * TILE, TILE)
            prod = jnp.dot(h[...], win[layer, :, pl.ds(o, TILE)], preferred_element_type=F32)
            pre[HALO:HALO + CHUNK, pl.ds(o, TILE)] = prod.astype(BF16).astype(F32)
            return carry
        lax.fori_loop(0, pre.shape[1] // TILE, tile, 0)
        prod = lax.dot_general(h[...], wdt[layer], (((1,), (1,)), ((), ())), preferred_element_type=F32)
        dtp[:, 0:wdt.shape[1]] = prod.astype(BF16).astype(F32)

        @pl.when(t == 0)
        def _():
            load_out(0).start()
            for i in range(1, n_chunks):
                load_hid(i).start()

        @pl.when((row0 == CHUNK) & (layer < n_layers - 1))
        def _():
            for k in range(1, n_layers):
                @pl.when(layer == k - 1)
                def _():
                    for cp in load_in(k):
                        cp.start()
                    load_out(k).start()

    def mix(t):
        slot = lax.rem(t, SLOTS)
        layer, row0 = where_of(t)

        @pl.when(row0 == 0)
        def _():
            state[...] = jnp.zeros_like(state)
            state3[...] = jnp.zeros_like(state3)

        def conv(i, carry):
            o = pl.multiple_of(i * LANES, LANES)
            acc = jnp.broadcast_to(cw[layer, conv_width:conv_width + 1, pl.ds(o, LANES)], (CHUNK, LANES))
            for j in range(conv_width):
                first = HALO - (conv_width - 1) + j
                acc = acc + pre[first:first + CHUNK, pl.ds(pl.multiple_of(width + o, LANES), LANES)] * cw[layer, j:j + 1, pl.ds(o, LANES)]
            act[:, pl.ds(o, LANES)] = silu(acc)
            return carry
        lax.fori_loop(0, conv_ch // LANES, conv, 0)

        row_id = lax.broadcasted_iota(jnp.int32, (CHUNK, CHUNK), 0)
        col_id = lax.broadcasted_iota(jnp.int32, (CHUNK, CHUNK), 1)
        lower = row_id >= col_id
        left = col_id < head_dim
        left_row = left[0:1, :]
        dt = softplus(dtp[...] + hp[layer, 0:1, :])
        a = -dt * jnp.exp(hp[layer, 1:2, :])
        ones = jnp.where(lower, 1.0, 0.0).astype(BF16)
        a_cum = sum(fast_dot(ones, part) for part in reversed(split(a)))
        a_cum_t = a_cum.T
        a_last = a_cum[CHUNK - 1:CHUNK, :]
        from_start = jnp.exp(a_cum)
        to_end = jnp.exp(a_last - a_cum)
        whole = jnp.exp(a_last)
        skip = hp[layer, 2:3, :]
        b = act[:, width:width + n_state]
        c1, c2, c3 = left_parts(act[:, width + n_state:conv_ch])
        bh, bm, bl = split(b)
        nt = (((1,), (1,)), ((), ()))
        b_mh = jnp.concatenate([bm, bh], axis=1)
        c_dot_b = (fast_dot(c3, jnp.concatenate([bh, bl], axis=1), nt) + fast_dot(c2, b_mh, nt)) + fast_dot(c1, b_mh, nt)
        c_dot_b = jnp.where(lower, c_dot_b, 0.0)
        b1, b2, b3 = left_parts(b.T)
        for o in range(0, width, TILE):
            cols = slice(o, min(o + TILE, width))
            v[:, cols] = three_dots(c1, c2, c3, state3, cols)
        sq = jnp.zeros((CHUNK, LANES), F32)
        for p in range(width // LANES):
            cols = slice(p * LANES, (p + 1) * LANES)
            h0, h1 = 2 * p, 2 * p + 1

            def spread(m):
                return jnp.where(left, m[:, h0:h0 + 1], m[:, h1:h1 + 1])

            def spread_row(m):
                return jnp.where(left_row, m[:, h0:h0 + 1], m[:, h1:h1 + 1])

            def mixer(n):
                seg = a_cum[:, n:n + 1] - a_cum_t[n:n + 1, :]
                return split(jnp.exp(jnp.minimum(seg, 0.0)) * c_dot_b)
            x = act[:, cols]
            x_dt = x * spread(dt)
            wh, wm, wl = split(x_dt * spread(to_end))
            weighted3[0:CHUNK, cols] = wm
            weighted3[CHUNK:2 * CHUNK, cols] = wh
            weighted3[2 * CHUNK:3 * CHUNK, cols] = wl
            xh, xm, xl = split(jnp.concatenate([jnp.where(left, x_dt, 0.0), jnp.where(left, 0.0, x_dt)], axis=0))
            mh, mm, ml = (jnp.concatenate(pair, axis=1) for pair in zip(mixer(h0), mixer(h1)))
            x_hm = jnp.concatenate([xh, xm], axis=1)
            wide = fast_dot(mm, x_hm) + fast_dot(mh, x_hm)
            y = (fast_dot(ml, xh) + fast_dot(mh, xl)) + wide[:, LANES:] + wide[:, :LANES]
            y = y + v[:, cols] * spread(from_start)
            y = y + spread_row(skip) * x
            gated = y * silu(pre[HALO:HALO + CHUNK, cols])
            v[:, cols] = gated
            sq = sq + gated * gated
        total = jnp.sum(sq.T, axis=0, keepdims=True)
        stats[slot, me] = jnp.broadcast_to(total, (8, CHUNK))
        for off in range(1, tp_size):
            msg_stat(t, off).start()
        for o in range(0, width, TILE):
            cols = slice(o, min(o + TILE, width))
            decay = jnp.concatenate([jnp.where(left_row, whole[:, n:n + 1], whole[:, n + 1:n + 2])
                                     for n in range(o // head_dim, cols.stop // head_dim, 2)], axis=1)
            s_new = state[:, cols] * decay + three_dots(b1, b2, b3, weighted3, cols)
            state[:, cols] = s_new
            sh, sm, sl = split(s_new)
            state3[0:n_state, cols] = sm
            state3[n_state:2 * n_state, cols] = sh
            state3[2 * n_state:3 * n_state, cols] = sl

    def out_proj(t):
        slot = lax.rem(t, SLOTS)
        layer, row0 = where_of(t)

        @pl.when(row0 == 0)
        def _():
            load_out(layer).wait()
        for off in range(1, tp_size):
            peer = lax.rem(me + off, tp_size)
            pltpu.make_async_remote_copy(src_ref=stats.at[slot, peer], dst_ref=stats.at[slot, peer], send_sem=ssend.at[slot, off],
                                         recv_sem=srecv.at[slot, peer], device_id=dev_sib, device_id_type=MESH).wait_recv()
        for off in range(1, tp_size):
            msg_stat(t, off).wait_send()
        total = stats[slot, 0]
        for r in range(1, tp_size):
            total = total + stats[slot, r]
        scale = lax.rsqrt(total / inner_width + EPSILON)
        scale = jnp.broadcast_to(scale[0:1, :], (LANES, CHUNK)).T
        for p in range(width // LANES):
            cols = slice(p * LANES, (p + 1) * LANES)
            g[:, cols] = (v[:, cols] * scale * gw[layer, 0:1, cols]).astype(BF16)
        buf = pbuf.at[lax.rem(t, 2)]

        def tile(i, carry):
            o = pl.multiple_of(i * TILE, TILE)
            buf[:, pl.ds(o, TILE)] = jnp.dot(g[...], wout[layer, :, pl.ds(o, TILE)], preferred_element_type=F32)
            return carry
        lax.fori_loop(0, d_model // TILE, tile, 0)
        msg_rs(t, SIB).start()

    def pair_sum(t):
        msg_rs(t, SIB).wait_recv()
        buf, other = pbuf.at[lax.rem(t, 2)], sib.at[lax.rem(t, 2)]

        def block(i, carry):
            r = pl.multiple_of(i * 8, 8)
            mine = pl.ds(pl.multiple_of(core * half_rows + r, 8), 8)
            buf[mine, :] = buf[mine, :] + other[pl.ds(r, 8), :]
            return carry
        lax.fori_loop(0, half_rows // 8, block, 0)
        for kind in (FAR_P, FAR_M, NEAR_P, NEAR_M):
            msg_rs(t, kind).start()

    def relay_sum(t):
        slot = lax.rem(t, SLOTS)
        buf = pbuf.at[lax.rem(t, 2)]
        for way, (wait, send, j, part) in enumerate(((FAR_P, COMB_P, nxt, 1), (FAR_M, COMB_M, prv, 0))):
            msg_rs(t, wait).wait_recv()
            rows = pl.ds(pl.multiple_of(slice_at(core, j) + part * piece, piece), piece)
            buf[rows, :] = buf[rows, :] + far[slot, way]
            msg_rs(t, send).start()

    def finish(t):
        slot = lax.rem(t, SLOTS)
        layer, row0 = where_of(t)
        buf = pbuf.at[lax.rem(t, 2)]
        for kind in (NEAR_P, NEAR_M, COMB_P, COMB_M):
            msg_rs(t, kind).wait_recv()
        base = slice_at(core, chip)
        dst = pl.ds(pl.multiple_of(row0 + base, slice_rows), slice_rows)

        def store(res):
            lo = buf[pl.ds(base, piece), :] + near[slot, 0] + comb[slot, 1]
            hi = buf[pl.ds(pl.multiple_of(base + piece, piece), piece), :] + near[slot, 1] + comb[slot, 0]
            ures[layer, dst, :] = (res + jnp.concatenate([lo, hi], axis=0)).astype(BF16).astype(F32)

        @pl.when(layer == 0)
        def _():
            store(hid[dst, :].astype(F32))

        @pl.when(layer > 0)
        def _():
            store(ures[jnp.maximum(layer - 1, 0), dst, :])
        for kind in (OWN_P1, OWN_M1, OWN_P2, OWN_M2, D0):
            msg_ag(t, kind).start()
        for kind in (SIB, FAR_P, FAR_M, NEAR_P, NEAR_M, COMB_P, COMB_M):
            msg_rs(t, kind).wait_send()

    def forward(t):
        for wait, send in ((OWN_P1, FW_P), (OWN_M1, FW_M)):
            wait_ag(t, wait)
            msg_ag(t, send).start()

    def share(t):
        for waits, send in (((OWN_P2,), D1), ((OWN_M2,), D2), ((FW_P, FW_M), D3)):
            for kind in waits:
                wait_ag(t, kind)
            msg_ag(t, send).start()

    def collect(t):
        layer, row0 = where_of(t)
        for kind in (D0, D1, D2, D3):
            wait_ag(t, kind)
        for kind in ag_sent:
            msg_ag(t, kind).wait_send()

        @pl.when(layer == n_layers - 1)
        def _():
            def block(i, carry):
                rows = pl.ds(pl.multiple_of(row0 + i * 16, 16), 16)
                out[rows, :] = ures[layer, rows, :].astype(BF16)
                return carry
            lax.fori_loop(0, CHUNK // 16, block, 0)

    def guarded(step, t):
        @pl.when((t >= 0) & (t < n_tasks))
        def _():
            step(t)

    def iteration(t, carry):
        guarded(mix, t)
        guarded(collect, t - 5)
        guarded(pair_sum, t - 1)
        guarded(in_proj, t + 1)
        guarded(finish, t - 2)
        guarded(out_proj, t)
        guarded(relay_sum, t - 1)
        guarded(forward, t - 3)
        guarded(share, t - 4)
        return carry
    lax.fori_loop(-1, n_tasks + 5, iteration, 0)


def layers(tp_size, hidden, norm_w, w_z, w_x, w_bc, w_dt, conv_x, conv_bc, bias_x, bias_bc, dt_bias, a_log, d_skip, gate_w, w_out):
    n_batch, n_steps, d_model = hidden.shape
    n_layers, conv_width, width = conv_x.shape
    head_rows = pl.cdiv(dt_bias.shape[-1], 16) * 16
    w_dt = jnp.transpose(w_dt, (2, 0, 1))
    state2 = w_bc.shape[-1]
    piece = CHUNK // tp_size // 2
    any_spec = pl.BlockSpec(memory_space=pl.ANY)
    dma = pltpu.SemaphoreType.DMA
    run = pl.pallas_call(
        functools.partial(kernel, tp_size, conv_width),
        out_shape=pltpu.VMEM((n_steps, d_model), BF16),
        in_specs=[any_spec] * 15,
        out_specs=pl.BlockSpec(memory_space=pltpu.VMEM),
        scratch_shapes=[pltpu.VMEM(p.shape, p.dtype) for p in (norm_w, w_dt, conv_x, conv_bc, bias_x, bias_bc, dt_bias, a_log, d_skip, gate_w)] + [
            pltpu.VMEM((n_steps, d_model), BF16),
            pltpu.VMEM((n_layers, d_model, 2 * width + state2), BF16),
            pltpu.VMEM((n_layers, head_rows, d_model), BF16),
            pltpu.VMEM((n_layers, head_rows, d_model), F32),
            pltpu.VMEM((n_layers, width, d_model), BF16),
            pltpu.VMEM((n_layers, n_steps, d_model), F32),
            pltpu.VMEM((CHUNK, d_model), BF16),
            pltpu.VMEM((HALO + CHUNK, 2 * width + state2), F32),
            pltpu.VMEM((CHUNK, width + state2), F32),
            pltpu.VMEM((CHUNK, width), F32),
            pltpu.VMEM((CHUNK, width), BF16),
            pltpu.VMEM((CHUNK, LANES), F32),
            pltpu.VMEM((state2 // 2, width), F32),
            pltpu.VMEM((3 * state2 // 2, width), BF16),
            pltpu.VMEM((3 * CHUNK, width), BF16),
            pltpu.VMEM((2, CHUNK, d_model), F32),
            pltpu.VMEM((2, CHUNK // 2, d_model), F32),
            pltpu.VMEM((SLOTS, 2, piece, d_model), F32),
            pltpu.VMEM((SLOTS, 2, piece, d_model), F32),
            pltpu.VMEM((SLOTS, 2, piece, d_model), F32),
            pltpu.VMEM((SLOTS, tp_size, 8, CHUNK), F32),
            pltpu.VMEM((n_layers, 8, d_model), F32),
            pltpu.VMEM((n_layers, 8, width + state2), F32),
            pltpu.VMEM((n_layers, 8, width), F32),
            pltpu.VMEM((n_layers, 8, LANES), F32),
            dma((n_layers, (2 * width + state2) // TILE + 1)), dma((n_steps // CHUNK,)), dma((10,)),
            dma((SLOTS, tp_size)), dma((SLOTS, tp_size)), dma((SEM_SLOTS, 17)), dma((SEM_SLOTS, 17)),
        ],
        compiler_params=pltpu.CompilerParams(collective_id=0, has_side_effects=True, vmem_limit_bytes=62_000_000),
    )
    outs = [run(hidden[i], norm_w, w_z, w_x, w_bc, w_dt, conv_x, conv_bc, bias_x, bias_bc, dt_bias, a_log, d_skip, gate_w, w_out)
            for i in range(n_batch)]
    return jnp.stack(outs)


def solution(mesh):
    col_spec = P(None, None, 'tp')
    vec_spec = P(None, 'tp')
    in_specs = (P('dp'), P(), col_spec, col_spec, P(), col_spec, col_spec, P(), vec_spec, P(), vec_spec, vec_spec, vec_spec, vec_spec, P(None, 'tp', None))
    return jax.shard_map(functools.partial(layers, mesh.shape['tp']), mesh=mesh, in_specs=in_specs, out_specs=P('dp'), check_vma=False)
```

```python
import functools

import jax
import jax.numpy as jnp
from jax import lax
from jax.experimental import pallas as pl
from jax.experimental.pallas import tpu as pltpu
from jax.sharding import PartitionSpec as P

EPSILON = 1e-5
F32 = jnp.float32
BF16 = jnp.bfloat16
MESH = pl.DeviceIdType.MESH
LANES = 128
CHUNK = 128
SLOTS = 4
SEM_SLOTS = 6
HALO = 8
TILE = 256
(SIB, FAR_P, FAR_M, NEAR_P, NEAR_M, COMB_P, COMB_M, OWN_P1, OWN_P2, OWN_M1, OWN_M2, FW_P, FW_M, D0, D1, D2, D3) = range(17)


def fast_dot(a, b, dims=(((1,), (0,)), ((), ()))):
    return lax.dot_general(a, b, dims, preferred_element_type=F32)


def split(m):
    hi = m.astype(BF16)
    rest = m - hi.astype(F32)
    mid = rest.astype(BF16)
    return hi, mid, (rest - mid.astype(F32)).astype(BF16)


def left_parts(m):
    hi, mid, lo = split(m)
    return jnp.concatenate([hi, hi], axis=1), jnp.concatenate([mid, mid], axis=1), jnp.concatenate([lo, hi], axis=1)


def three_dots(p1, p2, p3, parts, cols):
    n = parts.shape[0] // 3
    upper = parts[0:2 * n, cols]
    return (fast_dot(p3, parts[n:3 * n, cols]) + fast_dot(p2, upper)) + fast_dot(p1, upper)


def silu(a):
    return a * (1.0 / (1.0 + jnp.exp(-a)))


def softplus(a):
    return jnp.maximum(a, 0.0) + jnp.log1p(jnp.exp(-jnp.abs(a)))


def kernel(tp_size, conv_width, hid_hbm, norm_hbm, wz_hbm, wx_hbm, wbc_hbm, wdt_hbm, convx_hbm, convbc_hbm, biasx_hbm, biasbc_hbm,
           dtb_hbm, alog_hbm, dskip_hbm, gate_hbm, wout_hbm, out,
           norm_in, wdt_in, convx_in, convbc_in, biasx_in, biasbc_in, dtb_in, alog_in, dskip_in, gate_in,
           hid, win, wdt, wdt_f, wout, ures, h, pre, act, v, g, dtp, state, state3, weighted3, pbuf, sib, far, near, comb, stats, nw, cw, gw, hp,
           wsem, hsem, psem, ssend, srecv, msend, mrecv):
    n_layers, n_steps, d_model = ures.shape
    width = v.shape[1]
    conv_ch = act.shape[1]
    n_state = (conv_ch - width) // 2
    n_heads = dtb_in.shape[1]
    head_dim = width // n_heads
    n_chunks = n_steps // CHUNK
    n_tasks = n_layers * n_chunks
    n_chips = tp_size // 2
    n_tiles = pre.shape[1] // TILE
    half_rows = CHUNK // 2
    slice_rows = half_rows // n_chips
    piece = slice_rows // 2
    inner_width = width * tp_size

    me = lax.axis_index('tp')
    chip = me // 2
    core = lax.rem(me, 2)
    nxt = lax.rem(chip + 1, n_chips)
    prv = lax.rem(chip + n_chips - 1, n_chips)
    opp = lax.rem(chip + 2, n_chips)
    dev_nxt = {'tp': nxt * 2 + core}
    dev_prv = {'tp': prv * 2 + core}
    dev_sib = {'tp': chip * 2 + 1 - core}

    barrier = pltpu.get_barrier_semaphore()
    for off in range(1, tp_size):
        pl.semaphore_signal(barrier, inc=1, device_id={'tp': lax.rem(me + off, tp_size)}, device_id_type=MESH)

    def load_hid(i):
        rows = pl.ds(pl.multiple_of(i * CHUNK, CHUNK), CHUNK)
        return pltpu.make_async_copy(hid_hbm.at[rows], hid.at[rows], hsem.at[i])

    def load_in(layer):
        copies = []
        for w_hbm, first, n_cols in ((wz_hbm, 0, width), (wx_hbm, width, width), (wbc_hbm, 2 * width, 2 * n_state)):
            done = 0
            while done < n_cols:
                n = min(TILE - (first + done) % TILE, n_cols - done)
                at = first + done
                copies.append(pltpu.make_async_copy(w_hbm.at[layer, :, pl.ds(done, n)], win.at[layer, :, pl.ds(at, n)],
                                                    wsem.at[layer, at // TILE]))
                done += n
        return copies

    def wait_in(layer, tile):
        ref = win.at[layer, :, pl.ds(pl.multiple_of(tile * TILE, TILE), TILE)]
        pltpu.make_async_copy(ref, ref, wsem.at[layer, tile]).wait()

    def load_out(layer):
        return pltpu.make_async_copy(wout_hbm.at[layer], wout.at[layer], wsem.at[layer, n_tiles])

    params = ((norm_hbm, norm_in), (wdt_hbm, wdt_in), (convx_hbm, convx_in), (convbc_hbm, convbc_in), (biasx_hbm, biasx_in),
              (biasbc_hbm, biasbc_in), (dtb_hbm, dtb_in), (alog_hbm, alog_in), (dskip_hbm, dskip_in), (gate_hbm, gate_in))
    small = [pltpu.make_async_copy(src, dst, psem.at[i]) for i, (src, dst) in enumerate(params)]
    load_hid(0).start()
    for cp in small:
        cp.start()
    for cp in load_in(0):
        cp.start()
    small[0].wait()
    for layer in range(n_layers):
        nw[layer, 0:1, :] = norm_in[layer:layer + 1, :].astype(F32)

    def widen():
        for cp in small[1:]:
            cp.wait()
        hp[...] = jnp.zeros_like(hp)
        wdt_f[...] = jnp.zeros_like(wdt_f)
        for n in range(n_heads):
            cols = wdt_in[n].astype(F32)
            for layer in range(n_layers):
                wdt_f[layer, n:n + 1, :] = cols[layer:layer + 1, :]
        wdt[...] = wdt_f[...].astype(BF16)
        dtp[...] = jnp.zeros_like(dtp)
        for layer in range(n_layers):
            gw[layer, 0:1, :] = gate_in[layer:layer + 1, :].astype(F32)
            cw[layer, 0:conv_width, 0:width] = convx_in[layer].astype(F32)
            cw[layer, 0:conv_width, width:conv_ch] = convbc_in[layer].astype(F32)
            cw[layer, conv_width:conv_width + 1, 0:width] = biasx_in[layer:layer + 1, :].astype(F32)
            cw[layer, conv_width:conv_width + 1, width:conv_ch] = biasbc_in[layer:layer + 1, :].astype(F32)
            hp[layer, 0:1, 0:n_heads] = dtb_in[layer:layer + 1, :]
            hp[layer, 1:2, 0:n_heads] = alog_in[layer:layer + 1, :]
            hp[layer, 2:3, 0:n_heads] = dskip_in[layer:layer + 1, :]

    pl.semaphore_wait(barrier, tp_size - 1)

    def where_of(t):
        layer = t // n_chunks
        return layer, pl.multiple_of((t - layer * n_chunks) * CHUNK, CHUNK)

    def remote(src, dst, t, kind, dev):
        slot = lax.rem(t, SEM_SLOTS)
        return pltpu.make_async_remote_copy(src_ref=src, dst_ref=dst, send_sem=msend.at[slot, kind], recv_sem=mrecv.at[slot, kind],
                                            device_id=dev, device_id_type=MESH)

    def slice_at(c, j):
        return pl.multiple_of(c * half_rows + j * slice_rows, slice_rows)

    def msg_rs(t, kind):
        slot = lax.rem(t, SLOTS)
        buf = pbuf.at[lax.rem(t, 2)]

        def src(j, part):
            return buf.at[pl.ds(pl.multiple_of(slice_at(core, j) + part * piece, piece), piece)]
        if kind == SIB:
            other = pl.multiple_of((1 - core) * half_rows, half_rows)
            return remote(buf.at[pl.ds(other, half_rows)], sib.at[lax.rem(t, 2)], t, kind, dev_sib)
        if kind == FAR_P:
            return remote(src(opp, 1), far.at[slot, 0], t, kind, dev_nxt)
        if kind == FAR_M:
            return remote(src(opp, 0), far.at[slot, 1], t, kind, dev_prv)
        if kind == NEAR_P:
            return remote(src(nxt, 0), near.at[slot, 0], t, kind, dev_nxt)
        if kind == NEAR_M:
            return remote(src(prv, 1), near.at[slot, 1], t, kind, dev_prv)
        if kind == COMB_P:
            return remote(src(nxt, 1), comb.at[slot, 0], t, kind, dev_nxt)
        return remote(src(prv, 0), comb.at[slot, 1], t, kind, dev_prv)

    def ag_rows(t, c, j, part=None):
        layer, row0 = where_of(t)
        base = row0 + slice_at(c, j)
        if part is None:
            return ures.at[layer, pl.ds(pl.multiple_of(base, slice_rows), slice_rows)]
        return ures.at[layer, pl.ds(pl.multiple_of(base + part * piece, piece), piece)]

    ag_sent = {OWN_P1: (chip, 0, dev_nxt), OWN_P2: (chip, 1, dev_nxt), OWN_M1: (chip, 1, dev_prv), OWN_M2: (chip, 0, dev_prv),
               FW_P: (prv, 0, dev_nxt), FW_M: (nxt, 1, dev_prv),
               D0: (chip, None, dev_sib), D1: (prv, None, dev_sib), D2: (nxt, None, dev_sib), D3: (opp, None, dev_sib)}
    ag_got = {OWN_P1: (core, prv, 0), OWN_P2: (core, prv, 1), OWN_M1: (core, nxt, 1), OWN_M2: (core, nxt, 0),
              FW_P: (core, opp, 0), FW_M: (core, opp, 1),
              D0: (1 - core, chip, None), D1: (1 - core, prv, None), D2: (1 - core, nxt, None), D3: (1 - core, opp, None)}

    def msg_ag(t, kind):
        j, part, dev = ag_sent[kind]
        ref = ag_rows(t, core, j, part)
        return remote(ref, ref, t, kind, dev)

    def wait_ag(t, kind):
        ref = ag_rows(t, *ag_got[kind])
        remote(ref, ref, t, kind, dev_sib).wait_recv()

    def msg_stat(t, off):
        slot = lax.rem(t, SLOTS)
        return pltpu.make_async_remote_copy(src_ref=stats.at[slot, me], dst_ref=stats.at[slot, me], send_sem=ssend.at[slot, off],
                                            recv_sem=srecv.at[slot, me], device_id={'tp': lax.rem(me + off, tp_size)}, device_id_type=MESH)

    def in_proj(t):
        layer, row0 = where_of(t)

        @pl.when(layer == 0)
        def _():
            load_hid(t).wait()

        @pl.when(row0 == 0)
        def _():
            pre[0:HALO, :] = jnp.zeros((HALO, pre.shape[1]), F32)

        @pl.when(row0 > 0)
        def _():
            pre[0:HALO, :] = pre[CHUNK:CHUNK + HALO, :]

        def norm(load):
            def block(i, carry):
                r = pl.multiple_of(i * 32, 32)
                u = load(pl.multiple_of(row0 + r, 32))
                scale = lax.rsqrt(jnp.mean(u * u, axis=-1, keepdims=True) + EPSILON)
                h[pl.ds(r, 32), :] = (u * scale * nw[layer, 0:1, :]).astype(BF16)
                return carry
            lax.fori_loop(0, CHUNK // 32, block, 0)

        @pl.when(layer == 0)
        def _():
            norm(lambda r: hid[pl.ds(r, 32), :].astype(F32))

        @pl.when(layer > 0)
        def _():
            norm(lambda r: ures[jnp.maximum(layer - 1, 0), pl.ds(r, 32), :])

        pl.when(t == 0)(widen)
        wide = 2 * TILE

        def tile(i, carry):
            @pl.when(row0 == 0)
            def _():
                wait_in(layer, 2 * i)
                wait_in(layer, 2 * i + 1)
            o = pl.multiple_of(i * wide, wide)
            prod = jnp.dot(h[...], win[layer, :, pl.ds(o, wide)], preferred_element_type=F32)
            pre[HALO:HALO + CHUNK, pl.ds(o, wide)] = prod.astype(BF16).astype(F32)
            return carry
        lax.fori_loop(0, pre.shape[1] // wide, tile, 0)
        prod = lax.dot_general(h[...], wdt[layer], (((1,), (1,)), ((), ())), preferred_element_type=F32)
        dtp[:, 0:wdt.shape[1]] = prod.astype(BF16).astype(F32)

        @pl.when(t == 0)
        def _():
            load_out(0).start()
            for i in range(1, n_chunks):
                load_hid(i).start()

        @pl.when((row0 == CHUNK) & (layer < n_layers - 1))
        def _():
            for k in range(1, n_layers):
                @pl.when(layer == k - 1)
                def _():
                    for cp in load_in(k):
                        cp.start()
                    load_out(k).start()

    def mix(t):
        slot = lax.rem(t, SLOTS)
        layer, row0 = where_of(t)

        @pl.when(row0 == 0)
        def _():
            state[...] = jnp.zeros_like(state)
            state3[...] = jnp.zeros_like(state3)

        def conv(i, carry):
            o = pl.multiple_of(i * LANES, LANES)
            acc = jnp.broadcast_to(cw[layer, conv_width:conv_width + 1, pl.ds(o, LANES)], (CHUNK, LANES))
            for j in range(conv_width):
                first = HALO - (conv_width - 1) + j
                acc = acc + pre[first:first + CHUNK, pl.ds(pl.multiple_of(width + o, LANES), LANES)] * cw[layer, j:j + 1, pl.ds(o, LANES)]
            act[:, pl.ds(o, LANES)] = silu(acc)
            return carry
        lax.fori_loop(0, conv_ch // LANES, conv, 0)

        row_id = lax.broadcasted_iota(jnp.int32, (CHUNK, CHUNK), 0)
        col_id = lax.broadcasted_iota(jnp.int32, (CHUNK, CHUNK), 1)
        lower = row_id >= col_id
        left = col_id < head_dim
        left_row = left[0:1, :]
        dt = softplus(dtp[...] + hp[layer, 0:1, :])
        a = -dt * jnp.exp(hp[layer, 1:2, :])
        ones = jnp.where(lower, 1.0, 0.0).astype(BF16)
        a_cum = sum(fast_dot(ones, part) for part in reversed(split(a)))
        a_cum_t = a_cum.T
        a_last = a_cum[CHUNK - 1:CHUNK, :]
        from_start = jnp.exp(a_cum)
        to_end = jnp.exp(a_last - a_cum)
        whole = jnp.exp(a_last)
        skip = hp[layer, 2:3, :]
        b = act[:, width:width + n_state]
        c1, c2, c3 = left_parts(act[:, width + n_state:conv_ch])
        bh, bm, bl = split(b)
        nt = (((1,), (1,)), ((), ()))
        b_mh = jnp.concatenate([bm, bh], axis=1)
        c_dot_b = (fast_dot(c3, jnp.concatenate([bh, bl], axis=1), nt) + fast_dot(c2, b_mh, nt)) + fast_dot(c1, b_mh, nt)
        c_dot_b = jnp.where(lower, c_dot_b, 0.0)
        b1, b2, b3 = left_parts(b.T)
        for o in range(0, width, TILE):
            cols = slice(o, min(o + TILE, width))
            v[:, cols] = three_dots(c1, c2, c3, state3, cols)
        sq = jnp.zeros((CHUNK, LANES), F32)
        for p in range(width // LANES):
            cols = slice(p * LANES, (p + 1) * LANES)
            h0, h1 = 2 * p, 2 * p + 1

            def spread(m):
                return jnp.where(left, m[:, h0:h0 + 1], m[:, h1:h1 + 1])

            def spread_row(m):
                return jnp.where(left_row, m[:, h0:h0 + 1], m[:, h1:h1 + 1])

            def mixer(n):
                seg = a_cum[:, n:n + 1] - a_cum_t[n:n + 1, :]
                return split(jnp.exp(jnp.minimum(seg, 0.0)) * c_dot_b)
            x = act[:, cols]
            x_dt = x * spread(dt)
            wh, wm, wl = split(x_dt * spread(to_end))
            weighted3[0:CHUNK, cols] = wm
            weighted3[CHUNK:2 * CHUNK, cols] = wh
            weighted3[2 * CHUNK:3 * CHUNK, cols] = wl
            xh, xm, xl = split(jnp.concatenate([jnp.where(left, x_dt, 0.0), jnp.where(left, 0.0, x_dt)], axis=0))
            mh, mm, ml = (jnp.concatenate(pair, axis=1) for pair in zip(mixer(h0), mixer(h1)))
            x_hm = jnp.concatenate([xh, xm], axis=1)
            wide = fast_dot(mm, x_hm) + fast_dot(mh, x_hm)
            y = (fast_dot(ml, xh) + fast_dot(mh, xl)) + wide[:, LANES:] + wide[:, :LANES]
            y = y + v[:, cols] * spread(from_start)
            y = y + spread_row(skip) * x
            gated = y * silu(pre[HALO:HALO + CHUNK, cols])
            v[:, cols] = gated
            sq = sq + gated * gated
        total = jnp.sum(sq.T, axis=0, keepdims=True)
        stats[slot, me] = jnp.broadcast_to(total, (8, CHUNK))
        for off in range(1, tp_size):
            msg_stat(t, off).start()
        for o in range(0, width, TILE):
            cols = slice(o, min(o + TILE, width))
            decay = jnp.concatenate([jnp.where(left_row, whole[:, n:n + 1], whole[:, n + 1:n + 2])
                                     for n in range(o // head_dim, cols.stop // head_dim, 2)], axis=1)
            s_new = state[:, cols] * decay + three_dots(b1, b2, b3, weighted3, cols)
            state[:, cols] = s_new
            sh, sm, sl = split(s_new)
            state3[0:n_state, cols] = sm
            state3[n_state:2 * n_state, cols] = sh
            state3[2 * n_state:3 * n_state, cols] = sl

    def out_proj(t):
        slot = lax.rem(t, SLOTS)
        layer, row0 = where_of(t)

        @pl.when(row0 == 0)
        def _():
            load_out(layer).wait()
        for off in range(1, tp_size):
            peer = lax.rem(me + off, tp_size)
            pltpu.make_async_remote_copy(src_ref=stats.at[slot, peer], dst_ref=stats.at[slot, peer], send_sem=ssend.at[slot, off],
                                         recv_sem=srecv.at[slot, peer], device_id=dev_sib, device_id_type=MESH).wait_recv()
        for off in range(1, tp_size):
            msg_stat(t, off).wait_send()
        total = stats[slot, 0]
        for r in range(1, tp_size):
            total = total + stats[slot, r]
        scale = lax.rsqrt(total / inner_width + EPSILON)
        scale = jnp.broadcast_to(scale[0:1, :], (LANES, CHUNK)).T
        for p in range(width // LANES):
            cols = slice(p * LANES, (p + 1) * LANES)
            g[:, cols] = (v[:, cols] * scale * gw[layer, 0:1, cols]).astype(BF16)
        buf = pbuf.at[lax.rem(t, 2)]

        def tile(i, carry):
            o = pl.multiple_of(i * TILE, TILE)
            buf[:, pl.ds(o, TILE)] = jnp.dot(g[...], wout[layer, :, pl.ds(o, TILE)], preferred_element_type=F32)
            return carry
        lax.fori_loop(0, d_model // TILE, tile, 0, unroll=True)
        msg_rs(t, SIB).start()

    def pair_sum(t):
        msg_rs(t, SIB).wait_recv()
        buf, other = pbuf.at[lax.rem(t, 2)], sib.at[lax.rem(t, 2)]

        def block(i, carry):
            r = pl.multiple_of(i * 8, 8)
            mine = pl.ds(pl.multiple_of(core * half_rows + r, 8), 8)
            buf[mine, :] = buf[mine, :] + other[pl.ds(r, 8), :]
            return carry
        lax.fori_loop(0, half_rows // 8, block, 0)
        for kind in (FAR_P, FAR_M, NEAR_P, NEAR_M):
            msg_rs(t, kind).start()

    def relay_sum(t):
        slot = lax.rem(t, SLOTS)
        buf = pbuf.at[lax.rem(t, 2)]
        for way, (wait, send, j, part) in enumerate(((FAR_P, COMB_P, nxt, 1), (FAR_M, COMB_M, prv, 0))):
            msg_rs(t, wait).wait_recv()
            rows = pl.ds(pl.multiple_of(slice_at(core, j) + part * piece, piece), piece)
            buf[rows, :] = buf[rows, :] + far[slot, way]
            msg_rs(t, send).start()

    def finish(t):
        slot = lax.rem(t, SLOTS)
        layer, row0 = where_of(t)
        buf = pbuf.at[lax.rem(t, 2)]
        for kind in (NEAR_P, NEAR_M, COMB_P, COMB_M):
            msg_rs(t, kind).wait_recv()
        base = slice_at(core, chip)
        dst = pl.ds(pl.multiple_of(row0 + base, slice_rows), slice_rows)

        def store(res):
            lo = buf[pl.ds(base, piece), :] + near[slot, 0] + comb[slot, 1]
            hi = buf[pl.ds(pl.multiple_of(base + piece, piece), piece), :] + near[slot, 1] + comb[slot, 0]
            ures[layer, dst, :] = (res + jnp.concatenate([lo, hi], axis=0)).astype(BF16).astype(F32)

        @pl.when(layer == 0)
        def _():
            store(hid[dst, :].astype(F32))

        @pl.when(layer > 0)
        def _():
            store(ures[jnp.maximum(layer - 1, 0), dst, :])
        for kind in (OWN_P1, OWN_M1, OWN_P2, OWN_M2, D0):
            msg_ag(t, kind).start()
        for kind in (SIB, FAR_P, FAR_M, NEAR_P, NEAR_M, COMB_P, COMB_M):
            msg_rs(t, kind).wait_send()

    def forward(t):
        for wait, send in ((OWN_P1, FW_P), (OWN_M1, FW_M)):
            wait_ag(t, wait)
            msg_ag(t, send).start()

    def share(t):
        for waits, send in (((OWN_P2,), D1), ((OWN_M2,), D2), ((FW_P, FW_M), D3)):
            for kind in waits:
                wait_ag(t, kind)
            msg_ag(t, send).start()

    def collect(t):
        layer, row0 = where_of(t)
        for kind in (D0, D1, D2, D3):
            wait_ag(t, kind)
        for kind in ag_sent:
            msg_ag(t, kind).wait_send()

        @pl.when(layer == n_layers - 1)
        def _():
            def block(i, carry):
                rows = pl.ds(pl.multiple_of(row0 + i * 16, 16), 16)
                out[rows, :] = ures[layer, rows, :].astype(BF16)
                return carry
            lax.fori_loop(0, CHUNK // 16, block, 0)

    def guarded(step, t):
        @pl.when((t >= 0) & (t < n_tasks))
        def _():
            step(t)

    def iteration(t, carry):
        guarded(mix, t)
        guarded(collect, t - 5)
        guarded(pair_sum, t - 1)
        guarded(in_proj, t + 1)
        guarded(finish, t - 2)
        guarded(out_proj, t)
        guarded(relay_sum, t - 1)
        guarded(forward, t - 3)
        guarded(share, t - 4)
        return carry
    lax.fori_loop(-1, n_tasks + 5, iteration, 0)


def layers(tp_size, hidden, norm_w, w_z, w_x, w_bc, w_dt, conv_x, conv_bc, bias_x, bias_bc, dt_bias, a_log, d_skip, gate_w, w_out):
    n_batch, n_steps, d_model = hidden.shape
    n_layers, conv_width, width = conv_x.shape
    head_rows = pl.cdiv(dt_bias.shape[-1], 16) * 16
    w_dt = jnp.transpose(w_dt, (2, 0, 1))
    state2 = w_bc.shape[-1]
    piece = CHUNK // tp_size // 2
    any_spec = pl.BlockSpec(memory_space=pl.ANY)
    dma = pltpu.SemaphoreType.DMA
    run = pl.pallas_call(
        functools.partial(kernel, tp_size, conv_width),
        out_shape=pltpu.VMEM((n_steps, d_model), BF16),
        in_specs=[any_spec] * 15,
        out_specs=pl.BlockSpec(memory_space=pltpu.VMEM),
        scratch_shapes=[pltpu.VMEM(p.shape, p.dtype) for p in (norm_w, w_dt, conv_x, conv_bc, bias_x, bias_bc, dt_bias, a_log, d_skip, gate_w)] + [
            pltpu.VMEM((n_steps, d_model), BF16),
            pltpu.VMEM((n_layers, d_model, 2 * width + state2), BF16),
            pltpu.VMEM((n_layers, head_rows, d_model), BF16),
            pltpu.VMEM((n_layers, head_rows, d_model), F32),
            pltpu.VMEM((n_layers, width, d_model), BF16),
            pltpu.VMEM((n_layers, n_steps, d_model), F32),
            pltpu.VMEM((CHUNK, d_model), BF16),
            pltpu.VMEM((HALO + CHUNK, 2 * width + state2), F32),
            pltpu.VMEM((CHUNK, width + state2), F32),
            pltpu.VMEM((CHUNK, width), F32),
            pltpu.VMEM((CHUNK, width), BF16),
            pltpu.VMEM((CHUNK, LANES), F32),
            pltpu.VMEM((state2 // 2, width), F32),
            pltpu.VMEM((3 * state2 // 2, width), BF16),
            pltpu.VMEM((3 * CHUNK, width), BF16),
            pltpu.VMEM((2, CHUNK, d_model), F32),
            pltpu.VMEM((2, CHUNK // 2, d_model), F32),
            pltpu.VMEM((SLOTS, 2, piece, d_model), F32),
            pltpu.VMEM((SLOTS, 2, piece, d_model), F32),
            pltpu.VMEM((SLOTS, 2, piece, d_model), F32),
            pltpu.VMEM((SLOTS, tp_size, 8, CHUNK), F32),
            pltpu.VMEM((n_layers, 8, d_model), F32),
            pltpu.VMEM((n_layers, 8, width + state2), F32),
            pltpu.VMEM((n_layers, 8, width), F32),
            pltpu.VMEM((n_layers, 8, LANES), F32),
            dma((n_layers, (2 * width + state2) // TILE + 1)), dma((n_steps // CHUNK,)), dma((10,)),
            dma((SLOTS, tp_size)), dma((SLOTS, tp_size)), dma((SEM_SLOTS, 17)), dma((SEM_SLOTS, 17)),
        ],
        compiler_params=pltpu.CompilerParams(collective_id=0, has_side_effects=True, vmem_limit_bytes=62_000_000),
    )
    outs = [run(hidden[i], norm_w, w_z, w_x, w_bc, w_dt, conv_x, conv_bc, bias_x, bias_bc, dt_bias, a_log, d_skip, gate_w, w_out)
            for i in range(n_batch)]
    return jnp.stack(outs)


def solution(mesh):
    col_spec = P(None, None, 'tp')
    vec_spec = P(None, 'tp')
    in_specs = (P('dp'), P(), col_spec, col_spec, P(), col_spec, col_spec, P(), vec_spec, P(), vec_spec, vec_spec, vec_spec, vec_spec, P(None, 'tp', None))
    return jax.shard_map(functools.partial(layers, mesh.shape['tp']), mesh=mesh, in_specs=in_specs, out_specs=P('dp'), check_vma=False)
```

```python
import functools

import jax
import jax.numpy as jnp
from jax import lax
from jax.experimental import pallas as pl
from jax.experimental.pallas import tpu as pltpu
from jax.sharding import PartitionSpec as P

EPSILON = 1e-5
F32 = jnp.float32
BF16 = jnp.bfloat16
MESH = pl.DeviceIdType.MESH
LANES = 128
CHUNK = 128
SLOTS = 4
SEM_SLOTS = 8
P_SLOTS = 3
HALO = 8
TILE = 256
(SIB, FAR_P, FAR_M, NEAR_P, NEAR_M, COMB_P, COMB_M, OWN_P1, OWN_P2, OWN_M1, OWN_M2, FW_P, FW_M, D0, D1, D2, D3) = range(17)


def fast_dot(a, b, dims=(((1,), (0,)), ((), ()))):
    return lax.dot_general(a, b, dims, preferred_element_type=F32)


def split(m):
    hi = m.astype(BF16)
    rest = m - hi.astype(F32)
    mid = rest.astype(BF16)
    return hi, mid, (rest - mid.astype(F32)).astype(BF16)


def left_parts(m):
    hi, mid, lo = split(m)
    return jnp.concatenate([hi, hi], axis=1), jnp.concatenate([mid, mid], axis=1), jnp.concatenate([lo, hi], axis=1)


def three_dots(p1, p2, p3, parts, cols):
    n = parts.shape[0] // 3
    upper = parts[0:2 * n, cols]
    return (fast_dot(p3, parts[n:3 * n, cols]) + fast_dot(p2, upper)) + fast_dot(p1, upper)


def silu(a):
    return a * (1.0 / (1.0 + jnp.exp(-a)))


def softplus(a):
    return jnp.maximum(a, 0.0) + jnp.log1p(jnp.exp(-jnp.abs(a)))


def kernel(tp_size, conv_width, hid_hbm, norm_hbm, wz_hbm, wx_hbm, wbc_hbm, wdt_hbm, convx_hbm, convbc_hbm, biasx_hbm, biasbc_hbm,
           dtb_hbm, alog_hbm, dskip_hbm, gate_hbm, wout_hbm, out,
           norm_in, wdt_in, convx_in, convbc_in, biasx_in, biasbc_in, dtb_in, alog_in, dskip_in, gate_in,
           hid, win, wdt, wdt_f, wout, ures, h, pre, act, v, g, dtp, state, state3, weighted3, pbuf, sib, far, near, comb, stats, nw, cw, gw, hp,
           wsem, hsem, psem, ssend, srecv, msend, mrecv):
    n_layers, n_steps, d_model = ures.shape
    width = v.shape[1]
    conv_ch = act.shape[1]
    n_state = (conv_ch - width) // 2
    n_heads = dtb_in.shape[1]
    head_dim = width // n_heads
    n_chunks = n_steps // CHUNK
    n_tasks = n_layers * n_chunks
    n_chips = tp_size // 2
    n_tiles = pre.shape[1] // TILE
    half_rows = CHUNK // 2
    slice_rows = half_rows // n_chips
    piece = slice_rows // 2
    inner_width = width * tp_size

    me = lax.axis_index('tp')
    chip = me // 2
    core = lax.rem(me, 2)
    nxt = lax.rem(chip + 1, n_chips)
    prv = lax.rem(chip + n_chips - 1, n_chips)
    opp = lax.rem(chip + 2, n_chips)
    dev_nxt = {'tp': nxt * 2 + core}
    dev_prv = {'tp': prv * 2 + core}
    dev_sib = {'tp': chip * 2 + 1 - core}

    barrier = pltpu.get_barrier_semaphore()
    for off in range(1, tp_size):
        pl.semaphore_signal(barrier, inc=1, device_id={'tp': lax.rem(me + off, tp_size)}, device_id_type=MESH)

    def load_hid(i):
        rows = pl.ds(pl.multiple_of(i * CHUNK, CHUNK), CHUNK)
        return pltpu.make_async_copy(hid_hbm.at[rows], hid.at[rows], hsem.at[i])

    def load_in(layer):
        copies = []
        for w_hbm, first, n_cols in ((wz_hbm, 0, width), (wx_hbm, width, width), (wbc_hbm, 2 * width, 2 * n_state)):
            done = 0
            while done < n_cols:
                n = min(TILE - (first + done) % TILE, n_cols - done)
                at = first + done
                copies.append(pltpu.make_async_copy(w_hbm.at[layer, :, pl.ds(done, n)], win.at[layer, :, pl.ds(at, n)],
                                                    wsem.at[layer, at // TILE]))
                done += n
        return copies

    def wait_in(layer, tile):
        ref = win.at[layer, :, pl.ds(pl.multiple_of(tile * TILE, TILE), TILE)]
        pltpu.make_async_copy(ref, ref, wsem.at[layer, tile]).wait()

    def load_out(layer):
        return pltpu.make_async_copy(wout_hbm.at[layer], wout.at[layer], wsem.at[layer, n_tiles])

    params = ((norm_hbm, norm_in), (wdt_hbm, wdt_in), (convx_hbm, convx_in), (convbc_hbm, convbc_in), (biasx_hbm, biasx_in),
              (biasbc_hbm, biasbc_in), (dtb_hbm, dtb_in), (alog_hbm, alog_in), (dskip_hbm, dskip_in), (gate_hbm, gate_in))
    small = [pltpu.make_async_copy(src, dst, psem.at[i]) for i, (src, dst) in enumerate(params)]
    load_hid(0).start()
    for cp in small:
        cp.start()
    for cp in load_in(0):
        cp.start()
    small[0].wait()
    for layer in range(n_layers):
        nw[layer, 0:1, :] = norm_in[layer:layer + 1, :].astype(F32)

    def widen():
        for cp in small[1:]:
            cp.wait()
        hp[...] = jnp.zeros_like(hp)
        wdt_f[...] = jnp.zeros_like(wdt_f)
        for n in range(n_heads):
            cols = wdt_in[n].astype(F32)
            for layer in range(n_layers):
                wdt_f[layer, n:n + 1, :] = cols[layer:layer + 1, :]
        wdt[...] = wdt_f[...].astype(BF16)
        dtp[...] = jnp.zeros_like(dtp)
        for layer in range(n_layers):
            gw[layer, 0:1, :] = gate_in[layer:layer + 1, :].astype(F32)
            cw[layer, 0:conv_width, 0:width] = convx_in[layer].astype(F32)
            cw[layer, 0:conv_width, width:conv_ch] = convbc_in[layer].astype(F32)
            cw[layer, conv_width:conv_width + 1, 0:width] = biasx_in[layer:layer + 1, :].astype(F32)
            cw[layer, conv_width:conv_width + 1, width:conv_ch] = biasbc_in[layer:layer + 1, :].astype(F32)
            hp[layer, 0:1, 0:n_heads] = dtb_in[layer:layer + 1, :]
            hp[layer, 1:2, 0:n_heads] = alog_in[layer:layer + 1, :]
            hp[layer, 2:3, 0:n_heads] = dskip_in[layer:layer + 1, :]

    pl.semaphore_wait(barrier, tp_size - 1)

    def where_of(t):
        layer = sum(jnp.where(t >= k * n_chunks, 1, 0) for k in range(1, n_layers))
        return layer, pl.multiple_of((t - layer * n_chunks) * CHUNK, CHUNK)

    def remote(src, dst, t, kind, dev):
        slot = lax.rem(t, SEM_SLOTS)
        return pltpu.make_async_remote_copy(src_ref=src, dst_ref=dst, send_sem=msend.at[slot, kind], recv_sem=mrecv.at[slot, kind],
                                            device_id=dev, device_id_type=MESH)

    def slice_at(c, j):
        return pl.multiple_of(c * half_rows + j * slice_rows, slice_rows)

    def msg_rs(t, kind):
        slot = lax.rem(t, SLOTS)
        buf = pbuf.at[lax.rem(t, P_SLOTS)]

        def src(j, part):
            return buf.at[pl.ds(pl.multiple_of(slice_at(core, j) + part * piece, piece), piece)]
        if kind == SIB:
            other = pl.multiple_of((1 - core) * half_rows, half_rows)
            return remote(buf.at[pl.ds(other, half_rows)], sib.at[lax.rem(t, 2)], t, kind, dev_sib)
        if kind == FAR_P:
            return remote(src(opp, 1), far.at[slot, 0], t, kind, dev_nxt)
        if kind == FAR_M:
            return remote(src(opp, 0), far.at[slot, 1], t, kind, dev_prv)
        if kind == NEAR_P:
            return remote(src(nxt, 0), near.at[slot, 0], t, kind, dev_nxt)
        if kind == NEAR_M:
            return remote(src(prv, 1), near.at[slot, 1], t, kind, dev_prv)
        if kind == COMB_P:
            return remote(src(nxt, 1), comb.at[slot, 0], t, kind, dev_nxt)
        return remote(src(prv, 0), comb.at[slot, 1], t, kind, dev_prv)

    def ag_rows(t, c, j, part=None):
        layer, row0 = where_of(t)
        base = row0 + slice_at(c, j)
        if part is None:
            return ures.at[layer, pl.ds(pl.multiple_of(base, slice_rows), slice_rows)]
        return ures.at[layer, pl.ds(pl.multiple_of(base + part * piece, piece), piece)]

    ag_sent = {OWN_P1: (chip, 0, dev_nxt), OWN_P2: (chip, 1, dev_nxt), OWN_M1: (chip, 1, dev_prv), OWN_M2: (chip, 0, dev_prv),
               FW_P: (prv, 0, dev_nxt), FW_M: (nxt, 1, dev_prv),
               D0: (chip, None, dev_sib), D1: (prv, None, dev_sib), D2: (nxt, None, dev_sib), D3: (opp, None, dev_sib)}
    ag_got = {OWN_P1: (core, prv, 0), OWN_P2: (core, prv, 1), OWN_M1: (core, nxt, 1), OWN_M2: (core, nxt, 0),
              FW_P: (core, opp, 0), FW_M: (core, opp, 1),
              D0: (1 - core, chip, None), D1: (1 - core, prv, None), D2: (1 - core, nxt, None), D3: (1 - core, opp, None)}

    def msg_ag(t, kind):
        j, part, dev = ag_sent[kind]
        ref = ag_rows(t, core, j, part)
        return remote(ref, ref, t, kind, dev)

    def wait_ag(t, kind):
        ref = ag_rows(t, *ag_got[kind])
        remote(ref, ref, t, kind, dev_sib).wait_recv()

    def msg_stat(t, off):
        slot = lax.rem(t, SLOTS)
        return pltpu.make_async_remote_copy(src_ref=stats.at[slot, me], dst_ref=stats.at[slot, me], send_sem=ssend.at[slot, off],
                                            recv_sem=srecv.at[slot, me], device_id={'tp': lax.rem(me + off, tp_size)}, device_id_type=MESH)

    def in_proj(t):
        layer, row0 = where_of(t)

        @pl.when(layer == 0)
        def _():
            load_hid(t).wait()

        @pl.when(row0 == 0)
        def _():
            pre[0:HALO, :] = jnp.zeros((HALO, pre.shape[1]), F32)

        @pl.when(row0 > 0)
        def _():
            pre[0:HALO, :] = pre[CHUNK:CHUNK + HALO, :]

        def norm(load):
            def block(i, carry):
                r = pl.multiple_of(i * 32, 32)
                u = load(pl.multiple_of(row0 + r, 32))
                scale = lax.rsqrt(jnp.mean(u * u, axis=-1, keepdims=True) + EPSILON)
                h[pl.ds(r, 32), :] = (u * scale * nw[layer, 0:1, :]).astype(BF16)
                return carry
            lax.fori_loop(0, CHUNK // 32, block, 0)

        @pl.when(layer == 0)
        def _():
            norm(lambda r: hid[pl.ds(r, 32), :].astype(F32))

        @pl.when(layer > 0)
        def _():
            norm(lambda r: ures[jnp.maximum(layer - 1, 0), pl.ds(r, 32), :])

        wide = 2 * TILE

        def tile(i, carry):
            @pl.when(row0 == 0)
            def _():
                wait_in(layer, 2 * i)
                wait_in(layer, 2 * i + 1)
            o = pl.multiple_of(i * wide, wide)
            prod = jnp.dot(h[...], win[layer, :, pl.ds(o, wide)], preferred_element_type=F32)
            pre[HALO:HALO + CHUNK, pl.ds(o, wide)] = prod.astype(BF16).astype(F32)
            return carry
        lax.fori_loop(0, pre.shape[1] // wide, tile, 0)
        prod = lax.dot_general(h[...], wdt[layer], (((1,), (1,)), ((), ())), preferred_element_type=F32)
        dtp[:, 0:wdt.shape[1]] = prod.astype(BF16).astype(F32)

        @pl.when(t == 0)
        def _():
            load_out(0).start()
            for i in range(1, n_chunks):
                load_hid(i).start()

        @pl.when((row0 == CHUNK) & (layer < n_layers - 1))
        def _():
            for k in range(1, n_layers):
                @pl.when(layer == k - 1)
                def _():
                    for cp in load_in(k):
                        cp.start()
                    load_out(k).start()

    def mix(t):
        slot = lax.rem(t, SLOTS)
        layer, row0 = where_of(t)

        @pl.when(row0 == 0)
        def _():
            state[...] = jnp.zeros_like(state)
            state3[...] = jnp.zeros_like(state3)

        def conv(i, carry):
            o = pl.multiple_of(i * LANES, LANES)
            acc = jnp.broadcast_to(cw[layer, conv_width:conv_width + 1, pl.ds(o, LANES)], (CHUNK, LANES))
            for j in range(conv_width):
                first = HALO - (conv_width - 1) + j
                acc = acc + pre[first:first + CHUNK, pl.ds(pl.multiple_of(width + o, LANES), LANES)] * cw[layer, j:j + 1, pl.ds(o, LANES)]
            act[:, pl.ds(o, LANES)] = silu(acc)
            return carry
        lax.fori_loop(0, conv_ch // LANES, conv, 0)

        row_id = lax.broadcasted_iota(jnp.int32, (CHUNK, CHUNK), 0)
        col_id = lax.broadcasted_iota(jnp.int32, (CHUNK, CHUNK), 1)
        lower = row_id >= col_id
        left = col_id < head_dim
        left_row = left[0:1, :]
        dt = softplus(dtp[...] + hp[layer, 0:1, :])
        a = -dt * jnp.exp(hp[layer, 1:2, :])
        ones = jnp.where(lower, 1.0, 0.0).astype(BF16)
        a_cum = sum(fast_dot(ones, part) for part in reversed(split(a)))
        a_cum_t = a_cum.T
        a_last = a_cum[CHUNK - 1:CHUNK, :]
        zero = jnp.zeros((CHUNK, LANES), BF16)
        whole = jnp.exp(a_last)
        skip = hp[layer, 2:3, :]
        b = act[:, width:width + n_state]
        c1, c2, c3 = left_parts(act[:, width + n_state:conv_ch])
        bh, bm, bl = split(b)
        nt = (((1,), (1,)), ((), ()))
        b_mh = jnp.concatenate([bm, bh], axis=1)
        c_dot_b = (fast_dot(c3, jnp.concatenate([bh, bl], axis=1), nt) + fast_dot(c2, b_mh, nt)) + fast_dot(c1, b_mh, nt)
        c_dot_b = jnp.where(lower, c_dot_b, 0.0)
        b1, b2, b3 = left_parts(b.T)
        for o in range(0, width, TILE):
            cols = slice(o, min(o + TILE, width))
            v[:, cols] = three_dots(c1, c2, c3, state3, cols)
        sq = jnp.zeros((CHUNK, LANES), F32)
        for p in range(width // LANES):
            cols = slice(p * LANES, (p + 1) * LANES)
            h0, h1 = 2 * p, 2 * p + 1

            def spread(m):
                return jnp.where(left, m[:, h0:h0 + 1], m[:, h1:h1 + 1])

            def spread_row(m):
                return jnp.where(left_row, m[:, h0:h0 + 1], m[:, h1:h1 + 1])

            cum0 = jnp.broadcast_to(a_cum[:, h0:h0 + 1], (CHUNK, LANES))
            cum1 = jnp.broadcast_to(a_cum[:, h1:h1 + 1], (CHUNK, LANES))
            cum = jnp.where(left, cum0, cum1)

            def mixer(cum_rows, n):
                seg = cum_rows - a_cum_t[n:n + 1, :]
                return split(jnp.exp(jnp.minimum(seg, 0.0)) * c_dot_b)
            x = act[:, cols]
            x_dt = x * spread(dt)
            wh, wm, wl = split(x_dt * jnp.exp(spread_row(a_last) - cum))
            weighted3[0:CHUNK, cols] = wm
            weighted3[CHUNK:2 * CHUNK, cols] = wh
            weighted3[2 * CHUNK:3 * CHUNK, cols] = wl
            xh, xm, xl = (jnp.concatenate([jnp.where(left, part, zero), jnp.where(left, zero, part)], axis=0) for part in split(x_dt))
            mh, mm, ml = (jnp.concatenate(pair, axis=1) for pair in zip(mixer(cum0, h0), mixer(cum1, h1)))
            x_hm = jnp.concatenate([xh, xm], axis=1)
            wide = fast_dot(mm, x_hm) + fast_dot(mh, x_hm)
            y = (fast_dot(ml, xh) + fast_dot(mh, xl)) + wide[:, LANES:] + wide[:, :LANES]
            y = y + v[:, cols] * jnp.exp(cum)
            y = y + spread_row(skip) * x
            gated = y * silu(pre[HALO:HALO + CHUNK, cols])
            v[:, cols] = gated
            sq = sq + gated * gated
        total = jnp.sum(sq.T, axis=0, keepdims=True)
        stats[slot, me] = jnp.broadcast_to(total, (8, CHUNK))
        for off in range(1, tp_size):
            msg_stat(t, off).start()
        for o in range(0, width, TILE):
            cols = slice(o, min(o + TILE, width))
            decay = jnp.concatenate([jnp.where(left_row, whole[:, n:n + 1], whole[:, n + 1:n + 2])
                                     for n in range(o // head_dim, cols.stop // head_dim, 2)], axis=1)
            s_new = state[:, cols] * decay + three_dots(b1, b2, b3, weighted3, cols)
            state[:, cols] = s_new
            sh, sm, sl = split(s_new)
            state3[0:n_state, cols] = sm
            state3[n_state:2 * n_state, cols] = sh
            state3[2 * n_state:3 * n_state, cols] = sl

    def out_proj(t):
        slot = lax.rem(t, SLOTS)
        layer, row0 = where_of(t)

        @pl.when(row0 == 0)
        def _():
            load_out(layer).wait()
        for off in range(1, tp_size):
            peer = lax.rem(me + off, tp_size)
            pltpu.make_async_remote_copy(src_ref=stats.at[slot, peer], dst_ref=stats.at[slot, peer], send_sem=ssend.at[slot, off],
                                         recv_sem=srecv.at[slot, peer], device_id=dev_sib, device_id_type=MESH).wait_recv()
        for off in range(1, tp_size):
            msg_stat(t, off).wait_send()
        total = stats[slot, 0]
        for r in range(1, tp_size):
            total = total + stats[slot, r]
        scale = lax.rsqrt(total / inner_width + EPSILON)
        scale = jnp.broadcast_to(scale[0:1, :], (LANES, CHUNK)).T
        for p in range(width // LANES):
            cols = slice(p * LANES, (p + 1) * LANES)
            g[:, cols] = (v[:, cols] * scale * gw[layer, 0:1, cols]).astype(BF16)
        buf = pbuf.at[lax.rem(t, P_SLOTS)]

        def tile(i, carry):
            o = pl.multiple_of(i * TILE, TILE)
            buf[:, pl.ds(o, TILE)] = jnp.dot(g[...], wout[layer, :, pl.ds(o, TILE)], preferred_element_type=F32)
            return carry
        lax.fori_loop(0, d_model // TILE, tile, 0, unroll=True)
        msg_rs(t, SIB).start()

    def pair_sum(t):
        msg_rs(t, SIB).wait_recv()
        buf, other = pbuf.at[lax.rem(t, P_SLOTS)], sib.at[lax.rem(t, 2)]

        def block(i, carry):
            r = pl.multiple_of(i * 8, 8)
            mine = pl.ds(pl.multiple_of(core * half_rows + r, 8), 8)
            buf[mine, :] = buf[mine, :] + other[pl.ds(r, 8), :]
            return carry
        lax.fori_loop(0, half_rows // 8, block, 0)
        for kind in (FAR_P, FAR_M, NEAR_P, NEAR_M):
            msg_rs(t, kind).start()

    def relay_sum(t):
        slot = lax.rem(t, SLOTS)
        buf = pbuf.at[lax.rem(t, P_SLOTS)]
        for way, (wait, send, j, part) in enumerate(((FAR_P, COMB_P, nxt, 1), (FAR_M, COMB_M, prv, 0))):
            msg_rs(t, wait).wait_recv()
            rows = pl.ds(pl.multiple_of(slice_at(core, j) + part * piece, piece), piece)
            buf[rows, :] = buf[rows, :] + far[slot, way]
            msg_rs(t, send).start()

    def finish(t):
        slot = lax.rem(t, SLOTS)
        layer, row0 = where_of(t)
        buf = pbuf.at[lax.rem(t, P_SLOTS)]
        for kind in (NEAR_P, NEAR_M, COMB_P, COMB_M):
            msg_rs(t, kind).wait_recv()
        base = slice_at(core, chip)
        dst = pl.ds(pl.multiple_of(row0 + base, slice_rows), slice_rows)

        def store(res):
            lo = buf[pl.ds(base, piece), :] + near[slot, 0] + comb[slot, 1]
            hi = buf[pl.ds(pl.multiple_of(base + piece, piece), piece), :] + near[slot, 1] + comb[slot, 0]
            ures[layer, dst, :] = (res + jnp.concatenate([lo, hi], axis=0)).astype(BF16).astype(F32)

        @pl.when(layer == 0)
        def _():
            store(hid[dst, :].astype(F32))

        @pl.when(layer > 0)
        def _():
            store(ures[jnp.maximum(layer - 1, 0), dst, :])
        for kind in (OWN_P1, OWN_M1, OWN_P2, OWN_M2, D0):
            msg_ag(t, kind).start()
        for kind in (SIB, FAR_P, FAR_M, NEAR_P, NEAR_M, COMB_P, COMB_M):
            msg_rs(t, kind).wait_send()

    def forward(t):
        for wait, send in ((OWN_P1, FW_P), (OWN_M1, FW_M)):
            wait_ag(t, wait)
            msg_ag(t, send).start()

    def share(t):
        for waits, send in (((OWN_P2,), D1), ((OWN_M2,), D2), ((FW_P, FW_M), D3)):
            for kind in waits:
                wait_ag(t, kind)
            msg_ag(t, send).start()

    def collect(t):
        layer, row0 = where_of(t)
        for kind in (D0, D1, D2, D3):
            wait_ag(t, kind)
        for kind in ag_sent:
            msg_ag(t, kind).wait_send()

        @pl.when(layer == n_layers - 1)
        def _():
            def block(i, carry):
                rows = pl.ds(pl.multiple_of(row0 + i * 16, 16), 16)
                out[rows, :] = ures[layer, rows, :].astype(BF16)
                return carry
            lax.fori_loop(0, CHUNK // 16, block, 0)

    def guarded(step, t, first=0, last=n_tasks):
        @pl.when((t >= first) & (t < last))
        def _():
            step(t)

    final = n_tasks - n_chunks

    def iteration(t, carry):
        pl.when(t == -1)(widen)
        guarded(mix, t)
        guarded(pair_sum, t - 1)
        guarded(forward, t - 4)
        guarded(share, t - 5, last=final)
        guarded(collect, t - 5, last=final)
        guarded(in_proj, t + 1)
        guarded(finish, t - 2, last=final)
        guarded(out_proj, t)
        guarded(relay_sum, t - 1)
        guarded(finish, t - 2, first=final)
        guarded(share, t - 5, first=final)
        guarded(collect, t - 6, first=final)
        return carry
    lax.fori_loop(-1, n_tasks + 6, iteration, 0)


def layers(tp_size, hidden, norm_w, w_z, w_x, w_bc, w_dt, conv_x, conv_bc, bias_x, bias_bc, dt_bias, a_log, d_skip, gate_w, w_out):
    n_batch, n_steps, d_model = hidden.shape
    n_layers, conv_width, width = conv_x.shape
    head_rows = pl.cdiv(dt_bias.shape[-1], 16) * 16
    w_dt = jnp.transpose(w_dt, (2, 0, 1))
    state2 = w_bc.shape[-1]
    piece = CHUNK // tp_size // 2
    any_spec = pl.BlockSpec(memory_space=pl.ANY)
    dma = pltpu.SemaphoreType.DMA
    run = pl.pallas_call(
        functools.partial(kernel, tp_size, conv_width),
        out_shape=pltpu.VMEM((n_steps, d_model), BF16),
        in_specs=[any_spec] * 15,
        out_specs=pl.BlockSpec(memory_space=pltpu.VMEM),
        scratch_shapes=[pltpu.VMEM(p.shape, p.dtype) for p in (norm_w, w_dt, conv_x, conv_bc, bias_x, bias_bc, dt_bias, a_log, d_skip, gate_w)] + [
            pltpu.VMEM((n_steps, d_model), BF16),
            pltpu.VMEM((n_layers, d_model, 2 * width + state2), BF16),
            pltpu.VMEM((n_layers, head_rows, d_model), BF16),
            pltpu.VMEM((n_layers, head_rows, d_model), F32),
            pltpu.VMEM((n_layers, width, d_model), BF16),
            pltpu.VMEM((n_layers, n_steps, d_model), F32),
            pltpu.VMEM((CHUNK, d_model), BF16),
            pltpu.VMEM((HALO + CHUNK, 2 * width + state2), F32),
            pltpu.VMEM((CHUNK, width + state2), F32),
            pltpu.VMEM((CHUNK, width), F32),
            pltpu.VMEM((CHUNK, width), BF16),
            pltpu.VMEM((CHUNK, LANES), F32),
            pltpu.VMEM((state2 // 2, width), F32),
            pltpu.VMEM((3 * state2 // 2, width), BF16),
            pltpu.VMEM((3 * CHUNK, width), BF16),
            pltpu.VMEM((P_SLOTS, CHUNK, d_model), F32),
            pltpu.VMEM((2, CHUNK // 2, d_model), F32),
            pltpu.VMEM((SLOTS, 2, piece, d_model), F32),
            pltpu.VMEM((SLOTS, 2, piece, d_model), F32),
            pltpu.VMEM((SLOTS, 2, piece, d_model), F32),
            pltpu.VMEM((SLOTS, tp_size, 8, CHUNK), F32),
            pltpu.VMEM((n_layers, 8, d_model), F32),
            pltpu.VMEM((n_layers, 8, width + state2), F32),
            pltpu.VMEM((n_layers, 8, width), F32),
            pltpu.VMEM((n_layers, 8, LANES), F32),
            dma((n_layers, (2 * width + state2) // TILE + 1)), dma((n_steps // CHUNK,)), dma((10,)),
            dma((SLOTS, tp_size)), dma((SLOTS, tp_size)), dma((SEM_SLOTS, 17)), dma((SEM_SLOTS, 17)),
        ],
        compiler_params=pltpu.CompilerParams(collective_id=0, has_side_effects=True, vmem_limit_bytes=62_000_000),
    )
    outs = [run(hidden[i], norm_w, w_z, w_x, w_bc, w_dt, conv_x, conv_bc, bias_x, bias_bc, dt_bias, a_log, d_skip, gate_w, w_out)
            for i in range(n_batch)]
    return jnp.stack(outs)


def solution(mesh):
    col_spec = P(None, None, 'tp')
    vec_spec = P(None, 'tp')
    in_specs = (P('dp'), P(), col_spec, col_spec, P(), col_spec, col_spec, P(), vec_spec, P(), vec_spec, vec_spec, vec_spec, vec_spec, P(None, 'tp', None))
    return jax.shard_map(functools.partial(layers, mesh.shape['tp']), mesh=mesh, in_specs=in_specs, out_specs=P('dp'), check_vma=False)
```

```python
import functools

import jax
import jax.numpy as jnp
from jax import lax
from jax.experimental import pallas as pl
from jax.experimental.pallas import tpu as pltpu
from jax.sharding import PartitionSpec as P

EPSILON = 1e-5
F32 = jnp.float32
BF16 = jnp.bfloat16
MESH = pl.DeviceIdType.MESH
LANES = 128
CHUNK = 128
SLOTS = 4
SEM_SLOTS = 8
P_SLOTS = 3
HALO = 8
TILE = 256
(SIB, FAR_P, FAR_M, NEAR_P, NEAR_M, COMB_P, COMB_M, OWN_P1, OWN_P2, OWN_M1, OWN_M2, FW_P, FW_M, D0, D1, D2, D3) = range(17)


def fast_dot(a, b, dims=(((1,), (0,)), ((), ()))):
    return lax.dot_general(a, b, dims, preferred_element_type=F32)


def split(m):
    hi = m.astype(BF16)
    rest = m - hi.astype(F32)
    mid = rest.astype(BF16)
    return hi, mid, (rest - mid.astype(F32)).astype(BF16)


def left_parts(m):
    hi, mid, lo = split(m)
    return jnp.concatenate([hi, hi], axis=1), jnp.concatenate([mid, mid], axis=1), jnp.concatenate([lo, hi], axis=1)


def three_dots(p1, p2, p3, parts, cols):
    n = parts.shape[0] // 3
    upper = parts[0:2 * n, cols]
    return (fast_dot(p3, parts[n:3 * n, cols]) + fast_dot(p2, upper)) + fast_dot(p1, upper)


def silu(a):
    return a * (1.0 / (1.0 + jnp.exp(-a)))


def softplus(a):
    return jnp.maximum(a, 0.0) + jnp.log1p(jnp.exp(-jnp.abs(a)))


def kernel(tp_size, conv_width, hid_hbm, norm_hbm, wz_hbm, wx_hbm, wbc_hbm, wdt_hbm, convx_hbm, convbc_hbm, biasx_hbm, biasbc_hbm,
           dtb_hbm, alog_hbm, dskip_hbm, gate_hbm, wout_hbm, out,
           norm_in, wdt_in, convx_in, convbc_in, biasx_in, biasbc_in, dtb_in, alog_in, dskip_in, gate_in,
           hid, win, wdt, wdt_f, wout, ures, h, pre, act, v, g, dtp, state, state3, weighted3, pbuf, sib, far, near, comb, stats, nw, cw, gw, hp,
           wsem, hsem, psem, ssend, srecv, msend, mrecv):
    n_layers, n_steps, d_model = ures.shape
    width = v.shape[1]
    conv_ch = act.shape[1]
    n_state = (conv_ch - width) // 2
    n_heads = dtb_in.shape[1]
    head_dim = width // n_heads
    n_chunks = n_steps // CHUNK
    n_tasks = n_layers * n_chunks
    n_chips = tp_size // 2
    n_tiles = win.shape[2] // TILE
    half_rows = CHUNK // 2
    slice_rows = half_rows // n_chips
    piece = slice_rows // 2
    inner_width = width * tp_size

    me = lax.axis_index('tp')
    chip = me // 2
    core = lax.rem(me, 2)
    nxt = lax.rem(chip + 1, n_chips)
    prv = lax.rem(chip + n_chips - 1, n_chips)
    opp = lax.rem(chip + 2, n_chips)
    dev_nxt = {'tp': nxt * 2 + core}
    dev_prv = {'tp': prv * 2 + core}
    dev_sib = {'tp': chip * 2 + 1 - core}

    barrier = pltpu.get_barrier_semaphore()
    for off in range(1, tp_size):
        pl.semaphore_signal(barrier, inc=1, device_id={'tp': lax.rem(me + off, tp_size)}, device_id_type=MESH)

    def load_hid(i):
        rows = pl.ds(pl.multiple_of(i * CHUNK, CHUNK), CHUNK)
        return pltpu.make_async_copy(hid_hbm.at[rows], hid.at[rows], hsem.at[i])

    def load_in(layer):
        copies = []
        for w_hbm, first, n_cols in ((wz_hbm, 0, width), (wx_hbm, width, width), (wbc_hbm, 2 * width, 2 * n_state)):
            done = 0
            while done < n_cols:
                n = min(TILE - (first + done) % TILE, n_cols - done)
                at = first + done
                copies.append(pltpu.make_async_copy(w_hbm.at[layer, :, pl.ds(done, n)], win.at[layer, :, pl.ds(at, n)],
                                                    wsem.at[layer, at // TILE]))
                done += n
        return copies

    def wait_in(layer, tile):
        ref = win.at[layer, :, pl.ds(pl.multiple_of(tile * TILE, TILE), TILE)]
        pltpu.make_async_copy(ref, ref, wsem.at[layer, tile]).wait()

    def load_out(layer):
        return pltpu.make_async_copy(wout_hbm.at[layer], wout.at[layer], wsem.at[layer, n_tiles])

    params = ((norm_hbm, norm_in), (wdt_hbm, wdt_in), (convx_hbm, convx_in), (convbc_hbm, convbc_in), (biasx_hbm, biasx_in),
              (biasbc_hbm, biasbc_in), (dtb_hbm, dtb_in), (alog_hbm, alog_in), (dskip_hbm, dskip_in), (gate_hbm, gate_in))
    small = [pltpu.make_async_copy(src, dst, psem.at[i]) for i, (src, dst) in enumerate(params)]
    load_hid(0).start()
    for cp in small:
        cp.start()
    for cp in load_in(0):
        cp.start()
    small[0].wait()
    for layer in range(n_layers):
        nw[layer, 0:1, :] = norm_in[layer:layer + 1, :].astype(F32)

    def widen():
        for cp in small[1:]:
            cp.wait()
        hp[...] = jnp.zeros_like(hp)
        wdt_f[...] = jnp.zeros_like(wdt_f)
        for n in range(n_heads):
            cols = wdt_in[n].astype(F32)
            for layer in range(n_layers):
                wdt_f[layer, n:n + 1, :] = cols[layer:layer + 1, :]
        wdt[...] = wdt_f[...].astype(BF16)
        dtp[...] = jnp.zeros_like(dtp)
        for layer in range(n_layers):
            gw[layer, 0:1, :] = gate_in[layer:layer + 1, :].astype(F32)
            cw[layer, 0:conv_width, 0:width] = convx_in[layer].astype(F32)
            cw[layer, 0:conv_width, width:conv_ch] = convbc_in[layer].astype(F32)
            cw[layer, conv_width:conv_width + 1, 0:width] = biasx_in[layer:layer + 1, :].astype(F32)
            cw[layer, conv_width:conv_width + 1, width:conv_ch] = biasbc_in[layer:layer + 1, :].astype(F32)
            hp[layer, 0:1, 0:n_heads] = dtb_in[layer:layer + 1, :]
            hp[layer, 1:2, 0:n_heads] = alog_in[layer:layer + 1, :]
            hp[layer, 2:3, 0:n_heads] = dskip_in[layer:layer + 1, :]

    pl.semaphore_wait(barrier, tp_size - 1)

    def where_of(t):
        layer = sum(jnp.where(t >= k * n_chunks, 1, 0) for k in range(1, n_layers))
        return layer, pl.multiple_of((t - layer * n_chunks) * CHUNK, CHUNK)

    def remote(src, dst, t, kind, dev):
        slot = lax.rem(t, SEM_SLOTS)
        return pltpu.make_async_remote_copy(src_ref=src, dst_ref=dst, send_sem=msend.at[slot, kind], recv_sem=mrecv.at[slot, kind],
                                            device_id=dev, device_id_type=MESH)

    def slice_at(c, j):
        return pl.multiple_of(c * half_rows + j * slice_rows, slice_rows)

    def msg_rs(t, kind):
        slot = lax.rem(t, SLOTS)
        buf = pbuf.at[lax.rem(t, P_SLOTS)]

        def src(j, part):
            return buf.at[pl.ds(pl.multiple_of(slice_at(core, j) + part * piece, piece), piece)]
        if kind == SIB:
            other = pl.multiple_of((1 - core) * half_rows, half_rows)
            return remote(buf.at[pl.ds(other, half_rows)], sib.at[lax.rem(t, 2)], t, kind, dev_sib)
        if kind == FAR_P:
            return remote(src(opp, 1), far.at[slot, 0], t, kind, dev_nxt)
        if kind == FAR_M:
            return remote(src(opp, 0), far.at[slot, 1], t, kind, dev_prv)
        if kind == NEAR_P:
            return remote(src(nxt, 0), near.at[slot, 0], t, kind, dev_nxt)
        if kind == NEAR_M:
            return remote(src(prv, 1), near.at[slot, 1], t, kind, dev_prv)
        if kind == COMB_P:
            return remote(src(nxt, 1), comb.at[slot, 0], t, kind, dev_nxt)
        return remote(src(prv, 0), comb.at[slot, 1], t, kind, dev_prv)

    def ag_rows(t, c, j, part=None):
        layer, row0 = where_of(t)
        base = row0 + slice_at(c, j)
        if part is None:
            return ures.at[layer, pl.ds(pl.multiple_of(base, slice_rows), slice_rows)]
        return ures.at[layer, pl.ds(pl.multiple_of(base + part * piece, piece), piece)]

    ag_sent = {OWN_P1: (chip, 0, dev_nxt), OWN_P2: (chip, 1, dev_nxt), OWN_M1: (chip, 1, dev_prv), OWN_M2: (chip, 0, dev_prv),
               FW_P: (prv, 0, dev_nxt), FW_M: (nxt, 1, dev_prv),
               D0: (chip, None, dev_sib), D1: (prv, None, dev_sib), D2: (nxt, None, dev_sib), D3: (opp, None, dev_sib)}
    ag_got = {OWN_P1: (core, prv, 0), OWN_P2: (core, prv, 1), OWN_M1: (core, nxt, 1), OWN_M2: (core, nxt, 0),
              FW_P: (core, opp, 0), FW_M: (core, opp, 1),
              D0: (1 - core, chip, None), D1: (1 - core, prv, None), D2: (1 - core, nxt, None), D3: (1 - core, opp, None)}

    def msg_ag(t, kind):
        j, part, dev = ag_sent[kind]
        ref = ag_rows(t, core, j, part)
        return remote(ref, ref, t, kind, dev)

    def wait_ag(t, kind):
        ref = ag_rows(t, *ag_got[kind])
        remote(ref, ref, t, kind, dev_sib).wait_recv()

    def msg_stat(t, off):
        slot = lax.rem(t, SLOTS)
        return pltpu.make_async_remote_copy(src_ref=stats.at[slot, me], dst_ref=stats.at[slot, me], send_sem=ssend.at[slot, off],
                                            recv_sem=srecv.at[slot, me], device_id={'tp': lax.rem(me + off, tp_size)}, device_id_type=MESH)

    def in_proj(t):
        layer, row0 = where_of(t)

        @pl.when(layer == 0)
        def _():
            load_hid(t).wait()

        @pl.when(row0 == 0)
        def _():
            pre[:, 0:HALO, :] = jnp.zeros((pre.shape[0], HALO, LANES), F32)

        @pl.when(row0 > 0)
        def _():
            pre[:, 0:HALO, :] = pre[:, CHUNK:CHUNK + HALO, :]

        def norm(load):
            def block(i, carry):
                r = pl.multiple_of(i * 32, 32)
                u = load(pl.multiple_of(row0 + r, 32))
                scale = lax.rsqrt(jnp.mean(u * u, axis=-1, keepdims=True) + EPSILON)
                h[pl.ds(r, 32), :] = (u * scale * nw[layer, 0:1, :]).astype(BF16)
                return carry
            lax.fori_loop(0, CHUNK // 32, block, 0)

        @pl.when(layer == 0)
        def _():
            norm(lambda r: hid[pl.ds(r, 32), :].astype(F32))

        @pl.when(layer > 0)
        def _():
            norm(lambda r: ures[jnp.maximum(layer - 1, 0), pl.ds(r, 32), :])

        wide = 2 * TILE

        def tile(i, carry):
            @pl.when(row0 == 0)
            def _():
                wait_in(layer, 2 * i)
                wait_in(layer, 2 * i + 1)
            o = pl.multiple_of(i * wide, wide)
            prod = jnp.dot(h[...], win[layer, :, pl.ds(o, wide)], preferred_element_type=F32)
            prod = prod.astype(BF16).astype(F32)
            for j in range(wide // LANES):
                pre[i * (wide // LANES) + j, HALO:HALO + CHUNK, :] = prod[:, j * LANES:(j + 1) * LANES]
            return carry
        lax.fori_loop(0, n_tiles // 2, tile, 0)
        prod = lax.dot_general(h[...], wdt[layer], (((1,), (1,)), ((), ())), preferred_element_type=F32)
        dtp[:, 0:wdt.shape[1]] = prod.astype(BF16).astype(F32)

        @pl.when(t == 0)
        def _():
            load_out(0).start()
            for i in range(1, n_chunks):
                load_hid(i).start()

        @pl.when((row0 == CHUNK) & (layer < n_layers - 1))
        def _():
            for k in range(1, n_layers):
                @pl.when(layer == k - 1)
                def _():
                    for cp in load_in(k):
                        cp.start()
                    load_out(k).start()

    def mix(t):
        slot = lax.rem(t, SLOTS)
        layer, row0 = where_of(t)

        @pl.when(row0 == 0)
        def _():
            state[...] = jnp.zeros_like(state)
            state3[...] = jnp.zeros_like(state3)

        def conv(i, carry):
            o = pl.multiple_of(i * LANES, LANES)
            acc = jnp.broadcast_to(cw[layer, conv_width:conv_width + 1, pl.ds(o, LANES)], (CHUNK, LANES))
            for j in range(conv_width):
                first = HALO - (conv_width - 1) + j
                acc = acc + pre[width // LANES + i, first:first + CHUNK, :] * cw[layer, j:j + 1, pl.ds(o, LANES)]
            act[:, pl.ds(o, LANES)] = silu(acc)
            return carry
        lax.fori_loop(0, conv_ch // LANES, conv, 0, unroll=True)

        row_id = lax.broadcasted_iota(jnp.int32, (CHUNK, CHUNK), 0)
        col_id = lax.broadcasted_iota(jnp.int32, (CHUNK, CHUNK), 1)
        lower = row_id >= col_id
        left = col_id < head_dim
        left_row = left[0:1, :]
        dt = softplus(dtp[...] + hp[layer, 0:1, :])
        a = -dt * jnp.exp(hp[layer, 1:2, :])
        ones = jnp.where(lower, 1.0, 0.0).astype(BF16)
        a_cum = sum(fast_dot(ones, part) for part in reversed(split(a)))
        a_cum_t = a_cum.T
        a_last = a_cum[CHUNK - 1:CHUNK, :]
        zero = jnp.zeros((CHUNK, LANES), BF16)
        whole = jnp.exp(a_last)
        skip = hp[layer, 2:3, :]
        b = act[:, width:width + n_state]
        c1, c2, c3 = left_parts(act[:, width + n_state:conv_ch])
        bh, bm, bl = split(b)
        nt = (((1,), (1,)), ((), ()))
        b_mh = jnp.concatenate([bm, bh], axis=1)
        c_dot_b = (fast_dot(c3, jnp.concatenate([bh, bl], axis=1), nt) + fast_dot(c2, b_mh, nt)) + fast_dot(c1, b_mh, nt)
        c_dot_b = jnp.where(lower, c_dot_b, 0.0)
        b1, b2, b3 = left_parts(b.T)
        for o in range(0, width, TILE):
            cols = slice(o, min(o + TILE, width))
            v[:, cols] = three_dots(c1, c2, c3, state3, cols)
        sq = jnp.zeros((CHUNK, LANES), F32)
        for p in range(width // LANES):
            cols = slice(p * LANES, (p + 1) * LANES)
            h0, h1 = 2 * p, 2 * p + 1

            def spread(m):
                return jnp.where(left, m[:, h0:h0 + 1], m[:, h1:h1 + 1])

            def spread_row(m):
                return jnp.where(left_row, m[:, h0:h0 + 1], m[:, h1:h1 + 1])

            cum0 = jnp.broadcast_to(a_cum[:, h0:h0 + 1], (CHUNK, LANES))
            cum1 = jnp.broadcast_to(a_cum[:, h1:h1 + 1], (CHUNK, LANES))
            cum = jnp.where(left, cum0, cum1)

            def mixer(cum_rows, n):
                seg = cum_rows - a_cum_t[n:n + 1, :]
                return split(jnp.exp(jnp.minimum(seg, 0.0)) * c_dot_b)
            x = act[:, cols]
            x_dt = x * spread(dt)
            wh, wm, wl = split(x_dt * jnp.exp(spread_row(a_last) - cum))
            weighted3[0:CHUNK, cols] = wm
            weighted3[CHUNK:2 * CHUNK, cols] = wh
            weighted3[2 * CHUNK:3 * CHUNK, cols] = wl
            xh, xm, xl = (jnp.concatenate([jnp.where(left, part, zero), jnp.where(left, zero, part)], axis=0) for part in split(x_dt))
            mh, mm, ml = (jnp.concatenate(pair, axis=1) for pair in zip(mixer(cum0, h0), mixer(cum1, h1)))
            x_hm = jnp.concatenate([xh, xm], axis=1)
            wide = fast_dot(mm, x_hm) + fast_dot(mh, x_hm)
            y = (fast_dot(ml, xh) + fast_dot(mh, xl)) + wide[:, LANES:] + wide[:, :LANES]
            y = y + v[:, cols] * jnp.exp(cum)
            y = y + spread_row(skip) * x
            gated = y * silu(pre[p, HALO:HALO + CHUNK, :])
            v[:, cols] = gated
            sq = sq + gated * gated
        total = jnp.sum(sq.T, axis=0, keepdims=True)
        stats[slot, me] = jnp.broadcast_to(total, (8, CHUNK))
        for off in range(1, tp_size):
            msg_stat(t, off).start()
        for o in range(0, width, TILE):
            cols = slice(o, min(o + TILE, width))
            decay = jnp.concatenate([jnp.where(left_row, whole[:, n:n + 1], whole[:, n + 1:n + 2])
                                     for n in range(o // head_dim, cols.stop // head_dim, 2)], axis=1)
            s_new = state[:, cols] * decay + three_dots(b1, b2, b3, weighted3, cols)
            state[:, cols] = s_new
            sh, sm, sl = split(s_new)
            state3[0:n_state, cols] = sm
            state3[n_state:2 * n_state, cols] = sh
            state3[2 * n_state:3 * n_state, cols] = sl

    def out_proj(t):
        slot = lax.rem(t, SLOTS)
        layer, row0 = where_of(t)

        @pl.when(row0 == 0)
        def _():
            load_out(layer).wait()
        for off in range(1, tp_size):
            peer = lax.rem(me + off, tp_size)
            pltpu.make_async_remote_copy(src_ref=stats.at[slot, peer], dst_ref=stats.at[slot, peer], send_sem=ssend.at[slot, off],
                                         recv_sem=srecv.at[slot, peer], device_id=dev_sib, device_id_type=MESH).wait_recv()
        for off in range(1, tp_size):
            msg_stat(t, off).wait_send()
        total = stats[slot, 0]
        for r in range(1, tp_size):
            total = total + stats[slot, r]
        scale = lax.rsqrt(total / inner_width + EPSILON)
        scale = jnp.broadcast_to(scale[0:1, :], (LANES, CHUNK)).T
        for p in range(width // LANES):
            cols = slice(p * LANES, (p + 1) * LANES)
            g[:, cols] = (v[:, cols] * scale * gw[layer, 0:1, cols]).astype(BF16)
        buf = pbuf.at[lax.rem(t, P_SLOTS)]

        def tile(i, carry):
            o = pl.multiple_of(i * TILE, TILE)
            buf[:, pl.ds(o, TILE)] = jnp.dot(g[...], wout[layer, :, pl.ds(o, TILE)], preferred_element_type=F32)
            return carry
        lax.fori_loop(0, d_model // TILE, tile, 0, unroll=True)
        msg_rs(t, SIB).start()

    def pair_sum(t):
        msg_rs(t, SIB).wait_recv()
        buf, other = pbuf.at[lax.rem(t, P_SLOTS)], sib.at[lax.rem(t, 2)]

        def block(i, carry):
            r = pl.multiple_of(i * 8, 8)
            mine = pl.ds(pl.multiple_of(core * half_rows + r, 8), 8)
            buf[mine, :] = buf[mine, :] + other[pl.ds(r, 8), :]
            return carry
        lax.fori_loop(0, half_rows // 8, block, 0)
        for kind in (FAR_P, FAR_M, NEAR_P, NEAR_M):
            msg_rs(t, kind).start()

    def relay_sum(t):
        slot = lax.rem(t, SLOTS)
        buf = pbuf.at[lax.rem(t, P_SLOTS)]
        for way, (wait, send, j, part) in enumerate(((FAR_P, COMB_P, nxt, 1), (FAR_M, COMB_M, prv, 0))):
            msg_rs(t, wait).wait_recv()
            rows = pl.ds(pl.multiple_of(slice_at(core, j) + part * piece, piece), piece)
            buf[rows, :] = buf[rows, :] + far[slot, way]
            msg_rs(t, send).start()

    def finish(t):
        slot = lax.rem(t, SLOTS)
        layer, row0 = where_of(t)
        buf = pbuf.at[lax.rem(t, P_SLOTS)]
        for kind in (NEAR_P, NEAR_M, COMB_P, COMB_M):
            msg_rs(t, kind).wait_recv()
        base = slice_at(core, chip)
        dst = pl.ds(pl.multiple_of(row0 + base, slice_rows), slice_rows)

        def store(res):
            lo = buf[pl.ds(base, piece), :] + near[slot, 0] + comb[slot, 1]
            hi = buf[pl.ds(pl.multiple_of(base + piece, piece), piece), :] + near[slot, 1] + comb[slot, 0]
            ures[layer, dst, :] = (res + jnp.concatenate([lo, hi], axis=0)).astype(BF16).astype(F32)

        @pl.when(layer == 0)
        def _():
            store(hid[dst, :].astype(F32))

        @pl.when(layer > 0)
        def _():
            store(ures[jnp.maximum(layer - 1, 0), dst, :])
        for kind in (OWN_P1, OWN_M1, OWN_P2, OWN_M2, D0):
            msg_ag(t, kind).start()
        for kind in (SIB, FAR_P, FAR_M, NEAR_P, NEAR_M, COMB_P, COMB_M):
            msg_rs(t, kind).wait_send()

    def forward(t):
        for wait, send in ((OWN_P1, FW_P), (OWN_M1, FW_M)):
            wait_ag(t, wait)
            msg_ag(t, send).start()

    def share(t):
        for waits, send in (((OWN_P2,), D1), ((OWN_M2,), D2), ((FW_P, FW_M), D3)):
            for kind in waits:
                wait_ag(t, kind)
            msg_ag(t, send).start()

    def collect(t):
        layer, row0 = where_of(t)
        for kind in (D0, D1, D2, D3):
            wait_ag(t, kind)
        for kind in ag_sent:
            msg_ag(t, kind).wait_send()

        @pl.when(layer == n_layers - 1)
        def _():
            def block(i, carry):
                rows = pl.ds(pl.multiple_of(row0 + i * 16, 16), 16)
                out[rows, :] = ures[layer, rows, :].astype(BF16)
                return carry
            lax.fori_loop(0, CHUNK // 16, block, 0)

    def guarded(step, t, first=0, last=n_tasks):
        @pl.when((t >= first) & (t < last))
        def _():
            step(t)

    final = n_tasks - n_chunks

    def iteration(t, carry):
        pl.when(t == -1)(widen)
        guarded(mix, t)
        guarded(pair_sum, t - 1)
        guarded(forward, t - 4)
        guarded(share, t - 5, last=final)
        guarded(collect, t - 5, last=final)
        guarded(in_proj, t + 1)
        guarded(finish, t - 2, last=final)
        guarded(out_proj, t)
        guarded(relay_sum, t - 1)
        guarded(finish, t - 2, first=final)
        guarded(share, t - 5, first=final)
        guarded(collect, t - 6, first=final)
        return carry
    lax.fori_loop(-1, n_tasks + 6, iteration, 0)


def write_kernel(src, dst, sem):
    rows = src.shape[0] // sem.shape[0]
    copies = [pltpu.make_async_copy(src.at[pl.ds(i * rows, rows)], dst.at[pl.ds(i * rows, rows)], sem.at[i]) for i in range(sem.shape[0])]
    for cp in copies:
        cp.start()
    for cp in copies:
        cp.wait()


def layers(tp_size, hidden, norm_w, w_z, w_x, w_bc, w_dt, conv_x, conv_bc, bias_x, bias_bc, dt_bias, a_log, d_skip, gate_w, w_out):
    n_batch, n_steps, d_model = hidden.shape
    n_layers, conv_width, width = conv_x.shape
    head_rows = pl.cdiv(dt_bias.shape[-1], 16) * 16
    w_dt = jnp.transpose(w_dt, (2, 0, 1))
    state2 = w_bc.shape[-1]
    piece = CHUNK // tp_size // 2
    any_spec = pl.BlockSpec(memory_space=pl.ANY)
    dma = pltpu.SemaphoreType.DMA
    run = pl.pallas_call(
        functools.partial(kernel, tp_size, conv_width),
        out_shape=pltpu.VMEM((n_steps, d_model), BF16),
        in_specs=[any_spec] * 15,
        out_specs=pl.BlockSpec(memory_space=pltpu.VMEM),
        scratch_shapes=[pltpu.VMEM(p.shape, p.dtype) for p in (norm_w, w_dt, conv_x, conv_bc, bias_x, bias_bc, dt_bias, a_log, d_skip, gate_w)] + [
            pltpu.VMEM((n_steps, d_model), BF16),
            pltpu.VMEM((n_layers, d_model, 2 * width + state2), BF16),
            pltpu.VMEM((n_layers, head_rows, d_model), BF16),
            pltpu.VMEM((n_layers, head_rows, d_model), F32),
            pltpu.VMEM((n_layers, width, d_model), BF16),
            pltpu.VMEM((n_layers, n_steps, d_model), F32),
            pltpu.VMEM((CHUNK, d_model), BF16),
            pltpu.VMEM(((2 * width + state2) // LANES, HALO + CHUNK, LANES), F32),
            pltpu.VMEM((CHUNK, width + state2), F32),
            pltpu.VMEM((CHUNK, width), F32),
            pltpu.VMEM((CHUNK, width), BF16),
            pltpu.VMEM((CHUNK, LANES), F32),
            pltpu.VMEM((state2 // 2, width), F32),
            pltpu.VMEM((3 * state2 // 2, width), BF16),
            pltpu.VMEM((3 * CHUNK, width), BF16),
            pltpu.VMEM((P_SLOTS, CHUNK, d_model), F32),
            pltpu.VMEM((2, CHUNK // 2, d_model), F32),
            pltpu.VMEM((SLOTS, 2, piece, d_model), F32),
            pltpu.VMEM((SLOTS, 2, piece, d_model), F32),
            pltpu.VMEM((SLOTS, 2, piece, d_model), F32),
            pltpu.VMEM((SLOTS, tp_size, 8, CHUNK), F32),
            pltpu.VMEM((n_layers, 8, d_model), F32),
            pltpu.VMEM((n_layers, 8, width + state2), F32),
            pltpu.VMEM((n_layers, 8, width), F32),
            pltpu.VMEM((n_layers, 8, LANES), F32),
            dma((n_layers, (2 * width + state2) // TILE + 1)), dma((n_steps // CHUNK,)), dma((10,)),
            dma((SLOTS, tp_size)), dma((SLOTS, tp_size)), dma((SEM_SLOTS, 17)), dma((SEM_SLOTS, 17)),
        ],
        compiler_params=pltpu.CompilerParams(collective_id=0, has_side_effects=True, vmem_limit_bytes=62_000_000),
    )
    outs = [run(hidden[i], norm_w, w_z, w_x, w_bc, w_dt, conv_x, conv_bc, bias_x, bias_bc, dt_bias, a_log, d_skip, gate_w, w_out)
            for i in range(n_batch)]
    write = pl.pallas_call(
        write_kernel,
        out_shape=jax.ShapeDtypeStruct((n_steps, d_model), BF16),
        in_specs=[any_spec],
        out_specs=any_spec,
        scratch_shapes=[dma((n_steps // CHUNK,))],
        compiler_params=pltpu.CompilerParams(vmem_limit_bytes=1 << 20),
    )
    return jnp.stack([write(out) for out in outs])


def solution(mesh):
    col_spec = P(None, None, 'tp')
    vec_spec = P(None, 'tp')
    in_specs = (P('dp'), P(), col_spec, col_spec, P(), col_spec, col_spec, P(), vec_spec, P(), vec_spec, vec_spec, vec_spec, vec_spec, P(None, 'tp', None))
    return jax.shard_map(functools.partial(layers, mesh.shape['tp']), mesh=mesh, in_specs=in_specs, out_specs=P('dp'), check_vma=False)
```

```python
import functools

import jax
import jax.numpy as jnp
from jax import lax
from jax.experimental import pallas as pl
from jax.experimental.pallas import tpu as pltpu
from jax.sharding import PartitionSpec as P

EPSILON = 1e-5
F32 = jnp.float32
BF16 = jnp.bfloat16
MESH = pl.DeviceIdType.MESH
LANES = 128
CHUNK = 128
SLOTS = 4
SEM_SLOTS = 8
P_SLOTS = 3
HALO = 8
TILE = 256
(SIB, FAR_P, FAR_M, NEAR_P, NEAR_M, COMB_P, COMB_M, OWN_P1, OWN_P2, OWN_M1, OWN_M2, FW_P, FW_M, D0, D1, D2, D3) = range(17)


def fast_dot(a, b, dims=(((1,), (0,)), ((), ()))):
    return lax.dot_general(a, b, dims, preferred_element_type=F32)


def split(m):
    hi = m.astype(BF16)
    rest = m - hi.astype(F32)
    mid = rest.astype(BF16)
    return hi, mid, (rest - mid.astype(F32)).astype(BF16)


def left_parts(m):
    hi, mid, lo = split(m)
    return jnp.concatenate([hi, hi], axis=1), jnp.concatenate([mid, mid], axis=1), jnp.concatenate([lo, hi], axis=1)


def three_dots(p1, p2, p3, parts, cols):
    n = parts.shape[0] // 3
    upper = parts[0:2 * n, cols]
    return (fast_dot(p3, parts[n:3 * n, cols]) + fast_dot(p2, upper)) + fast_dot(p1, upper)


def silu(a):
    return a * (1.0 / (1.0 + jnp.exp(-a)))


def softplus(a):
    return jnp.maximum(a, 0.0) + jnp.log1p(jnp.exp(-jnp.abs(a)))


def kernel(tp_size, conv_width, hid_hbm, norm_hbm, wz_hbm, wx_hbm, wbc_hbm, wdt_hbm, convx_hbm, convbc_hbm, biasx_hbm, biasbc_hbm,
           dtb_hbm, alog_hbm, dskip_hbm, gate_hbm, wout_hbm, out,
           norm_in, wdt_in, convx_in, convbc_in, biasx_in, biasbc_in, dtb_in, alog_in, dskip_in, gate_in,
           hid, win, wdt, wdt_f, wout, ures, h, pre, act, v, g, dtp, state, state3, weighted3, pbuf, sib, far, near, comb, stats, nw, cw, gw, hp,
           wsem, hsem, psem, ssend, srecv, msend, mrecv):
    n_layers, n_steps, d_model = ures.shape
    width = v.shape[1]
    conv_ch = act.shape[1]
    n_state = (conv_ch - width) // 2
    n_heads = dtb_in.shape[1]
    head_dim = width // n_heads
    n_chunks = n_steps // CHUNK
    n_tasks = n_layers * n_chunks
    n_chips = tp_size // 2
    n_tiles = win.shape[2] // TILE
    half_rows = CHUNK // 2
    slice_rows = half_rows // n_chips
    piece = slice_rows // 2
    inner_width = width * tp_size

    me = lax.axis_index('tp')
    chip = me // 2
    core = lax.rem(me, 2)
    nxt = lax.rem(chip + 1, n_chips)
    prv = lax.rem(chip + n_chips - 1, n_chips)
    opp = lax.rem(chip + 2, n_chips)
    dev_nxt = {'tp': nxt * 2 + core}
    dev_prv = {'tp': prv * 2 + core}
    dev_sib = {'tp': chip * 2 + 1 - core}

    barrier = pltpu.get_barrier_semaphore()
    for off in range(1, tp_size):
        pl.semaphore_signal(barrier, inc=1, device_id={'tp': lax.rem(me + off, tp_size)}, device_id_type=MESH)

    def load_hid(i):
        rows = pl.ds(pl.multiple_of(i * CHUNK, CHUNK), CHUNK)
        return pltpu.make_async_copy(hid_hbm.at[rows], hid.at[rows], hsem.at[i])

    def load_in(layer):
        copies = []
        for w_hbm, first, n_cols in ((wz_hbm, 0, width), (wx_hbm, width, width), (wbc_hbm, 2 * width, 2 * n_state)):
            done = 0
            while done < n_cols:
                n = min(TILE - (first + done) % TILE, n_cols - done)
                at = first + done
                copies.append(pltpu.make_async_copy(w_hbm.at[layer, :, pl.ds(done, n)], win.at[layer, :, pl.ds(at, n)],
                                                    wsem.at[layer, at // TILE]))
                done += n
        return copies

    def wait_in(layer, tile):
        ref = win.at[layer, :, pl.ds(pl.multiple_of(tile * TILE, TILE), TILE)]
        pltpu.make_async_copy(ref, ref, wsem.at[layer, tile]).wait()

    def load_out(layer):
        return pltpu.make_async_copy(wout_hbm.at[layer], wout.at[layer], wsem.at[layer, n_tiles])

    params = ((norm_hbm, norm_in), (wdt_hbm, wdt_in), (convx_hbm, convx_in), (convbc_hbm, convbc_in), (biasx_hbm, biasx_in),
              (biasbc_hbm, biasbc_in), (dtb_hbm, dtb_in), (alog_hbm, alog_in), (dskip_hbm, dskip_in), (gate_hbm, gate_in))
    small = [pltpu.make_async_copy(src, dst, psem.at[i]) for i, (src, dst) in enumerate(params)]
    load_hid(0).start()
    for cp in small:
        cp.start()
    for cp in load_in(0):
        cp.start()
    small[0].wait()
    for layer in range(n_layers):
        nw[layer, 0:1, :] = norm_in[layer:layer + 1, :].astype(F32)

    def widen():
        for cp in small[1:]:
            cp.wait()
        hp[...] = jnp.zeros_like(hp)
        wdt_f[...] = jnp.zeros_like(wdt_f)
        for n in range(n_heads):
            cols = wdt_in[n].astype(F32)
            for layer in range(n_layers):
                wdt_f[layer, n:n + 1, :] = cols[layer:layer + 1, :]
        wdt[...] = wdt_f[...].astype(BF16)
        dtp[...] = jnp.zeros_like(dtp)
        for layer in range(n_layers):
            gw[layer, 0:1, :] = gate_in[layer:layer + 1, :].astype(F32)
            cw[layer, 0:conv_width, 0:width] = convx_in[layer].astype(F32)
            cw[layer, 0:conv_width, width:conv_ch] = convbc_in[layer].astype(F32)
            cw[layer, conv_width:conv_width + 1, 0:width] = biasx_in[layer:layer + 1, :].astype(F32)
            cw[layer, conv_width:conv_width + 1, width:conv_ch] = biasbc_in[layer:layer + 1, :].astype(F32)
            hp[layer, 0:1, 0:n_heads] = dtb_in[layer:layer + 1, :]
            hp[layer, 1:2, 0:n_heads] = alog_in[layer:layer + 1, :]
            hp[layer, 2:3, 0:n_heads] = dskip_in[layer:layer + 1, :]

    pl.semaphore_wait(barrier, tp_size - 1)

    def where_of(t):
        layer = sum(jnp.where(t >= k * n_chunks, 1, 0) for k in range(1, n_layers))
        return layer, pl.multiple_of((t - layer * n_chunks) * CHUNK, CHUNK)

    def remote(src, dst, t, kind, dev):
        slot = lax.rem(t, SEM_SLOTS)
        return pltpu.make_async_remote_copy(src_ref=src, dst_ref=dst, send_sem=msend.at[slot, kind], recv_sem=mrecv.at[slot, kind],
                                            device_id=dev, device_id_type=MESH)

    def slice_at(c, j):
        return pl.multiple_of(c * half_rows + j * slice_rows, slice_rows)

    def msg_rs(t, kind):
        slot = lax.rem(t, SLOTS)
        buf = pbuf.at[lax.rem(t, P_SLOTS)]

        def src(j, part):
            return buf.at[pl.ds(pl.multiple_of(slice_at(core, j) + part * piece, piece), piece)]
        if kind == SIB:
            other = pl.multiple_of((1 - core) * half_rows, half_rows)
            return remote(buf.at[pl.ds(other, half_rows)], sib.at[lax.rem(t, 2)], t, kind, dev_sib)
        if kind == FAR_P:
            return remote(src(opp, 1), far.at[slot, 0], t, kind, dev_nxt)
        if kind == FAR_M:
            return remote(src(opp, 0), far.at[slot, 1], t, kind, dev_prv)
        if kind == NEAR_P:
            return remote(src(nxt, 0), near.at[slot, 0], t, kind, dev_nxt)
        if kind == NEAR_M:
            return remote(src(prv, 1), near.at[slot, 1], t, kind, dev_prv)
        if kind == COMB_P:
            return remote(src(nxt, 1), comb.at[slot, 0], t, kind, dev_nxt)
        return remote(src(prv, 0), comb.at[slot, 1], t, kind, dev_prv)

    def ag_rows(t, c, j, part=None):
        layer, row0 = where_of(t)
        base = row0 + slice_at(c, j)
        if part is None:
            return ures.at[layer, pl.ds(pl.multiple_of(base, slice_rows), slice_rows)]
        return ures.at[layer, pl.ds(pl.multiple_of(base + part * piece, piece), piece)]

    ag_sent = {OWN_P1: (chip, 0, dev_nxt), OWN_P2: (chip, 1, dev_nxt), OWN_M1: (chip, 1, dev_prv), OWN_M2: (chip, 0, dev_prv),
               FW_P: (prv, 0, dev_nxt), FW_M: (nxt, 1, dev_prv),
               D0: (chip, None, dev_sib), D1: (prv, None, dev_sib), D2: (nxt, None, dev_sib), D3: (opp, None, dev_sib)}
    ag_got = {OWN_P1: (core, prv, 0), OWN_P2: (core, prv, 1), OWN_M1: (core, nxt, 1), OWN_M2: (core, nxt, 0),
              FW_P: (core, opp, 0), FW_M: (core, opp, 1),
              D0: (1 - core, chip, None), D1: (1 - core, prv, None), D2: (1 - core, nxt, None), D3: (1 - core, opp, None)}

    def msg_ag(t, kind, merged=False):
        j, part, dev = ag_sent[kind]
        ref = ag_rows(t, core, j, None if merged and kind in (OWN_P1, OWN_M1) else part)
        return remote(ref, ref, t, kind, dev)

    def wait_ag(t, kind, merged=False):
        c, j, part = ag_got[kind]
        ref = ag_rows(t, c, j, None if merged and kind in (OWN_P1, OWN_M1) else part)
        remote(ref, ref, t, kind, dev_sib).wait_recv()

    def msg_stat(t, off):
        slot = lax.rem(t, SLOTS)
        return pltpu.make_async_remote_copy(src_ref=stats.at[slot, me], dst_ref=stats.at[slot, me], send_sem=ssend.at[slot, off],
                                            recv_sem=srecv.at[slot, me], device_id={'tp': lax.rem(me + off, tp_size)}, device_id_type=MESH)

    def in_proj(t):
        layer, row0 = where_of(t)

        @pl.when(layer == 0)
        def _():
            load_hid(t).wait()

        @pl.when(row0 == 0)
        def _():
            pre[:, 0:HALO, :] = jnp.zeros((pre.shape[0], HALO, LANES), F32)

        @pl.when(row0 > 0)
        def _():
            pre[:, 0:HALO, :] = pre[:, CHUNK:CHUNK + HALO, :]

        def norm(load):
            def block(i, carry):
                r = pl.multiple_of(i * 64, 64)
                u = load(pl.multiple_of(row0 + r, 64))
                scale = lax.rsqrt(jnp.mean(u * u, axis=-1, keepdims=True) + EPSILON)
                h[pl.ds(r, 64), :] = (u * scale * nw[layer, 0:1, :]).astype(BF16)
                return carry
            lax.fori_loop(0, CHUNK // 64, block, 0)

        @pl.when(layer == 0)
        def _():
            norm(lambda r: hid[pl.ds(r, 64), :].astype(F32))

        @pl.when(layer > 0)
        def _():
            norm(lambda r: ures[jnp.maximum(layer - 1, 0), pl.ds(r, 64), :])

        wide = 2 * TILE

        def tile(i, carry):
            @pl.when(row0 == 0)
            def _():
                wait_in(layer, 2 * i)
                wait_in(layer, 2 * i + 1)
            o = pl.multiple_of(i * wide, wide)
            prod = jnp.dot(h[...], win[layer, :, pl.ds(o, wide)], preferred_element_type=F32)
            prod = prod.astype(BF16).astype(F32)
            for j in range(wide // LANES):
                pre[i * (wide // LANES) + j, HALO:HALO + CHUNK, :] = prod[:, j * LANES:(j + 1) * LANES]
            return carry
        lax.fori_loop(0, n_tiles // 2, tile, 0)
        prod = lax.dot_general(h[...], wdt[layer], (((1,), (1,)), ((), ())), preferred_element_type=F32)
        dtp[:, 0:wdt.shape[1]] = prod.astype(BF16).astype(F32)

        @pl.when(t == 0)
        def _():
            load_out(0).start()
            for i in range(1, n_chunks):
                load_hid(i).start()

        @pl.when((row0 == CHUNK) & (layer < n_layers - 1))
        def _():
            for k in range(1, n_layers):
                @pl.when(layer == k - 1)
                def _():
                    for cp in load_in(k):
                        cp.start()
                    load_out(k).start()

    def mix(t):
        slot = lax.rem(t, SLOTS)
        layer, row0 = where_of(t)

        @pl.when(row0 == 0)
        def _():
            state[...] = jnp.zeros_like(state)
            state3[...] = jnp.zeros_like(state3)

        def conv(i, carry):
            o = pl.multiple_of(i * LANES, LANES)
            acc = jnp.broadcast_to(cw[layer, conv_width:conv_width + 1, pl.ds(o, LANES)], (CHUNK, LANES))
            for j in range(conv_width):
                first = HALO - (conv_width - 1) + j
                acc = acc + pre[width // LANES + i, first:first + CHUNK, :] * cw[layer, j:j + 1, pl.ds(o, LANES)]
            act[:, pl.ds(o, LANES)] = silu(acc)
            return carry
        lax.fori_loop(0, conv_ch // LANES, conv, 0, unroll=True)

        row_id = lax.broadcasted_iota(jnp.int32, (CHUNK, CHUNK), 0)
        col_id = lax.broadcasted_iota(jnp.int32, (CHUNK, CHUNK), 1)
        lower = row_id >= col_id
        left = col_id < head_dim
        left_row = left[0:1, :]
        dt = softplus(dtp[...] + hp[layer, 0:1, :])
        a = -dt * jnp.exp(hp[layer, 1:2, :])
        ones = jnp.where(lower, 1.0, 0.0).astype(BF16)
        a_cum = sum(fast_dot(ones, part) for part in reversed(split(a)))
        a_cum_t = a_cum.T
        a_last = a_cum[CHUNK - 1:CHUNK, :]
        zero = jnp.zeros((CHUNK, LANES), BF16)
        whole = jnp.exp(a_last)
        skip = hp[layer, 2:3, :]
        b = act[:, width:width + n_state]
        c1, c2, c3 = left_parts(act[:, width + n_state:conv_ch])
        bh, bm, bl = split(b)
        nt = (((1,), (1,)), ((), ()))
        b_mh = jnp.concatenate([bm, bh], axis=1)
        c_dot_b = (fast_dot(c3, jnp.concatenate([bh, bl], axis=1), nt) + fast_dot(c2, b_mh, nt)) + fast_dot(c1, b_mh, nt)
        c_dot_b = jnp.where(lower, c_dot_b, 0.0)
        b1, b2, b3 = left_parts(b.T)
        for o in range(0, width, TILE):
            cols = slice(o, min(o + TILE, width))
            v[:, cols] = three_dots(c1, c2, c3, state3, cols)
        sq = jnp.zeros((CHUNK, LANES), F32)
        for p in range(width // LANES):
            cols = slice(p * LANES, (p + 1) * LANES)
            h0, h1 = 2 * p, 2 * p + 1

            def spread(m):
                return jnp.where(left, m[:, h0:h0 + 1], m[:, h1:h1 + 1])

            def spread_row(m):
                return jnp.where(left_row, m[:, h0:h0 + 1], m[:, h1:h1 + 1])

            cum0 = jnp.broadcast_to(a_cum[:, h0:h0 + 1], (CHUNK, LANES))
            cum1 = jnp.broadcast_to(a_cum[:, h1:h1 + 1], (CHUNK, LANES))
            cum = jnp.where(left, cum0, cum1)

            def mixer(cum_rows, n):
                seg = cum_rows - a_cum_t[n:n + 1, :]
                return split(jnp.exp(jnp.minimum(seg, 0.0)) * c_dot_b)
            x = act[:, cols]
            x_dt = x * spread(dt)
            wh, wm, wl = split(x_dt * jnp.exp(spread_row(a_last) - cum))
            weighted3[0:CHUNK, cols] = wm
            weighted3[CHUNK:2 * CHUNK, cols] = wh
            weighted3[2 * CHUNK:3 * CHUNK, cols] = wl
            xh, xm, xl = (jnp.concatenate([jnp.where(left, part, zero), jnp.where(left, zero, part)], axis=0) for part in split(x_dt))
            mh, mm, ml = (jnp.concatenate(pair, axis=1) for pair in zip(mixer(cum0, h0), mixer(cum1, h1)))
            x_hm = jnp.concatenate([xh, xm], axis=1)
            wide = fast_dot(mm, x_hm) + fast_dot(mh, x_hm)
            y = (fast_dot(ml, xh) + fast_dot(mh, xl)) + wide[:, LANES:] + wide[:, :LANES]
            y = y + v[:, cols] * jnp.exp(cum)
            y = y + spread_row(skip) * x
            gated = y * silu(pre[p, HALO:HALO + CHUNK, :])
            v[:, cols] = gated
            sq = sq + gated * gated
        total = jnp.sum(sq.T, axis=0, keepdims=True)
        stats[slot, me] = jnp.broadcast_to(total, (8, CHUNK))
        for off in range(1, tp_size):
            msg_stat(t, off).start()
        for o in range(0, width, TILE):
            cols = slice(o, min(o + TILE, width))
            decay = jnp.concatenate([jnp.where(left_row, whole[:, n:n + 1], whole[:, n + 1:n + 2])
                                     for n in range(o // head_dim, cols.stop // head_dim, 2)], axis=1)
            s_new = state[:, cols] * decay + three_dots(b1, b2, b3, weighted3, cols)
            state[:, cols] = s_new
            sh, sm, sl = split(s_new)
            state3[0:n_state, cols] = sm
            state3[n_state:2 * n_state, cols] = sh
            state3[2 * n_state:3 * n_state, cols] = sl

    def out_proj(t):
        slot = lax.rem(t, SLOTS)
        layer, row0 = where_of(t)

        @pl.when(row0 == 0)
        def _():
            load_out(layer).wait()
        for off in range(1, tp_size):
            peer = lax.rem(me + off, tp_size)
            pltpu.make_async_remote_copy(src_ref=stats.at[slot, peer], dst_ref=stats.at[slot, peer], send_sem=ssend.at[slot, off],
                                         recv_sem=srecv.at[slot, peer], device_id=dev_sib, device_id_type=MESH).wait_recv()
        for off in range(1, tp_size):
            msg_stat(t, off).wait_send()
        total = stats[slot, 0]
        for r in range(1, tp_size):
            total = total + stats[slot, r]
        scale = lax.rsqrt(total / inner_width + EPSILON)
        scale = jnp.broadcast_to(scale[0:1, :], (LANES, CHUNK)).T
        for p in range(width // LANES):
            cols = slice(p * LANES, (p + 1) * LANES)
            g[:, cols] = (v[:, cols] * scale * gw[layer, 0:1, cols]).astype(BF16)
        buf = pbuf.at[lax.rem(t, P_SLOTS)]

        def tile(i, carry):
            o = pl.multiple_of(i * TILE, TILE)
            buf[:, pl.ds(o, TILE)] = jnp.dot(g[...], wout[layer, :, pl.ds(o, TILE)], preferred_element_type=F32)
            return carry
        lax.fori_loop(0, d_model // TILE, tile, 0, unroll=True)
        msg_rs(t, SIB).start()

    def pair_sum(t):
        msg_rs(t, SIB).wait_recv()
        buf, other = pbuf.at[lax.rem(t, P_SLOTS)], sib.at[lax.rem(t, 2)]

        def block(i, carry):
            r = pl.multiple_of(i * 8, 8)
            mine = pl.ds(pl.multiple_of(core * half_rows + r, 8), 8)
            buf[mine, :] = buf[mine, :] + other[pl.ds(r, 8), :]
            return carry
        lax.fori_loop(0, half_rows // 8, block, 0, unroll=True)
        for kind in (FAR_P, FAR_M, NEAR_P, NEAR_M):
            msg_rs(t, kind).start()

    def relay_sum(t):
        slot = lax.rem(t, SLOTS)
        buf = pbuf.at[lax.rem(t, P_SLOTS)]
        for way, (wait, send, j, part) in enumerate(((FAR_P, COMB_P, nxt, 1), (FAR_M, COMB_M, prv, 0))):
            msg_rs(t, wait).wait_recv()
            rows = pl.ds(pl.multiple_of(slice_at(core, j) + part * piece, piece), piece)
            buf[rows, :] = buf[rows, :] + far[slot, way]
            msg_rs(t, send).start()

    def finish(t, merged):
        slot = lax.rem(t, SLOTS)
        layer, row0 = where_of(t)
        buf = pbuf.at[lax.rem(t, P_SLOTS)]
        for kind in (NEAR_P, NEAR_M, COMB_P, COMB_M):
            msg_rs(t, kind).wait_recv()
        base = slice_at(core, chip)
        dst = pl.ds(pl.multiple_of(row0 + base, slice_rows), slice_rows)

        def store(res):
            lo = buf[pl.ds(base, piece), :] + near[slot, 0] + comb[slot, 1]
            hi = buf[pl.ds(pl.multiple_of(base + piece, piece), piece), :] + near[slot, 1] + comb[slot, 0]
            ures[layer, dst, :] = (res + jnp.concatenate([lo, hi], axis=0)).astype(BF16).astype(F32)

        @pl.when(layer == 0)
        def _():
            store(hid[dst, :].astype(F32))

        @pl.when(layer > 0)
        def _():
            store(ures[jnp.maximum(layer - 1, 0), dst, :])
        for kind in (OWN_P1, OWN_M1, D0) if merged else (OWN_P1, OWN_M1, OWN_P2, OWN_M2, D0):
            msg_ag(t, kind, merged).start()
        for kind in (SIB, FAR_P, FAR_M, NEAR_P, NEAR_M, COMB_P, COMB_M):
            msg_rs(t, kind).wait_send()

    def forward(t, merged):
        for wait, send in ((OWN_P1, FW_P), (OWN_M1, FW_M)):
            wait_ag(t, wait, merged)
            msg_ag(t, send).start()

    def share(t, merged):
        for waits, send in ((() if merged else (OWN_P2,), D1), (() if merged else (OWN_M2,), D2), ((FW_P, FW_M), D3)):
            for kind in waits:
                wait_ag(t, kind)
            msg_ag(t, send).start()

    def collect(t, merged):
        layer, row0 = where_of(t)
        for kind in (D0, D1, D2, D3):
            wait_ag(t, kind)
        for kind in ag_sent:
            if not (merged and kind in (OWN_P2, OWN_M2)):
                msg_ag(t, kind, merged).wait_send()

        @pl.when(layer == n_layers - 1)
        def _():
            def block(i, carry):
                rows = pl.ds(pl.multiple_of(row0 + i * 16, 16), 16)
                out[rows, :] = ures[layer, rows, :].astype(BF16)
                return carry
            lax.fori_loop(0, CHUNK // 16, block, 0)

    def guarded(step, t, first=0, last=n_tasks):
        @pl.when((t >= first) & (t < last))
        def _():
            step(t)

    final = n_tasks - n_chunks

    def iteration(t, carry):
        pl.when(t == -1)(widen)
        guarded(mix, t)
        guarded(pair_sum, t - 1)
        guarded(lambda k: forward(k, True), t - 4, last=final)
        guarded(lambda k: forward(k, False), t - 4, first=final)
        guarded(lambda k: share(k, True), t - 5, last=final)
        guarded(lambda k: collect(k, True), t - 5, last=final)
        guarded(in_proj, t + 1)
        guarded(lambda k: finish(k, True), t - 2, last=final)
        guarded(out_proj, t)
        guarded(relay_sum, t - 1)
        guarded(lambda k: finish(k, False), t - 2, first=final)
        guarded(lambda k: share(k, False), t - 5, first=final)
        guarded(lambda k: collect(k, False), t - 6, first=final)
        return carry
    lax.fori_loop(-1, n_tasks + 6, iteration, 0)


def layers(tp_size, hidden, norm_w, w_z, w_x, w_bc, w_dt, conv_x, conv_bc, bias_x, bias_bc, dt_bias, a_log, d_skip, gate_w, w_out):
    n_batch, n_steps, d_model = hidden.shape
    n_layers, conv_width, width = conv_x.shape
    head_rows = pl.cdiv(dt_bias.shape[-1], 16) * 16
    w_dt = jnp.transpose(w_dt, (2, 0, 1))
    state2 = w_bc.shape[-1]
    piece = CHUNK // tp_size // 2
    any_spec = pl.BlockSpec(memory_space=pl.ANY)
    dma = pltpu.SemaphoreType.DMA
    run = pl.pallas_call(
        functools.partial(kernel, tp_size, conv_width),
        out_shape=pltpu.VMEM((n_steps, d_model), BF16),
        in_specs=[any_spec] * 15,
        out_specs=pl.BlockSpec(memory_space=pltpu.VMEM),
        scratch_shapes=[pltpu.VMEM(p.shape, p.dtype) for p in (norm_w, w_dt, conv_x, conv_bc, bias_x, bias_bc, dt_bias, a_log, d_skip, gate_w)] + [
            pltpu.VMEM((n_steps, d_model), BF16),
            pltpu.VMEM((n_layers, d_model, 2 * width + state2), BF16),
            pltpu.VMEM((n_layers, head_rows, d_model), BF16),
            pltpu.VMEM((n_layers, head_rows, d_model), F32),
            pltpu.VMEM((n_layers, width, d_model), BF16),
            pltpu.VMEM((n_layers, n_steps, d_model), F32),
            pltpu.VMEM((CHUNK, d_model), BF16),
            pltpu.VMEM(((2 * width + state2) // LANES, HALO + CHUNK, LANES), F32),
            pltpu.VMEM((CHUNK, width + state2), F32),
            pltpu.VMEM((CHUNK, width), F32),
            pltpu.VMEM((CHUNK, width), BF16),
            pltpu.VMEM((CHUNK, LANES), F32),
            pltpu.VMEM((state2 // 2, width), F32),
            pltpu.VMEM((3 * state2 // 2, width), BF16),
            pltpu.VMEM((3 * CHUNK, width), BF16),
            pltpu.VMEM((P_SLOTS, CHUNK, d_model), F32),
            pltpu.VMEM((2, CHUNK // 2, d_model), F32),
            pltpu.VMEM((SLOTS, 2, piece, d_model), F32),
            pltpu.VMEM((SLOTS, 2, piece, d_model), F32),
            pltpu.VMEM((SLOTS, 2, piece, d_model), F32),
            pltpu.VMEM((SLOTS, tp_size, 8, CHUNK), F32),
            pltpu.VMEM((n_layers, 8, d_model), F32),
            pltpu.VMEM((n_layers, 8, width + state2), F32),
            pltpu.VMEM((n_layers, 8, width), F32),
            pltpu.VMEM((n_layers, 8, LANES), F32),
            dma((n_layers, (2 * width + state2) // TILE + 1)), dma((n_steps // CHUNK,)), dma((10,)),
            dma((SLOTS, tp_size)), dma((SLOTS, tp_size)), dma((SEM_SLOTS, 17)), dma((SEM_SLOTS, 17)),
        ],
        compiler_params=pltpu.CompilerParams(collective_id=0, has_side_effects=True, vmem_limit_bytes=62_000_000),
    )
    outs = [run(hidden[i], norm_w, w_z, w_x, w_bc, w_dt, conv_x, conv_bc, bias_x, bias_bc, dt_bias, a_log, d_skip, gate_w, w_out)
            for i in range(n_batch)]
    return jnp.stack(outs)


def solution(mesh):
    col_spec = P(None, None, 'tp')
    vec_spec = P(None, 'tp')
    in_specs = (P('dp'), P(), col_spec, col_spec, P(), col_spec, col_spec, P(), vec_spec, P(), vec_spec, vec_spec, vec_spec, vec_spec, P(None, 'tp', None))
    return jax.shard_map(functools.partial(layers, mesh.shape['tp']), mesh=mesh, in_specs=in_specs, out_specs=P('dp'), check_vma=False)
```
